32 devices in a mesh: rep: 8 (over y, x, core), grp: 4 (over z).
Axes of the slice: x: 2, y: 2, z: 4, core: 2. Of those that a mesh axis runs over, the one named last changes fastest.
Arguments:
- tokens: bfloat16 [8, 1024, 512], P('rep', 'grp'), may hold values from -6 to 6
- segments: int32 [8, 1024], P('rep', 'grp'), may hold values from 0 to 1024, as said below
- positions: int32 [8, 1024], P('rep', 'grp'), may hold values from 0 to 1023, as said below
- norm1_gain: bfloat16 [512], P('grp'), may hold values from 0.5 to 1.5
- w_query: bfloat16 [512, 512], P('grp'), may hold values from -0.25 to 0.25
- w_key: bfloat16 [512, 512], P('grp'), may hold values from -0.25 to 0.25
- w_value: bfloat16 [512, 512], P('grp'), may hold values from -0.25 to 0.25
- w_out: bfloat16 [512, 512], P('grp'), may hold values from -1 to 1
- norm2_gain: bfloat16 [512], P('grp'), may hold values from 0.5 to 1.5
- w_gate: bfloat16 [512, 1376], P('grp'), may hold values from -0.25 to 0.25
- w_up: bfloat16 [512, 1376], P('grp'), may hold values from -0.25 to 0.25
- w_down: bfloat16 [1376, 512], P('grp'), may hold values from -0.15625 to 0.15625
- cotangent: bfloat16 [8, 1024, 512], P('rep', 'grp'), may hold values from -6 to 6
Outputs:
- output: bfloat16 [8, 1024, 512], P('rep', 'grp')
- input_grad: float32 [8, 1024, 512], P('rep', 'grp')
- grad_norm1: float32 [512], P('grp')
- grad_query: float32 [512, 512], P('grp')
- grad_key: float32 [512, 512], P('grp')
- grad_value: float32 [512, 512], P('grp')
- grad_out: float32 [512, 512], P('grp')
- grad_norm2: float32 [512], P('grp')
- grad_gate: float32 [512, 1376], P('grp')
- grad_up: float32 [512, 1376], P('grp')
- grad_down: float32 [1376, 512], P('grp')
The draws below stay inside these ranges and needn't reach their ends.
Inputs may be any that keep to these rules, and one draw needn't show every extreme that they name: `segments`: in each sequence the documents are runs of consecutive tokens numbered 1, 2, 3 in order; tokens after the last document, if any, are padding numbered 0. `positions`: A token's index in its sequence minus the index of the first token of its run (its document, or the padding).
All inputs are finite; a program needn't handle non-finite values.
Results may differ from the reference program's by a relative error of at most 0.019.
Values may be sent and summed in bfloat16 or wider, within the bound.
No kernel may reach another device: no remote copies, remote signals or barrier semaphores. Data moves between devices by JAX's collectives and lax.ppermute only.
A program may use at most 64 MiB of HBM per device.

```python
import jax
import jax.numpy as jnp
from jax import lax

D = 512
H = 8
KV = 8
HD = 64
FF = 1376
LEN = 1024
SEQS = 8


def document_layout(key):
    base_key = jax.random.fold_in(key, 7)
    rate_key, pad_key, flag_key = jax.random.split(base_key, 3)
    shifts = jax.random.randint(rate_key, (SEQS, 1), 1, 9)
    rates = jnp.maximum(jnp.right_shift(jnp.full((SEQS, 1), LEN, jnp.int32), shifts), 2)
    rows = jnp.arange(SEQS, dtype=jnp.int32)[:, None]
    padding = jax.random.randint(pad_key, (SEQS, 1), 0, LEN // 4 + 1)
    padding = jnp.where(rows < 2, 0, padding)
    flag_draws = jax.random.randint(flag_key, (SEQS, LEN), 0, 1 << 20)
    indices = jnp.arange(LEN, dtype=jnp.int32)[None, :]
    boundary = LEN - padding
    random_starts = flag_draws % rates == 0
    random_starts = jnp.where(rows == 0, False, jnp.where(rows == 1, True, random_starts))
    starts = random_starts | (indices == 0) | (indices == boundary)
    numbers = jnp.cumsum(starts.astype(jnp.int32), axis=1)
    seg_ids = jnp.where(indices >= boundary, 0, numbers)
    last_start = lax.cummax(jnp.where(starts, indices, 0), axis=1)
    return (seg_ids.astype(jnp.int32), (indices - last_start).astype(jnp.int32))


def draw_segments(key, part):
    seg_ids, places = document_layout(key)
    return seg_ids


def draw_positions(key, part):
    seg_ids, places = document_layout(key)
    return places


def steps_of(key, extent, cuts, low, largest):
    def one(dim, parts):
        steps = jax.random.uniform(jax.random.fold_in(jax.random.fold_in(key, 6), dim), (parts,), jnp.float32, low / len(cuts), largest / len(cuts))
        return jnp.repeat(jnp.exp(steps), extent[dim] // parts).reshape((-1,) + (1,) * (len(extent) - dim - 1))

    level = one(*cuts[0])
    for cut in cuts[1:]:
        level = level * one(*cut)
    return level


def scatter_about(rng, dims, width, reach, cuts=(), kind=jnp.bfloat16):
    level = steps_of(rng, dims, cuts, -0.22, 0.18) if cuts else 1.0
    result = jax.random.normal(rng, dims, jnp.float32) * width * level
    return jnp.minimum(jnp.maximum(result, -reach), reach).astype(kind)


def setup_inputs(seed: int = 0) -> dict:
    seeds = jax.random.split(jax.random.key(seed), 14)
    return {
        "tokens": scatter_about(seeds[0], (SEQS, LEN, D), 1.0, 6.0, ((0, 8), (1, 4))),
        "segments": draw_segments(jax.random.fold_in(seeds[13], 71), 0),
        "positions": draw_positions(jax.random.fold_in(seeds[13], 71), 0),
        "norm1_gain": jnp.clip(1.0 + 0.1 * jax.random.normal(seeds[3], (D,), jnp.float32), 0.5, 1.5).astype(jnp.bfloat16),
        "w_query": scatter_about(seeds[4], (D, H * HD), D ** -0.5, 0.25, ((0, 4),)),
        "w_key": scatter_about(seeds[5], (D, KV * HD), D ** -0.5, 0.25, ((0, 4),)),
        "w_value": scatter_about(seeds[6], (D, KV * HD), D ** -0.5, 0.25, ((0, 4),)),
        "w_out": scatter_about(seeds[7], (H * HD, D), (H * HD // 16) ** -0.5, 1.0, ((0, 4),)),
        "norm2_gain": jnp.clip(1.0 + 0.1 * jax.random.normal(seeds[8], (D,), jnp.float32), 0.5, 1.5).astype(jnp.bfloat16),
        "w_gate": scatter_about(seeds[9], (D, FF), D ** -0.5, 0.25, ((0, 4),)),
        "w_up": scatter_about(seeds[10], (D, FF), D ** -0.5, 0.25, ((0, 4),)),
        "w_down": scatter_about(seeds[11], (FF, D), FF ** -0.5, 0.15625, ((0, 4),)),
        "cotangent": scatter_about(seeds[12], (SEQS, LEN, D), 1.0, 6.0, ((0, 8), (1, 4))),
    }


EPSILON = 1e-05
NEGATIVE = -1e+30

@jax.custom_vjp
def low(v):
    return lax.optimization_barrier(v.astype(jnp.bfloat16)).astype(jnp.float32)

@jax.custom_vjp
def low_back(v):
    return v

def low_keep(v):
    return (low(v), None)

def low_pass(kept, grad):
    return (grad,)

def back_keep(v):
    return (v, None)

def back_low(kept, grad):
    return (low(grad),)
low.defvjp(low_keep, low_pass)
low_back.defvjp(back_keep, back_low)

def norm_scale(values):
    return lax.rsqrt(lax.optimization_barrier(jnp.mean(values * values, axis=-1, keepdims=True)) + EPSILON)

def rotate(values, positions):
    halves = values.shape[-1] // 2
    frequency = 10000.0 ** (-2.0 * jnp.arange(halves, dtype=jnp.float32) / values.shape[-1])
    angles = positions.astype(jnp.float32)[..., None, None] * frequency
    cosine = jnp.cos(angles)
    sines = jnp.sin(angles)
    first_half = values[..., :halves]
    second_half = values[..., halves:]
    return jnp.concatenate([first_half * cosine - second_half * sines, second_half * cosine + first_half * sines], axis=-1)

def layer(weights_all, inputs, segments, positions):
    gain_in, w_query, w_key, w_value, w_out, gain_mid, w_gate, w_up, w_down = weights_all
    highest = lax.Precision.HIGHEST
    batches = inputs.shape[0]
    length = inputs.shape[1]
    normed_in = low(inputs * norm_scale(inputs) * gain_in)
    query_raw = low_back(jnp.einsum('bld,de->ble', normed_in, w_query, precision=highest))
    key_raw = low_back(jnp.einsum('bld,de->ble', normed_in, w_key, precision=highest))
    value_raw = low_back(jnp.einsum('bld,de->ble', normed_in, w_value, precision=highest))
    query_rot = low(rotate(query_raw.reshape(batches, length, H, HD), positions)).reshape(batches, length, KV, H // KV, HD)
    key_rot = low(rotate(key_raw.reshape(batches, length, KV, HD), positions))
    value_low = low(value_raw.reshape(batches, length, KV, HD))
    indices = jnp.arange(length, dtype=jnp.int32)
    same_seg = segments[:, :, None] == segments[:, None, :]
    causal = indices[:, None] >= indices[None, :]
    diagonal = indices[:, None] == indices[None, :]
    allowed = same_seg & causal[None] & ((segments[:, :, None] != 0) | diagonal[None])
    scores = low_back(jnp.einsum('bqkgd,bjkd->bkgqj', query_rot, key_rot, precision=highest) * HD ** (-0.5))
    masked = jnp.where(allowed[:, None, None], scores, NEGATIVE)
    attn_weights = low(jax.nn.softmax(masked, axis=-1))
    attended = jnp.einsum('bkgqj,bjkd->bqkgd', attn_weights, value_low, precision=highest).reshape(batches, length, H * HD)
    attn_low = low(low_back(attended))
    middle = inputs + low_back(jnp.einsum('ble,ed->bld', attn_low, w_out, precision=highest))
    normed_mid = low(middle * norm_scale(middle) * gain_mid)
    gate_raw = low_back(jnp.einsum('bld,df->blf', normed_mid, w_gate, precision=highest))
    up_raw = low_back(jnp.einsum('bld,df->blf', normed_mid, w_up, precision=highest))
    hidden_low = low(jax.nn.silu(gate_raw) * up_raw)
    return middle + low_back(jnp.einsum('blf,fd->bld', hidden_low, w_down, precision=highest))

def reference(tokens, segments, positions, norm1_gain, w_query, w_key, w_value, w_out, norm2_gain, w_gate, w_up, w_down, cotangent):
    weights_all = (norm1_gain.astype(jnp.float32), w_query.astype(jnp.float32), w_key.astype(jnp.float32), w_value.astype(jnp.float32), w_out.astype(jnp.float32), norm2_gain.astype(jnp.float32), w_gate.astype(jnp.float32), w_up.astype(jnp.float32), w_down.astype(jnp.float32))
    pair_count = SEQS // 2
    pair_tokens = tokens.astype(jnp.float32).reshape(pair_count, 2, LEN, D)
    pair_segments = segments.astype(jnp.int32).reshape(pair_count, 2, LEN)
    pair_positions = positions.astype(jnp.int32).reshape(pair_count, 2, LEN)
    pair_cotangent = cotangent.astype(jnp.float32).reshape(pair_count, 2, LEN, D)

    def pair_step(summed, items):
        block_tokens, block_segments, block_positions, block_cotangent = items

        def forward(weights_now, inputs):
            return layer(weights_now, inputs, block_segments, block_positions)
        outputs, pullback = jax.vjp(forward, weights_all, block_tokens)
        gradients, input_part = pullback(block_cotangent)
        summed = jax.tree.map(jnp.add, summed, gradients)
        return (summed, (outputs.astype(jnp.bfloat16), input_part))
    initial = jax.tree.map(jnp.zeros_like, weights_all)
    summed, (outputs, input_parts) = lax.scan(pair_step, initial, (pair_tokens, pair_segments, pair_positions, pair_cotangent))
    return (outputs.reshape(SEQS, LEN, D), input_parts.reshape(SEQS, LEN, D), summed[0], summed[1], summed[2], summed[3], summed[4], summed[5], summed[6], summed[7], summed[8])
```

```python
import functools

import jax
import jax.numpy as jnp
import numpy as np
from jax import lax
from jax.experimental import pallas as pl
from jax.experimental.pallas import tpu as pltpu
from jax.sharding import PartitionSpec as P

D = 512
H = 8
HD = 64
FF = 1376
EPSILON = 1e-05
NEGATIVE = -1e30
SR = 16
PAIR = 2 * HD
F32 = jnp.float32
BF16 = jnp.bfloat16
VMEM = pl.BlockSpec(memory_space=pltpu.VMEM)
SMEM = pl.BlockSpec(memory_space=pltpu.SMEM)
PARAMS = pltpu.CompilerParams(vmem_limit_bytes=56 * 1024 * 1024)


class Plan:
    def __init__(self, mesh, tokens_shape):
        self.rep = mesh.shape["rep"]
        self.grp = mesh.shape["grp"]
        self.rows = D // self.grp
        self.slices = min(self.rep, self.rows // SR)
        self.half = self.slices // 2
        self.down = FF // self.grp
        self.pieces = -(-self.down // (self.slices * SR))
        self.down_pad = self.pieces * self.slices * SR
        self.ffp = self.down_pad * self.grp
        self.local = tokens_shape[1] // self.grp
        self.full = self.local * self.grp
        self.wide_a = 4 * D + 128
        self.wide_b = 2 * self.ffp + self.pieces * D


def dot(left, right, dims):
    return lax.dot_general(left, right, ((dims[0], dims[1]), ((), ())), preferred_element_type=F32)


def mm(left, right):
    return dot(left, right, ((1,), (0,)))


def against(left, right):
    return dot(left, right, ((1,), (1,)))


def rows_of(left, right):
    return dot(left, right, ((0,), (0,)))


def call(body, outs, name, args, scratch=(), flops=0, moved=0):
    specs = [SMEM if a.dtype == jnp.int32 and a.ndim == 1 else VMEM for a in args]
    return pl.pallas_call(
        body,
        out_shape=outs,
        in_specs=specs,
        out_specs=[VMEM] * len(outs),
        scratch_shapes=scratch,
        compiler_params=PARAMS,
        cost_estimate=pl.CostEstimate(flops=flops, bytes_accessed=moved, transcendentals=0),
        name=name,
    )(*args)


def sds(shape, dtype):
    return jax.ShapeDtypeStruct(shape, dtype)


def swap(axis, k, size, value):
    return lax.ppermute(value, axis, [(i, i ^ k) for i in range(size)])


def shift(k, size, value):
    return lax.ppermute(value, "grp", [(i, i + k) for i in range(size) if 0 <= i + k < size])


def xor(a, b):
    return lax.bitwise_xor(a, jnp.int32(b)) if isinstance(b, int) else lax.bitwise_xor(a, b)


def aligned(index):
    return pl.multiple_of(index, SR)


def rotary_tables(plan):
    halves = HD // 2
    frequency = 10000.0 ** (-2.0 * np.arange(halves) / HD)
    place = np.concatenate([np.arange(plan.local) - k * plan.local for k in range(plan.grp)])
    angle = place[:, None] * frequency[None, :]
    cosine = np.tile(np.cos(angle), (1, 4)).astype(np.float32)
    sines = np.tile(np.concatenate([-np.sin(angle), np.sin(angle)], axis=1), (1, 2))
    return cosine, sines.astype(np.float32)


def swap_halves(value):
    wide = value.shape[1]
    lane = lax.broadcasted_iota(jnp.int32, value.shape, 1)
    first = (lane % HD) < HD // 2
    return jnp.where(
        first, pltpu.roll(value, wide - HD // 2, 1), pltpu.roll(value, HD // 2, 1)
    )


def tile_heads(table, wide):
    return jnp.concatenate([table] * (wide // table.shape[1]), axis=1)


def rotate(value, cosine, sines):
    wide = value.shape[1]
    return value * tile_heads(cosine, wide) + swap_halves(value) * tile_heads(sines, wide)


def rotate_back(value, cosine, sines):
    wide = value.shape[1]
    return value * tile_heads(cosine, wide) - swap_halves(value) * tile_heads(sines, wide)


def two_heads(value):
    lane = lax.broadcasted_iota(jnp.int32, value.shape, 1)
    zero = jnp.zeros_like(value)
    return jnp.concatenate(
        [jnp.where(lane < HD, value, zero), jnp.where(lane < HD, zero, value)], axis=0
    )


def one_pair(value):
    count = value.shape[1] // 2
    return jnp.concatenate([value[:HD, :count], value[HD:, count:]], axis=0).T


def mask_bias(plan, reach, bias_ref):
    n = plan.local
    key = lax.broadcasted_iota(jnp.int32, (n, n), 0)
    query = lax.broadcasted_iota(jnp.int32, (n, n), 1)
    for k in range(plan.grp):
        offset = query - key + k * n
        seen = (offset >= 0) & (offset <= reach)
        bias = jnp.where(seen, 0.0, NEGATIVE).astype(F32)
        bias_ref[k * n : (k + 1) * n, :] = jnp.concatenate([bias, bias], axis=1)


def each_slice(plan, place, slice_id, mine, part, store):
    for c, source in enumerate((mine, part)):
        for o in range(plan.half):
            for k in range(1, plan.grp):
                row = (o * (plan.grp - 1) + k - 1) * SR
                store(xor(place, k), xor(slice_id, 2 * o + c), source[row : row + SR, :])


def attend_kernel(plan, ids, *refs):
    g = plan.grp
    parts = refs[:g]
    own = refs[g : g + 4]
    mine, part, gain, cosine, sines, reach = refs[g + 4 : g + 10]
    attn_ref, q_ref, k_ref, v_ref, n1_ref, lse_ref, wa_ref = refs[g + 10 : g + 17]
    bias_ref, = refs[g + 17 :]
    n = plan.local
    place, slice_id = ids[0], ids[1]
    for i in range(4):
        wa_ref[pl.ds(aligned(place * plan.rows), plan.rows), i * D : (i + 1) * D] = own[i][...]

    def store(z, s, rows):
        wa_ref[pl.ds(aligned(z * plan.rows + s * SR), SR), :] = rows[:, : 4 * D]

    each_slice(plan, place, slice_id, mine, part, store)
    mask_bias(plan, reach[...], bias_ref)
    gains = gain[...]
    for k in range(g):
        x = parts[k][...].astype(F32)
        unit = x * lax.rsqrt(jnp.mean(x * x, axis=1, keepdims=True) + EPSILON)
        n1 = (unit * gains).astype(BF16)
        rows = slice(k * n, (k + 1) * n)
        n1_ref[rows, :] = n1
        cos_k, sin_k = cosine[rows, :], sines[rows, :]
        k_ref[rows, :] = rotate(mm(n1, wa_ref[:, D : 2 * D]), cos_k, sin_k).astype(BF16)
        v_ref[rows, :] = mm(n1, wa_ref[:, 2 * D : 3 * D]).astype(BF16)
        if k == 0:
            q_ref[...] = rotate(mm(n1, wa_ref[:, :D]), cos_k, sin_k).astype(BF16) * BF16(
                HD**-0.5
            )

    def pair(i, carry):
        lanes = pl.ds(pl.multiple_of(i * PAIR, PAIR), PAIR)
        score = against(k_ref[:, lanes], two_heads(q_ref[:, lanes])) + bias_ref[...]
        peak = jnp.max(score, axis=0, keepdims=True)
        exponent = jnp.exp(score - peak)
        total = jnp.sum(exponent, axis=0, keepdims=True)
        out = rows_of(v_ref[:, lanes], exponent.astype(BF16)) / total
        attn_ref[:, lanes] = one_pair(out)
        lse_ref[i] = peak + jnp.log(total)
        return carry

    lax.fori_loop(0, H // 2, pair, 0)


def mlp_kernel(plan, ids, *refs):
    attn, x0, wa, gain, cot, own, mine, part = refs[:8]
    out_ref, dx1_ref, dout_ref, dattn_ref, n2_ref, hid_ref, dg_ref, dup_ref, attn_ref, norm_ref = refs[8:18]
    wgu_ref, wd_ref = refs[18:]
    ffp = plan.ffp
    place, slice_id = ids[0], ids[1]

    def store(z, s, rows):
        wgu_ref[pl.ds(aligned(z * plan.rows + s * SR), SR), :] = rows[:, : 2 * ffp]
        for i in range(plan.pieces):
            at = z * plan.down_pad + (s * plan.pieces + i) * SR
            wd_ref[pl.ds(aligned(at), SR), :] = rows[:, 2 * ffp + i * D : 2 * ffp + (i + 1) * D]

    for s in range(plan.slices):
        store(place, s, own[s * SR : (s + 1) * SR, :])
    each_slice(plan, place, slice_id, mine, part, store)

    attn_low = attn[...].astype(BF16)
    attn_ref[...] = attn_low
    x1 = x0[...].astype(F32) + mm(attn_low, wa[:, 3 * D : 4 * D])
    scale = lax.rsqrt(jnp.mean(x1 * x1, axis=1, keepdims=True) + EPSILON)
    unit = x1 * scale
    gains = gain[...]
    n2 = (unit * gains).astype(BF16)
    n2_ref[...] = n2
    c = cot[...]
    out = x1
    dn2 = jnp.zeros_like(x1)
    step = 512 if ffp % 512 == 0 else ffp
    for f in range(0, ffp, step):
        cols = slice(f, f + step)
        up_cols = slice(ffp + f, ffp + f + step)
        gate = mm(n2, wgu_ref[:, cols])
        up = mm(n2, wgu_ref[:, up_cols])
        dhid = against(c, wd_ref[cols, :])
        sig = 1.0 / (1.0 + jnp.exp(-gate))
        silu = gate * sig
        hid = (silu * up).astype(BF16)
        dup = (dhid * silu).astype(BF16)
        dg = (dhid * up * (sig * (1.0 + gate * (1.0 - sig)))).astype(BF16)
        hid_ref[:, cols] = hid
        dg_ref[:, cols] = dg
        dup_ref[:, cols] = dup
        out = out + mm(hid, wd_ref[cols, :])
        dn2 = dn2 + against(dg, wgu_ref[:, cols]) + against(dup, wgu_ref[:, up_cols])
    out_ref[...] = out.astype(BF16)
    norm_ref[...] = jnp.sum(dn2 * unit, axis=0, keepdims=True)
    e2 = dn2 * gains
    dx1 = c.astype(F32) + scale * (e2 - unit * jnp.mean(e2 * unit, axis=1, keepdims=True))
    dx1_ref[...] = dx1
    dout = dx1.astype(BF16)
    dout_ref[...] = dout
    dattn_ref[...] = against(dout, wa[:, 3 * D : 4 * D]).astype(BF16)


def spread(plan, place, slice_id, keep, send, copy):
    for c, target in enumerate((keep, send)):
        for o in range(plan.half):
            for k in range(plan.grp):
                copy(xor(place, k), xor(slice_id, 2 * o + c), target, o, k)


def mlp_grads_kernel(plan, ids, n2, hid, dg, dup, cot, keep, send, gu_ref, d_ref):
    ffp = plan.ffp
    n2_t = n2[...].T
    gu_ref[:, :ffp] = mm(n2_t, dg[...]).astype(BF16)
    gu_ref[:, ffp:] = mm(n2_t, dup[...]).astype(BF16)
    d_ref[...] = rows_of(hid[...], cot[...]).astype(BF16)

    def copy(z, s, target, o, k):
        target[o, k, :, : 2 * ffp] = gu_ref[pl.ds(aligned(z * plan.rows + s * SR), SR), :]
        for i in range(plan.pieces):
            at = z * plan.down_pad + (s * plan.pieces + i) * SR
            target[o, k, :, 2 * ffp + i * D : 2 * ffp + (i + 1) * D] = d_ref[
                pl.ds(aligned(at), SR), :
            ]

    spread(plan, ids[0], ids[1], keep, send, copy)


def attend_back_kernel(plan, q, k_in, v_in, attn, dattn, lse, cosine, sines, reach, dq_ref, dk_ref, dv_ref, bias_ref, dq_scr, dk_scr):
    mask_bias(plan, reach[...], bias_ref)

    def pair(i, carry):
        lanes = pl.ds(pl.multiple_of(i * PAIR, PAIR), PAIR)
        q2 = two_heads(q[:, lanes])
        da = dattn[:, lanes]
        da2 = two_heads(da)
        prod = two_heads(da.astype(F32) * attn[:, lanes])
        ones = jnp.ones((8, PAIR), F32)
        mean = lax.dot_general(
            ones, prod, (((1,), (1,)), ((), ())), precision=lax.Precision.HIGHEST,
            preferred_element_type=F32,
        )[0:1, :]
        keys = k_in[:, lanes]
        values = v_in[:, lanes]
        prob = jnp.exp(against(keys, q2) + (bias_ref[...] - lse[i]))
        dprob = against(values, da2)
        dscore = (prob * (dprob - mean)).astype(BF16)
        dv_ref[:, lanes] = mm(prob.astype(BF16), da2).astype(BF16)
        dk_scr[:, lanes] = mm(dscore, q2)
        dq_scr[:, lanes] = one_pair(rows_of(keys, dscore)) * (HD**-0.5)
        return carry

    lax.fori_loop(0, H // 2, pair, 0)
    n = plan.local
    dq_ref[...] = rotate_back(dq_scr[...], cosine[:n, :], sines[:n, :]).astype(BF16)
    for k in range(plan.grp):
        rows = slice(k * n, (k + 1) * n)
        dk_ref[rows, :] = rotate_back(dk_scr[rows, :], cosine[rows, :], sines[rows, :]).astype(BF16)


def input_kernel(plan, *refs):
    g = plan.grp
    parts = refs[:g]
    dq, dk, dv, wa = refs[g : g + 4]
    own_ref, norm_ref = refs[g + 4 : g + 6]
    sends = refs[g + 6 :]
    n = plan.local
    norm = jnp.zeros((1, D), F32)
    for k in reversed(range(g)):
        rows = slice(k * n, (k + 1) * n)
        dn1 = against(dk[rows, :], wa[:, D : 2 * D]) + against(dv[rows, :], wa[:, 2 * D : 3 * D])
        if k == 0:
            dn1 = dn1 + against(dq[...], wa[:, :D])
            own_ref[...] = dn1
        else:
            sends[k - 1][...] = dn1.astype(BF16)
        x = parts[k][...].astype(F32)
        unit = x * lax.rsqrt(jnp.mean(x * x, axis=1, keepdims=True) + EPSILON)
        norm = norm + jnp.sum(dn1 * unit, axis=0, keepdims=True)
    norm_ref[...] = norm


def attend_grads_kernel(plan, ids, n1, dq, dk, dv, attn, dout, norms, keep, send, ga_ref):
    n1_t = n1[...].T
    ga_ref[:, :D] = mm(n1_t[:, : plan.local], dq[...]).astype(BF16)
    ga_ref[:, D : 2 * D] = mm(n1_t, dk[...]).astype(BF16)
    ga_ref[:, 2 * D : 3 * D] = mm(n1_t, dv[...]).astype(BF16)
    ga_ref[:, 3 * D :] = rows_of(attn[...], dout[...]).astype(BF16)

    def copy(z, s, target, o, k):
        target[o, k, :, : 4 * D] = ga_ref[pl.ds(aligned(z * plan.rows + s * SR), SR), :]
        flag = (s == 0).astype(F32)
        target[o, k, :, 4 * D :] = (norms[z] * flag).astype(BF16)

    spread(plan, ids[0], ids[1], keep, send, copy)


def finish_kernel(plan, ids, mine, part, out_ref):
    for c, source in enumerate((mine, part)):
        for o in range(plan.half):
            s = xor(ids[1], 2 * o + c)
            out_ref[pl.ds(aligned(s * SR), SR), :] = source[o * SR : (o + 1) * SR, :].astype(F32)


def residual_kernel(plan, *refs):
    own, x0, dx1, gain = refs[:4]
    received = refs[4:-1]
    out_ref = refs[-1]
    dn1 = own[...]
    for r in received:
        dn1 = dn1 + r[...].astype(F32)
    x = x0[...].astype(F32)
    scale = lax.rsqrt(jnp.mean(x * x, axis=1, keepdims=True) + EPSILON)
    unit = x * scale
    e1 = dn1 * gain[...]
    out_ref[...] = dx1[...] + scale * (e1 - unit * jnp.mean(e1 * unit, axis=1, keepdims=True))


def fetch(plan, slab):
    parts = [swap("grp", k, plan.grp, slab) for k in range(1, plan.grp)]
    block = jnp.concatenate(parts, axis=0)
    mine = jnp.concatenate(
        [block] + [swap("rep", 2 * o, plan.rep, block) for o in range(1, plan.half)], axis=0
    )
    return mine, swap("rep", 1, plan.rep, mine)


def add(*values):
    total = values[0].astype(F32)
    for v in values[1:]:
        total = total + v.astype(F32)
    return total.astype(BF16)


def combine(plan, keep, send):
    got = swap("rep", 1, plan.rep, send)
    terms = [add(keep[o], got[o]) for o in range(plan.half)]
    total = add(
        terms[0], *[swap("rep", 2 * o, plan.rep, terms[o]) for o in range(1, plan.half)]
    )
    final = add(total[0], *[swap("grp", k, plan.grp, total[k]) for k in range(1, plan.grp)])
    bit = plan.slices
    while bit < plan.rep:
        final = add(final, swap("rep", bit, plan.rep, final))
        bit *= 2
    mine = jnp.concatenate(
        [final] + [swap("rep", 2 * o, plan.rep, final) for o in range(1, plan.half)], axis=0
    )
    return mine, swap("rep", 1, plan.rep, mine)


def pad_columns(plan, weight):
    rows = weight.shape[0]
    blocks = weight.reshape(rows, plan.grp, plan.down)
    blocks = jnp.pad(blocks, ((0, 0), (0, 0), (0, plan.down_pad - plan.down)))
    return blocks.reshape(rows, plan.ffp)


def drop_columns(plan, grad):
    return jnp.concatenate(
        [grad[:, z * plan.down_pad : z * plan.down_pad + plan.down] for z in range(plan.grp)],
        axis=1,
    )


def body(plan, tokens, segments, positions, norm1_gain, w_query, w_key, w_value, w_out, norm2_gain, w_gate, w_up, w_down, cotangent):
    g, n = plan.grp, plan.local
    place = lax.axis_index("grp").astype(jnp.int32)
    slice_id = (lax.axis_index("rep") % plan.slices).astype(jnp.int32)
    ids = jnp.stack([place, slice_id])
    x0 = tokens.reshape(n, D)
    cot = cotangent.reshape(n, D)
    reach = jnp.where(segments != 0, positions, 0).reshape(1, n)
    table_cos, table_sin = rotary_tables(plan)
    cosine, sines = jnp.asarray(table_cos), jnp.asarray(table_sin)

    gains = jnp.stack([norm1_gain, norm2_gain])
    gain_tile = jnp.pad(gains, ((0, SR - 2), (0, 128 - plan.rows)))
    own_a = (w_query, w_key, w_value, w_out)
    start = slice_id * SR
    slab_a = jnp.concatenate(
        [lax.dynamic_slice(w, (start, 0), (SR, D)) for w in own_a] + [gain_tile], axis=1
    )
    down_rows = jnp.pad(w_down, ((0, plan.down_pad - plan.down), (0, 0)))
    down_rows = down_rows.reshape(plan.slices, plan.pieces, SR, D).transpose(0, 2, 1, 3)
    own_b = jnp.concatenate(
        [
            pad_columns(plan, w_gate),
            pad_columns(plan, w_up),
            down_rows.reshape(plan.rows, plan.pieces * D),
        ],
        axis=1,
    )
    slab_b = lax.dynamic_slice(own_b, (start, 0), (SR, plan.wide_b))

    mine_a, part_a = fetch(plan, slab_a)
    parts = [x0] + [shift(k, g, x0) for k in range(1, g)]
    mine_b, part_b = fetch(plan, slab_b)

    tiles = jnp.stack(
        [gains] + [mine_a[k * SR : k * SR + 2, 4 * D : 4 * D + plan.rows] for k in range(g - 1)]
    )
    order = jnp.bitwise_xor(jnp.arange(g, dtype=jnp.int32), place)
    chosen = sum(
        jnp.where((order == k)[:, None, None], tiles[k][None], 0).astype(F32) for k in range(g)
    )
    gain1 = chosen[:, 0].reshape(1, D)
    gain2 = chosen[:, 1].reshape(1, D)

    full = plan.full
    attn, q, k_all, v_all, n1, lse, wa = call(
        functools.partial(attend_kernel, plan),
        [
            sds((n, D), F32),
            sds((n, D), BF16),
            sds((full, D), BF16),
            sds((full, D), BF16),
            sds((full, D), BF16),
            sds((H // 2, 1, 2 * n), F32),
            sds((D, 4 * D), BF16),
        ],
        "attend",
        (ids, *parts, *own_a, mine_a, part_a, gain1, cosine, sines, reach),
        [pltpu.VMEM((full, 2 * n), F32)],
        flops=4 * 10**9,
        moved=8 * 10**6,
    )

    ffp = plan.ffp
    output, dx1, dout, dattn, n2, hid, dg, dup, attn_low, norm2 = call(
        functools.partial(mlp_kernel, plan),
        [
            sds((n, D), BF16),
            sds((n, D), F32),
            sds((n, D), BF16),
            sds((n, D), BF16),
            sds((n, D), BF16),
            sds((n, ffp), BF16),
            sds((n, ffp), BF16),
            sds((n, ffp), BF16),
            sds((n, D), BF16),
            sds((1, D), F32),
        ],
        "mlp",
        (ids, attn, x0, wa, gain2, cot, own_b, mine_b, part_b),
        [pltpu.VMEM((D, 2 * ffp), BF16), pltpu.VMEM((ffp, D), BF16)],
        flops=4 * 10**9,
        moved=12 * 10**6,
    )

    slabs_b = sds((plan.half, g, SR, plan.wide_b), BF16)
    keep_b, send_b = call(
        functools.partial(mlp_grads_kernel, plan),
        [slabs_b, slabs_b],
        "mlp_grads",
        (ids, n2, hid, dg, dup, cot),
        [pltpu.VMEM((D, 2 * ffp), BF16), pltpu.VMEM((ffp, D), BF16)],
        flops=2 * 10**9,
        moved=8 * 10**6,
    )
    dq, dk, dv = call(
        functools.partial(attend_back_kernel, plan),
        [sds((n, D), BF16), sds((full, D), BF16), sds((full, D), BF16)],
        "attend_back",
        (q, k_all, v_all, attn, dattn, lse, cosine, sines, reach),
        [pltpu.VMEM((full, 2 * n), F32), pltpu.VMEM((n, D), F32), pltpu.VMEM((full, D), F32)],
        flops=8 * 10**9,
        moved=8 * 10**6,
    )
    own, norm1, *sends = call(
        functools.partial(input_kernel, plan),
        [sds((n, D), F32), sds((1, D), F32)] + [sds((n, D), BF16)] * (g - 1),
        "dn1",
        (*parts, dq, dk, dv, wa),
        flops=2 * 10**9,
        moved=4 * 10**6,
    )
    received = [shift(-k, g, sends[k - 1]) for k in range(1, g)]

    norms = jnp.concatenate([norm1, norm2], axis=0).reshape(2, g, plan.rows).transpose(1, 0, 2)
    norms = jnp.pad(norms, ((0, 0), (0, SR - 2), (0, 128 - plan.rows)))
    slabs_a = sds((plan.half, g, SR, plan.wide_a), BF16)
    keep_a, send_a = call(
        functools.partial(attend_grads_kernel, plan),
        [slabs_a, slabs_a],
        "attend_grads",
        (ids, n1, dq, dk, dv, attn_low, dout, norms),
        [pltpu.VMEM((D, 4 * D), BF16)],
        flops=2 * 10**9,
        moved=8 * 10**6,
    )

    def finish(halves, wide, name):
        (out,) = call(
            functools.partial(finish_kernel, plan),
            [sds((plan.slices * SR, wide), F32)],
            name,
            (ids, *halves),
            moved=4 * 10**6,
        )
        return out

    grads_b = finish(combine(plan, keep_b, send_b), plan.wide_b, "finish_b")
    grads_a = finish(combine(plan, keep_a, send_a), plan.wide_a, "finish_a")
    (input_grad,) = call(
        functools.partial(residual_kernel, plan),
        [sds((n, D), F32)],
        "residual",
        (own, x0, dx1, gain1, *received),
        moved=4 * 10**6,
    )
    down = grads_b[:, 2 * ffp :].reshape(plan.slices, SR, plan.pieces, D).transpose(0, 2, 1, 3)
    return (
        output.reshape(tokens.shape),
        input_grad.reshape(tokens.shape),
        grads_a[0, 4 * D : 4 * D + plan.rows],
        grads_a[:, :D],
        grads_a[:, D : 2 * D],
        grads_a[:, 2 * D : 3 * D],
        grads_a[:, 3 * D : 4 * D],
        grads_a[1, 4 * D : 4 * D + plan.rows],
        drop_columns(plan, grads_b[:, :ffp]),
        drop_columns(plan, grads_b[:, ffp : 2 * ffp]),
        down.reshape(plan.down_pad, D)[: plan.down],
    )


def solution(mesh):
    wide, line, pair = P("grp", None), P("grp"), P("rep", "grp")
    three = P("rep", "grp", None)

    def run(tokens, *rest):
        plan = Plan(mesh, tokens.shape)
        return jax.shard_map(
            functools.partial(body, plan),
            mesh=mesh,
            in_specs=(three, pair, pair, line, wide, wide, wide, wide, line, wide, wide, wide, three),
            out_specs=(three, three, line, wide, wide, wide, wide, line, wide, wide, wide),
            check_vma=False,
        )(tokens, *rest)

    return run
```

```python
import functools

import jax
import jax.numpy as jnp
import numpy as np
from jax import lax
from jax.experimental import pallas as pl
from jax.experimental.pallas import tpu as pltpu
from jax.sharding import PartitionSpec as P

D = 512
H = 8
HD = 64
FF = 1376
EPSILON = 1e-05
NEGATIVE = -1e30
SR = 16
PAIR = 2 * HD
F32 = jnp.float32
BF16 = jnp.bfloat16
VMEM = pl.BlockSpec(memory_space=pltpu.VMEM)
SMEM = pl.BlockSpec(memory_space=pltpu.SMEM)
PARAMS = pltpu.CompilerParams(vmem_limit_bytes=56 * 1024 * 1024)


class Plan:
    def __init__(self, mesh, tokens_shape):
        self.rep = mesh.shape["rep"]
        self.grp = mesh.shape["grp"]
        self.rows = D // self.grp
        self.slices = min(self.rep, self.rows // SR)
        self.half = self.slices // 2
        self.down = FF // self.grp
        self.pieces = -(-self.down // (self.slices * SR))
        self.down_pad = self.pieces * self.slices * SR
        self.ffp = self.down_pad * self.grp
        self.local = tokens_shape[1] // self.grp
        self.full = self.local * self.grp
        self.wide_a = 4 * D + 128
        self.wide_b = 2 * self.ffp + self.pieces * D


def dot(left, right, dims):
    return lax.dot_general(left, right, ((dims[0], dims[1]), ((), ())), preferred_element_type=F32)


def mm(left, right):
    return dot(left, right, ((1,), (0,)))


def against(left, right):
    return dot(left, right, ((1,), (1,)))


def rows_of(left, right):
    return dot(left, right, ((0,), (0,)))


def call(body, outs, name, args, scratch=(), flops=0, moved=0):
    specs = [SMEM if a.dtype == jnp.int32 and a.ndim == 1 else VMEM for a in args]
    return pl.pallas_call(
        body,
        out_shape=outs,
        in_specs=specs,
        out_specs=[VMEM] * len(outs),
        scratch_shapes=scratch,
        compiler_params=PARAMS,
        cost_estimate=pl.CostEstimate(flops=0, bytes_accessed=0, transcendentals=0),
        name=name,
    )(*args)


def sds(shape, dtype):
    return jax.ShapeDtypeStruct(shape, dtype)


def swap(axis, k, size, value):
    return lax.ppermute(value, axis, [(i, i ^ k) for i in range(size)])


def shift(k, size, value):
    return lax.ppermute(value, "grp", [(i, i + k) for i in range(size) if 0 <= i + k < size])


def xor(a, b):
    return lax.bitwise_xor(a, jnp.int32(b)) if isinstance(b, int) else lax.bitwise_xor(a, b)


def aligned(index):
    return pl.multiple_of(index, SR)


def rotary_tables(plan):
    halves = HD // 2
    frequency = 10000.0 ** (-2.0 * np.arange(halves) / HD)
    place = np.concatenate([np.arange(plan.local) - k * plan.local for k in range(plan.grp)])
    angle = place[:, None] * frequency[None, :]
    cosine = np.tile(np.cos(angle), (1, 4)).astype(np.float32)
    sines = np.tile(np.concatenate([-np.sin(angle), np.sin(angle)], axis=1), (1, 2))
    return cosine, sines.astype(np.float32)


def swap_halves(value):
    wide = value.shape[1]
    lane = lax.broadcasted_iota(jnp.int32, value.shape, 1)
    first = (lane % HD) < HD // 2
    return jnp.where(
        first, pltpu.roll(value, wide - HD // 2, 1), pltpu.roll(value, HD // 2, 1)
    )


def tile_heads(table, wide):
    return jnp.concatenate([table] * (wide // table.shape[1]), axis=1)


def rotate(value, cosine, sines):
    wide = value.shape[1]
    return value * tile_heads(cosine, wide) + swap_halves(value) * tile_heads(sines, wide)


def rotate_back(value, cosine, sines):
    wide = value.shape[1]
    return value * tile_heads(cosine, wide) - swap_halves(value) * tile_heads(sines, wide)


def two_heads(value):
    lane = lax.broadcasted_iota(jnp.int32, value.shape, 1)
    zero = jnp.zeros_like(value)
    return jnp.concatenate(
        [jnp.where(lane < HD, value, zero), jnp.where(lane < HD, zero, value)], axis=0
    )


def one_pair(value):
    count = value.shape[1] // 2
    return jnp.concatenate([value[:HD, :count], value[HD:, count:]], axis=0).T


def mask_bias(plan, reach, bias_ref):
    n = plan.local
    key = lax.broadcasted_iota(jnp.int32, (n, n), 0)
    query = lax.broadcasted_iota(jnp.int32, (n, n), 1)
    for k in range(plan.grp):
        offset = query - key + k * n
        seen = (offset >= 0) & (offset <= reach)
        bias = jnp.where(seen, 0.0, NEGATIVE).astype(F32)
        bias_ref[k * n : (k + 1) * n, :] = jnp.concatenate([bias, bias], axis=1)


def each_slice(plan, place, slice_id, mine, part, store):
    for c, source in enumerate((mine, part)):
        for o in range(plan.half):
            for k in range(1, plan.grp):
                row = (o * (plan.grp - 1) + k - 1) * SR
                store(xor(place, k), xor(slice_id, 2 * o + c), source[row : row + SR, :])


def pack_a_kernel(plan, ids, wq, wk, wv, wo, gain1, gain2, out_ref):
    start = aligned(ids[1] * SR)
    for i, w in enumerate((wq, wk, wv, wo)):
        out_ref[:, i * D : (i + 1) * D] = w[pl.ds(start, SR), :]
    out_ref[:, 4 * D :] = jnp.zeros((SR, 128), BF16)
    out_ref[0:1, 4 * D : 4 * D + plan.rows] = gain1[...]
    out_ref[1:2, 4 * D : 4 * D + plan.rows] = gain2[...]


def pack_b_kernel(plan, ids, gate_t, up_t, down, own_ref, slab_ref):
    for i, w in enumerate((gate_t, up_t)):
        for z in range(plan.grp):
            rows = w[z * plan.down : (z + 1) * plan.down, :].astype(F32)
            gap = jnp.zeros((plan.down_pad - plan.down, plan.rows), F32)
            at = i * plan.ffp + z * plan.down_pad
            block = jnp.concatenate([rows, gap], axis=0).T
            own_ref[:, at : at + plan.down_pad] = block.astype(BF16)
    for s in range(plan.slices):
        for i in range(plan.pieces):
            at = (s * plan.pieces + i) * SR
            have = max(0, min(SR, plan.down - at))
            rows = []
            if have:
                rows.append(down[at : at + have, :])
            if have < SR:
                rows.append(jnp.zeros((SR - have, D), BF16))
            cols = slice(2 * plan.ffp + i * D, 2 * plan.ffp + (i + 1) * D)
            own_ref[s * SR : (s + 1) * SR, cols] = (
                jnp.concatenate(rows, axis=0) if len(rows) > 1 else rows[0]
            )
    slab_ref[...] = own_ref[pl.ds(aligned(ids[1] * SR), SR), :]


def gather_slices(plan, slice_id, mine, part, target):
    for c, source in enumerate((mine, part)):
        for o in range(plan.half):
            s = xor(slice_id, 2 * o + c)
            target[pl.ds(aligned(s * SR), SR), :] = source[o * SR : (o + 1) * SR, :]


def finish_a_kernel(plan, ids, mine, part, *refs):
    scratch = refs[-1]
    gather_slices(plan, ids[1], mine, part, scratch)
    for i in range(4):
        refs[i][...] = scratch[:, i * D : (i + 1) * D].astype(F32)
    norms = scratch[0:SR, 4 * D : 4 * D + plan.rows].astype(F32)
    refs[4][...] = norms[0:1, :]
    refs[5][...] = norms[1:2, :]


def finish_b_kernel(plan, ids, mine, part, gate_ref, up_ref, down_ref, scratch):
    gather_slices(plan, ids[1], mine, part, scratch)
    for i, ref in enumerate((gate_ref, up_ref)):
        for z in range(plan.grp):
            at = i * plan.ffp + z * plan.down_pad
            block = scratch[:, at : at + plan.down_pad].astype(F32).T
            ref[z * plan.down : (z + 1) * plan.down, :] = block[: plan.down, :]
    for s in range(plan.slices):
        for i in range(plan.pieces):
            at = (s * plan.pieces + i) * SR
            have = max(0, min(SR, plan.down - at))
            if have:
                cols = slice(2 * plan.ffp + i * D, 2 * plan.ffp + (i + 1) * D)
                rows = scratch[s * SR : (s + 1) * SR, cols].astype(F32)
                down_ref[at : at + have, :] = rows[:have, :]


def attend_kernel(plan, ids, *refs):
    g = plan.grp
    parts = refs[:g]
    own = refs[g : g + 4]
    mine, part, gain, cosine, sines, reach = refs[g + 4 : g + 10]
    attn_ref, q_ref, k_ref, v_ref, n1_ref, lse_ref, wa_ref = refs[g + 10 : g + 17]
    bias_ref, = refs[g + 17 :]
    n = plan.local
    place, slice_id = ids[0], ids[1]
    for i in range(4):
        wa_ref[pl.ds(aligned(place * plan.rows), plan.rows), i * D : (i + 1) * D] = own[i][...]

    def store(z, s, rows):
        wa_ref[pl.ds(aligned(z * plan.rows + s * SR), SR), :] = rows[:, : 4 * D]

    each_slice(plan, place, slice_id, mine, part, store)
    mask_bias(plan, reach[...], bias_ref)
    gains = gain[...]
    for k in range(g):
        x = parts[k][...].astype(F32)
        unit = x * lax.rsqrt(jnp.mean(x * x, axis=1, keepdims=True) + EPSILON)
        n1 = (unit * gains).astype(BF16)
        rows = slice(k * n, (k + 1) * n)
        n1_ref[rows, :] = n1
        cos_k, sin_k = cosine[rows, :], sines[rows, :]
        k_ref[rows, :] = rotate(mm(n1, wa_ref[:, D : 2 * D]), cos_k, sin_k).astype(BF16)
        v_ref[rows, :] = mm(n1, wa_ref[:, 2 * D : 3 * D]).astype(BF16)
        if k == 0:
            q_ref[...] = rotate(mm(n1, wa_ref[:, :D]), cos_k, sin_k).astype(BF16) * BF16(
                HD**-0.5
            )

    def pair(i, carry):
        lanes = pl.ds(pl.multiple_of(i * PAIR, PAIR), PAIR)
        score = against(k_ref[:, lanes], two_heads(q_ref[:, lanes])) + bias_ref[...]
        peak = jnp.max(score, axis=0, keepdims=True)
        exponent = jnp.exp(score - peak)
        total = jnp.sum(exponent, axis=0, keepdims=True)
        out = rows_of(v_ref[:, lanes], exponent.astype(BF16)) / total
        attn_ref[:, lanes] = one_pair(out)
        lse_ref[i] = peak + jnp.log(total)
        return carry

    lax.fori_loop(0, H // 2, pair, 0)


def mlp_kernel(plan, ids, *refs):
    attn, x0, wa, gain, cot, own, mine, part = refs[:8]
    out_ref, dx1_ref, dout_ref, dattn_ref, n2_ref, hid_ref, dg_ref, dup_ref, attn_ref, norm_ref = refs[8:18]
    wgu_ref, wd_ref = refs[18:]
    ffp = plan.ffp
    place, slice_id = ids[0], ids[1]

    def store(z, s, rows):
        wgu_ref[pl.ds(aligned(z * plan.rows + s * SR), SR), :] = rows[:, : 2 * ffp]
        for i in range(plan.pieces):
            at = z * plan.down_pad + (s * plan.pieces + i) * SR
            wd_ref[pl.ds(aligned(at), SR), :] = rows[:, 2 * ffp + i * D : 2 * ffp + (i + 1) * D]

    for s in range(plan.slices):
        store(place, s, own[s * SR : (s + 1) * SR, :])
    each_slice(plan, place, slice_id, mine, part, store)

    attn_low = attn[...].astype(BF16)
    attn_ref[...] = attn_low
    x1 = x0[...].astype(F32) + mm(attn_low, wa[:, 3 * D : 4 * D])
    scale = lax.rsqrt(jnp.mean(x1 * x1, axis=1, keepdims=True) + EPSILON)
    unit = x1 * scale
    gains = gain[...]
    n2 = (unit * gains).astype(BF16)
    n2_ref[...] = n2
    c = cot[...]
    out = x1
    dn2 = jnp.zeros_like(x1)
    step = 512 if ffp % 512 == 0 else ffp
    for f in range(0, ffp, step):
        cols = slice(f, f + step)
        up_cols = slice(ffp + f, ffp + f + step)
        gate = mm(n2, wgu_ref[:, cols])
        up = mm(n2, wgu_ref[:, up_cols])
        dhid = against(c, wd_ref[cols, :])
        sig = 1.0 / (1.0 + jnp.exp(-gate))
        silu = gate * sig
        hid = (silu * up).astype(BF16)
        dup = (dhid * silu).astype(BF16)
        dg = (dhid * up * (sig * (1.0 + gate * (1.0 - sig)))).astype(BF16)
        hid_ref[:, cols] = hid
        dg_ref[:, cols] = dg
        dup_ref[:, cols] = dup
        out = out + mm(hid, wd_ref[cols, :])
        dn2 = dn2 + against(dg, wgu_ref[:, cols]) + against(dup, wgu_ref[:, up_cols])
    out_ref[...] = out.astype(BF16)
    norm_ref[...] = jnp.sum(dn2 * unit, axis=0, keepdims=True)
    e2 = dn2 * gains
    dx1 = c.astype(F32) + scale * (e2 - unit * jnp.mean(e2 * unit, axis=1, keepdims=True))
    dx1_ref[...] = dx1
    dout = dx1.astype(BF16)
    dout_ref[...] = dout
    dattn_ref[...] = against(dout, wa[:, 3 * D : 4 * D]).astype(BF16)


def spread(plan, place, slice_id, keep, send, copy):
    for c, target in enumerate((keep, send)):
        for o in range(plan.half):
            for k in range(plan.grp):
                copy(xor(place, k), xor(slice_id, 2 * o + c), target, o, k)


def mlp_grads_kernel(plan, ids, n2, hid, dg, dup, cot, keep, send, gu_ref, d_ref):
    ffp = plan.ffp
    n2_t = n2[...].T
    gu_ref[:, :ffp] = mm(n2_t, dg[...]).astype(BF16)
    gu_ref[:, ffp:] = mm(n2_t, dup[...]).astype(BF16)
    d_ref[...] = rows_of(hid[...], cot[...]).astype(BF16)

    def copy(z, s, target, o, k):
        target[o, k, :, : 2 * ffp] = gu_ref[pl.ds(aligned(z * plan.rows + s * SR), SR), :]
        for i in range(plan.pieces):
            at = z * plan.down_pad + (s * plan.pieces + i) * SR
            target[o, k, :, 2 * ffp + i * D : 2 * ffp + (i + 1) * D] = d_ref[
                pl.ds(aligned(at), SR), :
            ]

    spread(plan, ids[0], ids[1], keep, send, copy)


def attend_back_kernel(plan, first, count, q, k_in, v_in, attn, dattn, lse, cosine, sines, reach, dq_ref, dk_ref, dv_ref, bias_ref, dq_scr, dk_scr):
    mask_bias(plan, reach[...], bias_ref)

    def pair(i, carry):
        lanes = pl.ds(pl.multiple_of((first + i) * PAIR, PAIR), PAIR)
        outs = pl.ds(pl.multiple_of(i * PAIR, PAIR), PAIR)
        q2 = two_heads(q[:, lanes])
        da = dattn[:, lanes]
        da2 = two_heads(da)
        prod = two_heads(da.astype(F32) * attn[:, lanes])
        ones = jnp.ones((8, PAIR), F32)
        mean = lax.dot_general(
            ones, prod, (((1,), (1,)), ((), ())), precision=lax.Precision.HIGHEST,
            preferred_element_type=F32,
        )[0:1, :]
        keys = k_in[:, lanes]
        values = v_in[:, lanes]
        prob = jnp.exp(against(keys, q2) + (bias_ref[...] - lse[first + i]))
        dprob = against(values, da2)
        dscore = (prob * (dprob - mean)).astype(BF16)
        dv_ref[:, outs] = mm(prob.astype(BF16), da2).astype(BF16)
        dk_scr[:, outs] = mm(dscore, q2)
        dq_scr[:, outs] = one_pair(rows_of(keys, dscore)) * (HD**-0.5)
        return carry

    lax.fori_loop(0, count, pair, 0)
    n = plan.local
    dq_ref[...] = rotate_back(dq_scr[...], cosine[:n, :], sines[:n, :]).astype(BF16)
    for k in range(plan.grp):
        rows = slice(k * n, (k + 1) * n)
        dk_ref[rows, :] = rotate_back(dk_scr[rows, :], cosine[rows, :], sines[rows, :]).astype(BF16)


def input_kernel(plan, halves, *refs):
    g = plan.grp
    parts = refs[:g]
    back = refs[g : g + 3 * halves]
    wa, own_ref, norm_ref = refs[g + 3 * halves : g + 3 * halves + 3]
    sends = refs[g + 3 * halves + 3 :]
    n = plan.local
    wide = D // halves
    norm = jnp.zeros((1, D), F32)
    for k in reversed(range(g)):
        rows = slice(k * n, (k + 1) * n)
        dn1 = None
        for h in range(halves):
            dq, dk, dv = back[3 * h : 3 * h + 3]
            at = h * wide
            term = against(dk[rows, :], wa[:, D + at : D + at + wide])
            term = term + against(dv[rows, :], wa[:, 2 * D + at : 2 * D + at + wide])
            if k == 0:
                term = term + against(dq[...], wa[:, at : at + wide])
            dn1 = term if dn1 is None else dn1 + term
        if k == 0:
            own_ref[...] = dn1
        else:
            sends[k - 1][...] = dn1.astype(BF16)
        x = parts[k][...].astype(F32)
        unit = x * lax.rsqrt(jnp.mean(x * x, axis=1, keepdims=True) + EPSILON)
        norm = norm + jnp.sum(dn1 * unit, axis=0, keepdims=True)
    norm_ref[...] = norm


def attend_grads_kernel(plan, halves, ids, n1, *refs):
    back = refs[: 3 * halves]
    attn, dout, norms, keep, send, ga_ref = refs[3 * halves :]
    n1_t = n1[...].T
    wide = D // halves
    for h in range(halves):
        dq, dk, dv = back[3 * h : 3 * h + 3]
        at = h * wide
        ga_ref[:, at : at + wide] = mm(n1_t[:, : plan.local], dq[...]).astype(BF16)
        ga_ref[:, D + at : D + at + wide] = mm(n1_t, dk[...]).astype(BF16)
        ga_ref[:, 2 * D + at : 2 * D + at + wide] = mm(n1_t, dv[...]).astype(BF16)
    ga_ref[:, 3 * D :] = rows_of(attn[...], dout[...]).astype(BF16)

    def copy(z, s, target, o, k):
        target[o, k, :, : 4 * D] = ga_ref[pl.ds(aligned(z * plan.rows + s * SR), SR), :]
        flag = (s == 0).astype(F32)
        target[o, k, :, 4 * D :] = (norms[z] * flag).astype(BF16)

    spread(plan, ids[0], ids[1], keep, send, copy)


def finish_kernel(plan, ids, mine, part, out_ref):
    for c, source in enumerate((mine, part)):
        for o in range(plan.half):
            s = xor(ids[1], 2 * o + c)
            out_ref[pl.ds(aligned(s * SR), SR), :] = source[o * SR : (o + 1) * SR, :].astype(F32)


def residual_kernel(plan, *refs):
    own, x0, dx1, gain = refs[:4]
    received = refs[4:-1]
    out_ref = refs[-1]
    dn1 = own[...]
    for r in received:
        dn1 = dn1 + r[...].astype(F32)
    x = x0[...].astype(F32)
    scale = lax.rsqrt(jnp.mean(x * x, axis=1, keepdims=True) + EPSILON)
    unit = x * scale
    e1 = dn1 * gain[...]
    out_ref[...] = dx1[...] + scale * (e1 - unit * jnp.mean(e1 * unit, axis=1, keepdims=True))


def fetch_line(plan, slab):
    return jnp.concatenate([swap("grp", k, plan.grp, slab) for k in range(1, plan.grp)], axis=0)


def fetch_plane(plan, block):
    return jnp.concatenate(
        [block] + [swap("rep", 2 * o, plan.rep, block) for o in range(1, plan.half)], axis=0
    )


def fetch_core(plan, mine):
    return swap("rep", 1, plan.rep, mine)


def tie(value, *others):
    return lax.optimization_barrier((value, *others))[0]


def add(*values):
    total = values[0].astype(F32)
    for v in values[1:]:
        total = total + v.astype(F32)
    return total.astype(BF16)


def combine_cores(plan, keep, send):
    got = swap("rep", 1, plan.rep, send)
    return [add(keep[o], got[o]) for o in range(plan.half)]


def combine_plane(plan, terms, after=()):
    got = [swap("rep", 2 * o, plan.rep, terms[o]) for o in range(1, plan.half)]
    return add(tie(terms[0], *after), *got)


def combine_line(plan, total):
    final = add(total[0], *[swap("grp", k, plan.grp, total[k]) for k in range(1, plan.grp)])
    bit = plan.slices
    while bit < plan.rep:
        final = add(final, swap("rep", bit, plan.rep, final))
        bit *= 2
    mine = fetch_plane(plan, final)
    return mine, fetch_core(plan, mine)


def pad_columns(plan, weight):
    rows = weight.shape[0]
    blocks = weight.reshape(rows, plan.grp, plan.down)
    blocks = jnp.pad(blocks, ((0, 0), (0, 0), (0, plan.down_pad - plan.down)))
    return blocks.reshape(rows, plan.ffp)


def drop_columns(plan, grad):
    return jnp.concatenate(
        [grad[:, z * plan.down_pad : z * plan.down_pad + plan.down] for z in range(plan.grp)],
        axis=1,
    )


def pack_b(plan, ids, w_gate, w_up, w_down):
    if plan.down % 8 == 0:
        return call(
            functools.partial(pack_b_kernel, plan),
            [sds((plan.rows, plan.wide_b), BF16), sds((SR, plan.wide_b), BF16)],
            "pack_b",
            (ids, w_gate.T, w_up.T, w_down),
            moved=3 * 10**6,
        )
    rows = jnp.pad(w_down, ((0, plan.down_pad - plan.down), (0, 0)))
    rows = rows.reshape(plan.slices, plan.pieces, SR, D).transpose(0, 2, 1, 3)
    own = jnp.concatenate(
        [
            pad_columns(plan, w_gate),
            pad_columns(plan, w_up),
            rows.reshape(plan.rows, plan.pieces * D),
        ],
        axis=1,
    )
    return own, lax.dynamic_slice(own, (ids[1] * SR, 0), (SR, plan.wide_b))


def finish_b(plan, ids, final):
    if plan.down % 8 == 0:
        tall = sds((FF, plan.rows), F32)
        gate, up, down = call(
            functools.partial(finish_b_kernel, plan),
            [tall, tall, sds((plan.down, D), F32)],
            "finish_b",
            (ids, *final),
            [pltpu.VMEM((plan.rows, plan.wide_b), BF16)],
            moved=3 * 10**6,
        )
        return gate.T, up.T, down
    (grads,) = call(
        functools.partial(finish_kernel, plan),
        [sds((plan.rows, plan.wide_b), F32)],
        "finish_b",
        (ids, *final),
        moved=4 * 10**6,
    )
    ffp = plan.ffp
    down = grads[:, 2 * ffp :].reshape(plan.slices, SR, plan.pieces, D).transpose(0, 2, 1, 3)
    return (
        drop_columns(plan, grads[:, :ffp]),
        drop_columns(plan, grads[:, ffp : 2 * ffp]),
        down.reshape(plan.down_pad, D)[: plan.down],
    )


def body(plan, tokens, segments, positions, norm1_gain, w_query, w_key, w_value, w_out, norm2_gain, w_gate, w_up, w_down, cotangent):
    g, n = plan.grp, plan.local
    place = lax.axis_index("grp").astype(jnp.int32)
    slice_id = (lax.axis_index("rep") % plan.slices).astype(jnp.int32)
    ids = jnp.stack([place, slice_id])
    x0 = tokens.reshape(n, D)
    cot = cotangent.reshape(n, D)
    reach = jnp.where(segments != 0, positions, 0).reshape(1, n)
    table_cos, table_sin = rotary_tables(plan)
    cosine, sines = jnp.asarray(table_cos), jnp.asarray(table_sin)

    own_a = (w_query, w_key, w_value, w_out)
    gains = jnp.stack([norm1_gain, norm2_gain])
    (slab_a,) = call(
        functools.partial(pack_a_kernel, plan),
        [sds((SR, plan.wide_a), BF16)],
        "pack_a",
        (ids, *own_a, norm1_gain.reshape(1, -1), norm2_gain.reshape(1, -1)),
        moved=10**6,
    )
    own_b, slab_b = pack_b(plan, ids, w_gate, w_up, w_down)

    block_a = fetch_line(plan, slab_a)
    block_b = fetch_line(plan, slab_b)
    parts = [x0]
    for _ in range(1, g):
        parts.append(shift(1, g, parts[-1]))
    mine_a = fetch_plane(plan, block_a)
    mine_b = fetch_plane(plan, tie(block_b, mine_a))
    part_a = fetch_core(plan, mine_a)
    part_b = fetch_core(plan, mine_b)

    tiles = jnp.stack(
        [gains] + [mine_a[k * SR : k * SR + 2, 4 * D : 4 * D + plan.rows] for k in range(g - 1)]
    )
    order = jnp.bitwise_xor(jnp.arange(g, dtype=jnp.int32), place)
    chosen = sum(
        jnp.where((order == k)[:, None, None], tiles[k][None], 0).astype(F32) for k in range(g)
    )
    gain1 = chosen[:, 0].reshape(1, D)
    gain2 = chosen[:, 1].reshape(1, D)

    full = plan.full
    attn, q, k_all, v_all, n1, lse, wa = call(
        functools.partial(attend_kernel, plan),
        [
            sds((n, D), F32),
            sds((n, D), BF16),
            sds((full, D), BF16),
            sds((full, D), BF16),
            sds((full, D), BF16),
            sds((H // 2, 1, 2 * n), F32),
            sds((D, 4 * D), BF16),
        ],
        "attend",
        (ids, *parts, *own_a, mine_a, part_a, gain1, cosine, sines, reach),
        [pltpu.VMEM((full, 2 * n), F32)],
        flops=4 * 10**9,
        moved=8 * 10**6,
    )

    ffp = plan.ffp
    output, dx1, dout, dattn, n2, hid, dg, dup, attn_low, norm2 = call(
        functools.partial(mlp_kernel, plan),
        [
            sds((n, D), BF16),
            sds((n, D), F32),
            sds((n, D), BF16),
            sds((n, D), BF16),
            sds((n, D), BF16),
            sds((n, ffp), BF16),
            sds((n, ffp), BF16),
            sds((n, ffp), BF16),
            sds((n, D), BF16),
            sds((1, D), F32),
        ],
        "mlp",
        (ids, attn, x0, wa, gain2, cot, own_b, mine_b, part_b),
        [pltpu.VMEM((D, 2 * ffp), BF16), pltpu.VMEM((ffp, D), BF16)],
        flops=4 * 10**9,
        moved=12 * 10**6,
    )

    slabs_b = sds((plan.half, g, SR, plan.wide_b), BF16)
    keep_b, send_b = call(
        functools.partial(mlp_grads_kernel, plan),
        [slabs_b, slabs_b],
        "mlp_grads",
        (ids, n2, hid, dg, dup, cot),
        [pltpu.VMEM((D, 2 * ffp), BF16), pltpu.VMEM((ffp, D), BF16)],
        flops=2 * 10**9,
        moved=8 * 10**6,
    )
    halves = 2
    count = H // 2 // halves
    wide = D // halves

    def attend_back(first, dattn):
        return call(
            functools.partial(attend_back_kernel, plan, first, count),
            [sds((n, wide), BF16), sds((full, wide), BF16), sds((full, wide), BF16)],
            "attend_back",
            (q, k_all, v_all, attn, dattn, lse, cosine, sines, reach),
            [
                pltpu.VMEM((full, 2 * n), F32),
                pltpu.VMEM((n, wide), F32),
                pltpu.VMEM((full, wide), F32),
            ],
            flops=4 * 10**9,
            moved=8 * 10**6,
        )

    back = list(attend_back(0, tie(dattn, keep_b)))
    terms_b = combine_cores(plan, keep_b, send_b)
    back += attend_back(count, tie(dattn, *terms_b, back[0]))
    own, norm1, *sends = call(
        functools.partial(input_kernel, plan, halves),
        [sds((n, D), F32), sds((1, D), F32)] + [sds((n, D), BF16)] * (g - 1),
        "dn1",
        (*parts, *back, wa),
        flops=2 * 10**9,
        moved=4 * 10**6,
    )
    moving = sends[g - 2]
    for k in reversed(range(1, g)):
        moving = shift(-1, g, moving)
        if k > 1:
            moving = add(moving, sends[k - 2])

    norms = jnp.concatenate([norm1, norm2], axis=0).reshape(2, g, plan.rows).transpose(1, 0, 2)
    norms = jnp.pad(norms, ((0, 0), (0, SR - 2), (0, 128 - plan.rows)))
    slabs_a = sds((plan.half, g, SR, plan.wide_a), BF16)
    keep_a, send_a = call(
        functools.partial(attend_grads_kernel, plan, halves),
        [slabs_a, slabs_a],
        "attend_grads",
        (ids, n1, *back, attn_low, dout, norms),
        [pltpu.VMEM((D, 4 * D), BF16)],
        flops=2 * 10**9,
        moved=8 * 10**6,
    )

    total_b = combine_plane(plan, terms_b, (own,))
    final_b = combine_line(plan, total_b)
    total_a = combine_plane(plan, combine_cores(plan, keep_a, send_a))
    (input_grad,) = call(
        functools.partial(residual_kernel, plan),
        [sds((n, D), F32)],
        "residual",
        (own, x0, dx1, gain1, moving),
        moved=4 * 10**6,
    )
    final_a = combine_line(plan, tie(total_a, input_grad))
    gate, up, down = finish_b(plan, ids, final_b)
    shard = sds((plan.rows, D), F32)
    line = sds((1, plan.rows), F32)
    grads_a = call(
        functools.partial(finish_a_kernel, plan),
        [shard, shard, shard, shard, line, line],
        "finish_a",
        (ids, *final_a),
        [pltpu.VMEM((plan.rows, plan.wide_a), BF16)],
        moved=2 * 10**6,
    )
    return (
        output.reshape(tokens.shape),
        input_grad.reshape(tokens.shape),
        grads_a[4].reshape(plan.rows),
        *grads_a[:4],
        grads_a[5].reshape(plan.rows),
        gate,
        up,
        down,
    )


def solution(mesh):
    wide, line, pair = P("grp", None), P("grp"), P("rep", "grp")
    three = P("rep", "grp", None)

    def run(tokens, *rest):
        plan = Plan(mesh, tokens.shape)
        return jax.shard_map(
            functools.partial(body, plan),
            mesh=mesh,
            in_specs=(three, pair, pair, line, wide, wide, wide, wide, line, wide, wide, wide, three),
            out_specs=(three, three, line, wide, wide, wide, wide, line, wide, wide, wide),
            check_vma=False,
        )(tokens, *rest)

    return run
```

```python
import functools

import jax
import jax.numpy as jnp
import numpy as np
from jax import lax
from jax.experimental import pallas as pl
from jax.experimental.pallas import tpu as pltpu
from jax.sharding import PartitionSpec as P

D = 512
H = 8
HD = 64
FF = 1376
EPSILON = 1e-05
NEGATIVE = -1e30
SR = 16
PAIR = 2 * HD
F32 = jnp.float32
BF16 = jnp.bfloat16
VMEM = pl.BlockSpec(memory_space=pltpu.VMEM)
SMEM = pl.BlockSpec(memory_space=pltpu.SMEM)
PARAMS = pltpu.CompilerParams(vmem_limit_bytes=56 * 1024 * 1024)


class Plan:
    def __init__(self, mesh, tokens_shape):
        self.rep = mesh.shape["rep"]
        self.grp = mesh.shape["grp"]
        self.rows = D // self.grp
        self.slices = min(self.rep, self.rows // SR)
        self.half = self.slices // 2
        self.down = FF // self.grp
        self.pieces = -(-self.down // (self.slices * SR))
        self.down_pad = self.pieces * self.slices * SR
        self.ffp = self.down_pad * self.grp
        self.local = tokens_shape[1] // self.grp
        self.full = self.local * self.grp
        self.wide_a = 3 * D + 128
        self.tall_b = 2 * self.ffp + D
        self.wide_b = self.tall_b + self.pieces * D
        self.line = [bit for bit in (1, 2, 4, 8, 16) if bit < self.grp]
        self.plane = [bit for bit in (1, 2, 4, 8, 16) if bit < self.half]
        order = [0]
        for bit in reversed(self.line):
            order += [k ^ bit for k in order]
        self.order = order[1:]


def dot(left, right, dims):
    return lax.dot_general(left, right, ((dims[0], dims[1]), ((), ())), preferred_element_type=F32)


def mm(left, right):
    return dot(left, right, ((1,), (0,)))


def against(left, right):
    return dot(left, right, ((1,), (1,)))


def rows_of(left, right):
    return dot(left, right, ((0,), (0,)))


def call(body, outs, name, args, scratch=(), us=0):
    specs = [SMEM if a.dtype == jnp.int32 and a.ndim == 1 else VMEM for a in args]
    return pl.pallas_call(
        body,
        out_shape=outs,
        in_specs=specs,
        out_specs=[VMEM] * len(outs),
        scratch_shapes=scratch,
        compiler_params=PARAMS,
        cost_estimate=pl.CostEstimate(flops=us * 10**9, bytes_accessed=0, transcendentals=0),
        name=name,
    )(*args)


def sds(shape, dtype):
    return jax.ShapeDtypeStruct(shape, dtype)


def swap(axis, k, size, value):
    return lax.ppermute(value, axis, [(i, i ^ k) for i in range(size)])


def shift(k, size, value):
    return lax.ppermute(value, "grp", [(i, i + k) for i in range(size) if 0 <= i + k < size])


def xor(a, b):
    return lax.bitwise_xor(a, jnp.int32(b)) if isinstance(b, int) else lax.bitwise_xor(a, b)


def aligned(index):
    return pl.multiple_of(index, SR)


def rotary_tables(plan):
    halves = HD // 2
    frequency = 10000.0 ** (-2.0 * np.arange(halves) / HD)
    place = np.concatenate([np.arange(plan.local) - k * plan.local for k in range(plan.grp)])
    angle = place[:, None] * frequency[None, :]
    cosine = np.tile(np.cos(angle), (1, 4)).astype(np.float32)
    sines = np.tile(np.concatenate([-np.sin(angle), np.sin(angle)], axis=1), (1, 2))
    return cosine, sines.astype(np.float32)


def swap_halves(value):
    wide = value.shape[1]
    lane = lax.broadcasted_iota(jnp.int32, value.shape, 1)
    first = (lane % HD) < HD // 2
    return jnp.where(
        first, pltpu.roll(value, wide - HD // 2, 1), pltpu.roll(value, HD // 2, 1)
    )


def tile_heads(table, wide):
    return jnp.concatenate([table] * (wide // table.shape[1]), axis=1)


def rotate(value, cosine, sines):
    wide = value.shape[1]
    return value * tile_heads(cosine, wide) + swap_halves(value) * tile_heads(sines, wide)


def rotate_back(value, cosine, sines):
    wide = value.shape[1]
    return value * tile_heads(cosine, wide) - swap_halves(value) * tile_heads(sines, wide)


def two_heads(value):
    lane = lax.broadcasted_iota(jnp.int32, value.shape, 1)
    zero = jnp.zeros_like(value)
    return jnp.concatenate(
        [jnp.where(lane < HD, value, zero), jnp.where(lane < HD, zero, value)], axis=0
    )


def one_pair(value):
    count = value.shape[1] // 2
    return jnp.concatenate([value[:HD, :count], value[HD:, count:]], axis=0).T


def mask_bias(plan, reach, bias_ref):
    n = plan.local
    key = lax.broadcasted_iota(jnp.int32, (n, n), 0)
    query = lax.broadcasted_iota(jnp.int32, (n, n), 1)
    for k in range(plan.grp):
        offset = query - key + k * n
        seen = (offset >= 0) & (offset <= reach)
        bias = jnp.where(seen, 0.0, NEGATIVE).astype(F32)
        bias_ref[k * n : (k + 1) * n, :] = jnp.concatenate([bias, bias], axis=1)


def each_slice(plan, place, slice_id, mine, part, store):
    for c, source in enumerate((mine, part)):
        for o in range(plan.half):
            for i, k in enumerate(plan.order):
                row = (o * (plan.grp - 1) + i) * SR
                rows = [ref[row : row + SR, :] for ref in source]
                rows = jnp.concatenate(rows, axis=1) if len(rows) > 1 else rows[0]
                store(xor(place, k), xor(slice_id, 2 * o + c), rows)


def pack_a_kernel(plan, ids, wq, wk, wv, gain1, gain2, out_ref):
    start = aligned(ids[1] * SR)
    for i, w in enumerate((wq, wk, wv)):
        out_ref[:, i * D : (i + 1) * D] = w[pl.ds(start, SR), :]
    out_ref[:, 3 * D :] = jnp.zeros((SR, 128), BF16)
    out_ref[0:1, 3 * D : 3 * D + plan.rows] = gain1[...]
    out_ref[1:2, 3 * D : 3 * D + plan.rows] = gain2[...]


def pack_b_kernel(plan, ids, gate_t, up_t, out, down, own_ref, slab_ref):
    for i, w in enumerate((gate_t, up_t)):
        for z in range(plan.grp):
            rows = w[z * plan.down : (z + 1) * plan.down, :].astype(F32)
            gap = jnp.zeros((plan.down_pad - plan.down, plan.rows), F32)
            at = i * plan.ffp + z * plan.down_pad
            block = jnp.concatenate([rows, gap], axis=0).T
            own_ref[:, at : at + plan.down_pad] = block.astype(BF16)
    own_ref[:, 2 * plan.ffp : plan.tall_b] = out[...]
    for s in range(plan.slices):
        for i in range(plan.pieces):
            at = (s * plan.pieces + i) * SR
            have = max(0, min(SR, plan.down - at))
            rows = []
            if have:
                rows.append(down[at : at + have, :])
            if have < SR:
                rows.append(jnp.zeros((SR - have, D), BF16))
            cols = slice(plan.tall_b + i * D, plan.tall_b + (i + 1) * D)
            own_ref[s * SR : (s + 1) * SR, cols] = (
                jnp.concatenate(rows, axis=0) if len(rows) > 1 else rows[0]
            )
    slab_ref[...] = own_ref[pl.ds(aligned(ids[1] * SR), SR), :]


def gather_slices(plan, slice_id, mine, part, target):
    for c, source in enumerate((mine, part)):
        for o in range(plan.half):
            s = xor(slice_id, 2 * o + c)
            target[pl.ds(aligned(s * SR), SR), :] = source[o * SR : (o + 1) * SR, :]


def row_sums(value):
    ones = jnp.ones((8, value.shape[1]), F32)
    return lax.dot_general(
        ones, value, (((1,), (1,)), ((), ())), precision=lax.Precision.HIGHEST,
        preferred_element_type=F32,
    )[0:1, :]


def finish_a_kernel(plan, ids, mine, part, wq, wk, wv, gain, *refs):
    scratch = refs[-1]
    gather_slices(plan, ids[1], mine, part, scratch)
    dots = jnp.zeros((plan.rows, D), F32)
    for i, w in enumerate((wq, wk, wv)):
        grad = scratch[:, i * D : (i + 1) * D].astype(F32)
        refs[i][...] = grad
        dots = dots + grad * w[...].astype(F32)
    refs[3][...] = row_sums(dots) / gain[...].astype(F32)


def finish_b_kernel(plan, ids, mine, part, gate_t, up_t, gain, gate_ref, up_ref, down_ref, out_ref, norm_ref, scratch):
    gather_slices(plan, ids[1], mine, part, scratch)
    norm = jnp.zeros((1, plan.rows), F32)
    for i, (ref, weight) in enumerate(((gate_ref, gate_t), (up_ref, up_t))):
        for z in range(plan.grp):
            at = i * plan.ffp + z * plan.down_pad
            block = scratch[:, at : at + plan.down_pad].astype(F32).T[: plan.down, :]
            rows = slice(z * plan.down, (z + 1) * plan.down)
            ref[rows, :] = block
            norm = norm + jnp.sum(block * weight[rows, :].astype(F32), axis=0, keepdims=True)
    norm_ref[...] = norm / gain[...].astype(F32)
    out_ref[...] = scratch[:, 2 * plan.ffp : plan.tall_b].astype(F32)
    for s in range(plan.slices):
        for i in range(plan.pieces):
            at = (s * plan.pieces + i) * SR
            have = max(0, min(SR, plan.down - at))
            if have:
                cols = slice(plan.tall_b + i * D, plan.tall_b + (i + 1) * D)
                rows = scratch[s * SR : (s + 1) * SR, cols].astype(F32)
                down_ref[at : at + have, :] = rows[:have, :]


def attend_kernel(plan, ids, *refs):
    g = plan.grp
    parts = refs[:g]
    own = refs[g : g + 3]
    mine, part, gain, cosine, sines, reach = refs[g + 3 : g + 9]
    attn_ref, q_ref, k_ref, v_ref, n1_ref, lse_ref, wa_ref = refs[g + 9 : g + 16]
    bias_ref, = refs[g + 16 :]
    n = plan.local
    place, slice_id = ids[0], ids[1]
    for i in range(3):
        wa_ref[pl.ds(aligned(place * plan.rows), plan.rows), i * D : (i + 1) * D] = own[i][...]

    def store(z, s, rows):
        wa_ref[pl.ds(aligned(z * plan.rows + s * SR), SR), :] = rows[:, : 3 * D]

    each_slice(plan, place, slice_id, [mine], [part], store)
    mask_bias(plan, reach[...], bias_ref)
    gains = gain[...]
    for k in range(g):
        x = parts[k][...].astype(F32)
        unit = x * lax.rsqrt(jnp.mean(x * x, axis=1, keepdims=True) + EPSILON)
        n1 = (unit * gains).astype(BF16)
        rows = slice(k * n, (k + 1) * n)
        n1_ref[rows, :] = n1
        cos_k, sin_k = cosine[rows, :], sines[rows, :]
        k_ref[rows, :] = rotate(mm(n1, wa_ref[:, D : 2 * D]), cos_k, sin_k).astype(BF16)
        v_ref[rows, :] = mm(n1, wa_ref[:, 2 * D : 3 * D]).astype(BF16)
        if k == 0:
            q_ref[...] = rotate(mm(n1, wa_ref[:, :D]), cos_k, sin_k).astype(BF16) * BF16(
                HD**-0.5
            )

    def pair(i, carry):
        lanes = pl.ds(pl.multiple_of(i * PAIR, PAIR), PAIR)
        score = against(k_ref[:, lanes], two_heads(q_ref[:, lanes])) + bias_ref[...]
        peak = jnp.max(score, axis=0, keepdims=True)
        exponent = jnp.exp(score - peak)
        total = jnp.sum(exponent, axis=0, keepdims=True)
        out = rows_of(v_ref[:, lanes], exponent.astype(BF16)) / total
        attn_ref[:, lanes] = one_pair(out)
        lse_ref[i] = peak + jnp.log(total)
        return carry

    lax.fori_loop(0, H // 2, pair, 0)


def mlp_kernel(plan, ids, *refs):
    attn, x0, gain, cot, own = refs[:5]
    mine, part = refs[5:7], refs[7:9]
    out_ref, dx1_ref, dout_ref, dattn_ref, n2_ref, hid_ref, dg_ref, dup_ref, attn_ref = refs[9:18]
    wgu_ref, wd_ref = refs[18:]
    ffp, tall = plan.ffp, plan.tall_b
    place, slice_id = ids[0], ids[1]

    def store(z, s, rows):
        wgu_ref[pl.ds(aligned(z * plan.rows + s * SR), SR), :] = rows[:, :tall]
        for i in range(plan.pieces):
            at = z * plan.down_pad + (s * plan.pieces + i) * SR
            wd_ref[pl.ds(aligned(at), SR), :] = rows[:, tall + i * D : tall + (i + 1) * D]

    for s in range(plan.slices):
        store(place, s, own[s * SR : (s + 1) * SR, :])
    each_slice(plan, place, slice_id, mine, part, store)

    attn_low = attn[...].astype(BF16)
    attn_ref[...] = attn_low
    x1 = x0[...].astype(F32) + mm(attn_low, wgu_ref[:, 2 * ffp :])
    scale = lax.rsqrt(jnp.mean(x1 * x1, axis=1, keepdims=True) + EPSILON)
    unit = x1 * scale
    gains = gain[...]
    n2 = (unit * gains).astype(BF16)
    n2_ref[...] = n2
    c = cot[...]
    out = x1
    dn2 = jnp.zeros_like(x1)
    step = 512 if ffp % 512 == 0 else ffp
    for f in range(0, ffp, step):
        cols = slice(f, f + step)
        up_cols = slice(ffp + f, ffp + f + step)
        gate = mm(n2, wgu_ref[:, cols])
        up = mm(n2, wgu_ref[:, up_cols])
        dhid = against(c, wd_ref[cols, :])
        sig = 1.0 / (1.0 + jnp.exp(-gate))
        silu = gate * sig
        hid = (silu * up).astype(BF16)
        dup = (dhid * silu).astype(BF16)
        dg = (dhid * up * (sig * (1.0 + gate * (1.0 - sig)))).astype(BF16)
        hid_ref[:, cols] = hid
        dg_ref[:, cols] = dg
        dup_ref[:, cols] = dup
        out = out + mm(hid, wd_ref[cols, :])
        dn2 = dn2 + against(dg, wgu_ref[:, cols]) + against(dup, wgu_ref[:, up_cols])
    out_ref[...] = out.astype(BF16)
    e2 = dn2 * gains
    dx1 = c.astype(F32) + scale * (e2 - unit * jnp.mean(e2 * unit, axis=1, keepdims=True))
    dx1_ref[...] = dx1
    dout = dx1.astype(BF16)
    dout_ref[...] = dout
    dattn_ref[...] = against(dout, wgu_ref[:, 2 * ffp :]).astype(BF16)


def spread(plan, place, slice_id, keep, send, copy):
    for c, target in enumerate((keep, send)):
        for o in range(plan.half):
            for k in range(plan.grp):
                copy(xor(place, k), xor(slice_id, 2 * o + c), target, o, k)


def mlp_grads_kernel(plan, ids, n2, hid, dg, dup, cot, attn, dout, keep, send, gu_ref, d_ref):
    ffp, tall = plan.ffp, plan.tall_b
    n2_t = n2[...].T
    gu_ref[:, :ffp] = mm(n2_t, dg[...]).astype(BF16)
    gu_ref[:, ffp : 2 * ffp] = mm(n2_t, dup[...]).astype(BF16)
    gu_ref[:, 2 * ffp :] = rows_of(attn[...], dout[...]).astype(BF16)
    d_ref[...] = rows_of(hid[...], cot[...]).astype(BF16)

    def copy(z, s, target, o, k):
        target[o, k, :, :tall] = gu_ref[pl.ds(aligned(z * plan.rows + s * SR), SR), :]
        for i in range(plan.pieces):
            at = z * plan.down_pad + (s * plan.pieces + i) * SR
            target[o, k, :, tall + i * D : tall + (i + 1) * D] = d_ref[pl.ds(aligned(at), SR), :]

    spread(plan, ids[0], ids[1], keep, send, copy)


def attend_back_kernel(plan, first, count, q, k_in, v_in, attn, dattn, lse, cosine, sines, reach, dq_ref, dk_ref, dv_ref, bias_ref, dq_scr, dk_scr):
    mask_bias(plan, reach[...], bias_ref)

    def pair(i, carry):
        lanes = pl.ds(pl.multiple_of((first + i) * PAIR, PAIR), PAIR)
        outs = pl.ds(pl.multiple_of(i * PAIR, PAIR), PAIR)
        q2 = two_heads(q[:, lanes])
        da = dattn[:, lanes]
        da2 = two_heads(da)
        prod = two_heads(da.astype(F32) * attn[:, lanes])
        ones = jnp.ones((8, PAIR), F32)
        mean = lax.dot_general(
            ones, prod, (((1,), (1,)), ((), ())), precision=lax.Precision.HIGHEST,
            preferred_element_type=F32,
        )[0:1, :]
        keys = k_in[:, lanes]
        values = v_in[:, lanes]
        prob = jnp.exp(against(keys, q2) + (bias_ref[...] - lse[first + i]))
        dprob = against(values, da2)
        dscore = (prob * (dprob - mean)).astype(BF16)
        dv_ref[:, outs] = mm(prob.astype(BF16), da2).astype(BF16)
        dk_scr[:, outs] = mm(dscore, q2)
        dq_scr[:, outs] = one_pair(rows_of(keys, dscore)) * (HD**-0.5)
        return carry

    lax.fori_loop(0, count, pair, 0)
    n = plan.local
    dq_ref[...] = rotate_back(dq_scr[...], cosine[:n, :], sines[:n, :]).astype(BF16)
    for k in range(plan.grp):
        rows = slice(k * n, (k + 1) * n)
        dk_ref[rows, :] = rotate_back(dk_scr[rows, :], cosine[rows, :], sines[rows, :]).astype(BF16)


def input_kernel(plan, halves, *refs):
    back = refs[: 3 * halves]
    wa, own_ref = refs[3 * halves : 3 * halves + 2]
    sends = refs[3 * halves + 2 :]
    n = plan.local
    wide = D // halves
    for k in reversed(range(plan.grp)):
        rows = slice(k * n, (k + 1) * n)
        dn1 = None
        for h in range(halves):
            dq, dk, dv = back[3 * h : 3 * h + 3]
            at = h * wide
            term = against(dk[rows, :], wa[:, D + at : D + at + wide])
            term = term + against(dv[rows, :], wa[:, 2 * D + at : 2 * D + at + wide])
            if k == 0:
                term = term + against(dq[...], wa[:, at : at + wide])
            dn1 = term if dn1 is None else dn1 + term
        if k == 0:
            own_ref[...] = dn1
        else:
            sends[k - 1][...] = dn1.astype(BF16)


def attend_grads_kernel(plan, halves, ids, n1, *refs):
    back = refs[: 3 * halves]
    keep, send, ga_ref = refs[3 * halves :]
    n1_t = n1[...].T
    wide = D // halves
    for h in range(halves):
        dq, dk, dv = back[3 * h : 3 * h + 3]
        at = h * wide
        ga_ref[:, at : at + wide] = mm(n1_t[:, : plan.local], dq[...]).astype(BF16)
        ga_ref[:, D + at : D + at + wide] = mm(n1_t, dk[...]).astype(BF16)
        ga_ref[:, 2 * D + at : 2 * D + at + wide] = mm(n1_t, dv[...]).astype(BF16)

    def copy(z, s, target, o, k):
        target[o, k] = ga_ref[pl.ds(aligned(z * plan.rows + s * SR), SR), :]

    spread(plan, ids[0], ids[1], keep, send, copy)


def finish_kernel(plan, ids, mine, part, out_ref):
    for c, source in enumerate((mine, part)):
        for o in range(plan.half):
            s = xor(ids[1], 2 * o + c)
            out_ref[pl.ds(aligned(s * SR), SR), :] = source[o * SR : (o + 1) * SR, :].astype(F32)


def residual_kernel(plan, *refs):
    own, x0, dx1, gain = refs[:4]
    received = refs[4:-1]
    out_ref = refs[-1]
    dn1 = own[...]
    for r in received:
        dn1 = dn1 + r[...].astype(F32)
    x = x0[...].astype(F32)
    scale = lax.rsqrt(jnp.mean(x * x, axis=1, keepdims=True) + EPSILON)
    unit = x * scale
    e1 = dn1 * gain[...]
    out_ref[...] = dx1[...] + scale * (e1 - unit * jnp.mean(e1 * unit, axis=1, keepdims=True))


def fetch_line(plan, slab):
    blocks = [slab]
    for bit in reversed(plan.line):
        got = swap("grp", bit, plan.grp, jnp.concatenate(blocks, axis=0))
        blocks += jnp.split(got, len(blocks), axis=0)
    return jnp.concatenate(blocks[1:], axis=0)


def fetch_plane(plan, block):
    return jnp.concatenate(
        [block] + [swap("rep", 2 * o, plan.rep, block) for o in range(1, plan.half)], axis=0
    )


def fetch_plane_halves(plan, block, after):
    terms = []
    for half, bits in zip(column_halves(block), (plan.plane, plan.plane[::-1])):
        terms.append(({0: half}, bits))
    for step in range(len(plan.plane)):
        done = []
        for blocks, bits in terms:
            moved = tie(jnp.concatenate(list(blocks.values()), axis=0), *after[step : step + 1])
            got = jnp.split(swap("rep", 2 * bits[step], plan.rep, moved), len(blocks), axis=0)
            done.append((blocks | {o ^ bits[step]: g for o, g in zip(list(blocks), got)}, bits))
        terms = done
    return [jnp.concatenate([mine[o] for o in range(plan.half)], axis=0) for mine, _ in terms]


def column_halves(value):
    middle = value.shape[-1] // 256 * 128
    return value[..., :middle], value[..., middle:]


def fetch_core(plan, mine):
    return swap("rep", 1, plan.rep, mine)


def tie(value, *others):
    return lax.optimization_barrier((value, *others))[0]


def add(*values):
    total = values[0].astype(F32)
    for v in values[1:]:
        total = total + v.astype(F32)
    return total.astype(BF16)


def combine_cores(plan, keep, send):
    got = swap("rep", 1, plan.rep, send)
    return add(keep, got)


def plane_terms(plan, total):
    orders = (plan.plane, plan.plane[::-1])
    return [
        ({o: half[o] for o in range(plan.half)}, bits)
        for half, bits in zip(column_halves(total), orders)
    ]


def plane_step(plan, terms, before=(), after=()):
    done = []
    for mine, bits in terms:
        leave = [o for o in mine if o & bits[0]]
        moved = tie(jnp.stack([mine[o] for o in leave]), *before)
        got = swap("rep", 2 * bits[0], plan.rep, moved)
        kept = {}
        for i, o in enumerate(leave):
            kept[o ^ bits[0]] = add(tie(mine[o ^ bits[0]], *after), got[i])
        done.append((kept, bits[1:]))
    return done


def arrays_of(terms):
    return [value for mine, _ in terms for value in mine.values()]


def combine_line(plan, total, after=()):
    terms = {k: total[k] for k in range(plan.grp)}
    for step, bit in enumerate(plan.line):
        leave = [k for k in terms if k & bit]
        moved = tie(jnp.stack([terms[k] for k in leave]), *after[step : step + 1])
        got = swap("grp", bit, plan.grp, moved)
        terms = {k ^ bit: add(terms[k ^ bit], got[i]) for i, k in enumerate(leave)}
    final = terms[0]
    bit = plan.slices
    while bit < plan.rep:
        final = add(final, swap("rep", bit, plan.rep, final))
        bit *= 2
    return final


def share(plan, final):
    mine = fetch_plane(plan, final)
    return mine, fetch_core(plan, mine)


def pad_columns(plan, weight):
    rows = weight.shape[0]
    blocks = weight.reshape(rows, plan.grp, plan.down)
    blocks = jnp.pad(blocks, ((0, 0), (0, 0), (0, plan.down_pad - plan.down)))
    return blocks.reshape(rows, plan.ffp)


def drop_columns(plan, grad):
    return jnp.concatenate(
        [grad[:, z * plan.down_pad : z * plan.down_pad + plan.down] for z in range(plan.grp)],
        axis=1,
    )


def pack_b(plan, ids, w_gate, w_up, w_out, w_down):
    if plan.down % 8 == 0:
        return call(
            functools.partial(pack_b_kernel, plan),
            [sds((plan.rows, plan.wide_b), BF16), sds((SR, plan.wide_b), BF16)],
            "pack_b",
            (ids, w_gate.T, w_up.T, w_out, w_down),
        )
    rows = jnp.pad(w_down, ((0, plan.down_pad - plan.down), (0, 0)))
    rows = rows.reshape(plan.slices, plan.pieces, SR, D).transpose(0, 2, 1, 3)
    own = jnp.concatenate(
        [
            pad_columns(plan, w_gate),
            pad_columns(plan, w_up),
            w_out,
            rows.reshape(plan.rows, plan.pieces * D),
        ],
        axis=1,
    )
    return own, lax.dynamic_slice(own, (ids[1] * SR, 0), (SR, plan.wide_b))


def finish_b(plan, ids, final, w_gate, w_up, gain):
    line = gain.reshape(1, -1)
    if plan.down % 8 == 0:
        tall = sds((FF, plan.rows), F32)
        gate, up, down, out, norm = call(
            functools.partial(finish_b_kernel, plan),
            [tall, tall, sds((plan.down, D), F32), sds((plan.rows, D), F32), sds(line.shape, F32)],
            "finish_b",
            (ids, *final, w_gate.T, w_up.T, line),
            [pltpu.VMEM((plan.rows, plan.wide_b), BF16)],
        )
        return gate.T, up.T, down, out, norm.reshape(-1)
    (grads,) = call(
        functools.partial(finish_kernel, plan),
        [sds((plan.rows, plan.wide_b), F32)],
        "finish_b",
        (ids, *final),
    )
    ffp = plan.ffp
    down = grads[:, plan.tall_b :].reshape(plan.slices, SR, plan.pieces, D).transpose(0, 2, 1, 3)
    gate = drop_columns(plan, grads[:, :ffp])
    up = drop_columns(plan, grads[:, ffp : 2 * ffp])
    norm = jnp.sum(gate * w_gate.astype(F32) + up * w_up.astype(F32), axis=1) / gain.astype(F32)
    return (
        gate,
        up,
        down.reshape(plan.down_pad, D)[: plan.down],
        grads[:, 2 * ffp : plan.tall_b],
        norm,
    )


def body(plan, tokens, segments, positions, norm1_gain, w_query, w_key, w_value, w_out, norm2_gain, w_gate, w_up, w_down, cotangent):
    g, n = plan.grp, plan.local
    place = lax.axis_index("grp").astype(jnp.int32)
    slice_id = (lax.axis_index("rep") % plan.slices).astype(jnp.int32)
    ids = jnp.stack([place, slice_id])
    x0 = tokens.reshape(n, D)
    cot = cotangent.reshape(n, D)
    reach = jnp.where(segments != 0, positions, 0).reshape(1, n)
    table_cos, table_sin = rotary_tables(plan)
    cosine, sines = jnp.asarray(table_cos), jnp.asarray(table_sin)

    own_a = (w_query, w_key, w_value)
    gains = jnp.stack([norm1_gain, norm2_gain])
    (slab_a,) = call(
        functools.partial(pack_a_kernel, plan),
        [sds((SR, plan.wide_a), BF16)],
        "pack_a",
        (ids, *own_a, norm1_gain.reshape(1, -1), norm2_gain.reshape(1, -1)),
        us=2,
    )
    own_b, slab_b = pack_b(plan, ids, w_gate, w_up, w_out, w_down)

    parts = [x0]
    for _ in range(1, g):
        parts.append(shift(1, g, parts[-1]))
    block_a = fetch_line(plan, slab_a)
    block_b = fetch_line(plan, slab_b)
    mine_a = fetch_plane(plan, tie(block_a, parts[1]))
    mine_b = fetch_plane_halves(plan, tie(block_b, mine_a), (parts[-2], parts[-1]))
    part_a = fetch_core(plan, mine_a)

    lines = [mine_a[i * SR : i * SR + 2, 3 * D : 3 * D + plan.rows] for i in range(g - 1)]
    order = jnp.bitwise_xor(jnp.arange(g, dtype=jnp.int32), place)
    chosen = sum(
        jnp.where((order == k)[:, None, None], tile[None], 0).astype(F32)
        for k, tile in zip([0, *plan.order], [gains, *lines])
    )
    gain1 = chosen[:, 0].reshape(1, D)
    gain2 = chosen[:, 1].reshape(1, D)

    full = plan.full
    attn, q, k_all, v_all, n1, lse, wa = call(
        functools.partial(attend_kernel, plan),
        [
            sds((n, D), F32),
            sds((n, D), BF16),
            sds((full, D), BF16),
            sds((full, D), BF16),
            sds((full, D), BF16),
            sds((H // 2, 1, 2 * n), F32),
            sds((D, 3 * D), BF16),
        ],
        "attend",
        (ids, *parts, *own_a, mine_a, part_a, gain1, cosine, sines, reach),
        [pltpu.VMEM((full, 2 * n), F32)],
        us=11,
    )
    part_b = [fetch_core(plan, tie(half, attn)) for half in mine_b]

    ffp = plan.ffp
    output, dx1, dout, dattn, n2, hid, dg, dup, attn_low = call(
        functools.partial(mlp_kernel, plan),
        [
            sds((n, D), BF16),
            sds((n, D), F32),
            sds((n, D), BF16),
            sds((n, D), BF16),
            sds((n, D), BF16),
            sds((n, ffp), BF16),
            sds((n, ffp), BF16),
            sds((n, ffp), BF16),
            sds((n, D), BF16),
        ],
        "mlp",
        (ids, attn, x0, gain2, cot, own_b, *mine_b, *part_b),
        [pltpu.VMEM((D, plan.tall_b), BF16), pltpu.VMEM((ffp, D), BF16)],
        us=8,
    )

    slabs_b = sds((plan.half, g, SR, plan.wide_b), BF16)
    keep_b, send_b = call(
        functools.partial(mlp_grads_kernel, plan),
        [slabs_b, slabs_b],
        "mlp_grads",
        (ids, n2, hid, dg, dup, cot, attn_low, dout),
        [pltpu.VMEM((D, plan.tall_b), BF16), pltpu.VMEM((ffp, D), BF16)],
        us=6,
    )
    halves = 2
    count = H // 2 // halves
    wide = D // halves

    def attend_back(first, dattn):
        return call(
            functools.partial(attend_back_kernel, plan, first, count),
            [sds((n, wide), BF16), sds((full, wide), BF16), sds((full, wide), BF16)],
            "attend_back",
            (q, k_all, v_all, attn, dattn, lse, cosine, sines, reach),
            [
                pltpu.VMEM((full, 2 * n), F32),
                pltpu.VMEM((n, wide), F32),
                pltpu.VMEM((full, wide), F32),
            ],
            us=8,
        )

    back = list(attend_back(0, tie(dattn, keep_b)))
    core_b = combine_cores(plan, keep_b, send_b)
    back += attend_back(count, tie(dattn, core_b, back[0]))
    terms_b = plane_terms(plan, core_b)
    steps = len(plan.plane)
    if steps:
        terms_b = plane_step(plan, terms_b)

    slabs_a = sds((plan.half, g, SR, 3 * D), BF16)
    keep_a, send_a = call(
        functools.partial(attend_grads_kernel, plan, halves),
        [slabs_a, slabs_a],
        "attend_grads",
        (ids, n1, *back),
        [pltpu.VMEM((D, 3 * D), BF16)],
        us=0,
    )
    own, *sends = call(
        functools.partial(input_kernel, plan, halves),
        [sds((n, D), F32)] + [sds((n, D), BF16)] * (g - 1),
        "dn1",
        (*back, tie(wa, keep_a, *arrays_of(terms_b))),
        us=4,
    )
    moving = sends[g - 2]
    hops = []
    for k in reversed(range(1, g)):
        moving = shift(-1, g, moving)
        hops.append(moving)
        if k > 1:
            moving = add(moving, sends[k - 2])
    core_a = combine_cores(plan, keep_a, send_a)
    terms_a = plane_terms(plan, tie(core_a, own))
    for step in range(steps):
        if step:
            terms_b = plane_step(plan, terms_b, after=(own,))
        terms_a = plane_step(plan, terms_a)
    total_a = jnp.concatenate([mine[0] for mine, _ in terms_a], axis=-1)
    total_b = jnp.concatenate([mine[0] for mine, _ in terms_b], axis=-1)
    final_b = share(plan, tie(combine_line(plan, total_b, (own, hops[0])), hops[1]))
    final_a = share(plan, tie(combine_line(plan, total_a, (hops[0], hops[1])), hops[-1]))
    (input_grad,) = call(
        functools.partial(residual_kernel, plan),
        [sds((n, D), F32)],
        "residual",
        (own, x0, dx1, gain1, moving),
        us=2,
    )
    gate, up, down, out, norm2 = finish_b(plan, ids, final_b, w_gate, w_up, norm2_gain)
    shard = sds((plan.rows, D), F32)
    query, key, value, norm1 = call(
        functools.partial(finish_a_kernel, plan),
        [shard, shard, shard, sds((1, plan.rows), F32)],
        "finish_a",
        (ids, *final_a, *own_a, norm1_gain.reshape(1, -1)),
        [pltpu.VMEM((plan.rows, 3 * D), BF16)],
        us=2,
    )
    return (
        output.reshape(tokens.shape),
        input_grad.reshape(tokens.shape),
        norm1.reshape(-1),
        query,
        key,
        value,
        out,
        norm2,
        gate,
        up,
        down,
    )


def solution(mesh):
    wide, line, pair = P("grp", None), P("grp"), P("rep", "grp")
    three = P("rep", "grp", None)

    def run(tokens, *rest):
        plan = Plan(mesh, tokens.shape)
        return jax.shard_map(
            functools.partial(body, plan),
            mesh=mesh,
            in_specs=(three, pair, pair, line, wide, wide, wide, wide, line, wide, wide, wide, three),
            out_specs=(three, three, line, wide, wide, wide, wide, line, wide, wide, wide),
            check_vma=False,
        )(tokens, *rest)

    return run
```

```python
import functools

import jax
import jax.numpy as jnp
import numpy as np
from jax import lax
from jax.experimental import pallas as pl
from jax.experimental.pallas import tpu as pltpu
from jax.sharding import PartitionSpec as P

D = 512
H = 8
HD = 64
FF = 1376
EPSILON = 1e-05
NEGATIVE = -1e30
SR = 16
PAIR = 2 * HD
F32 = jnp.float32
BF16 = jnp.bfloat16
VMEM = pl.BlockSpec(memory_space=pltpu.VMEM)
SMEM = pl.BlockSpec(memory_space=pltpu.SMEM)
PARAMS = pltpu.CompilerParams(vmem_limit_bytes=32 * 1024 * 1024)


class Plan:
    def __init__(self, mesh, tokens_shape):
        self.rep = mesh.shape["rep"]
        self.grp = mesh.shape["grp"]
        self.rows = D // self.grp
        self.slices = min(self.rep, self.rows // SR)
        self.half = self.slices // 2
        self.down = FF // self.grp
        self.pieces = -(-self.down // (self.slices * SR))
        self.down_pad = self.pieces * self.slices * SR
        self.ffp = self.down_pad * self.grp
        self.local = tokens_shape[1] // self.grp
        self.full = self.local * self.grp
        self.wide_a = 3 * D + 128
        self.tall_b = 2 * self.ffp + D
        self.wide_b = self.tall_b + self.pieces * D
        self.line = [bit for bit in (1, 2, 4, 8, 16) if bit < self.grp]
        self.plane = [bit for bit in (1, 2, 4, 8, 16) if bit < self.half]
        order = [0]
        for bit in reversed(self.line):
            order += [k ^ bit for k in order]
        self.order = order[1:]


def dot(left, right, dims):
    return lax.dot_general(left, right, ((dims[0], dims[1]), ((), ())), preferred_element_type=F32)


def mm(left, right):
    return dot(left, right, ((1,), (0,)))


def against(left, right):
    return dot(left, right, ((1,), (1,)))


def rows_of(left, right):
    return dot(left, right, ((0,), (0,)))


def call(body, outs, name, args, scratch=(), us=0):
    specs = [SMEM if a.dtype == jnp.int32 and a.ndim == 1 else VMEM for a in args]
    args = [a if s is SMEM else near(a) for a, s in zip(args, specs)]
    return pl.pallas_call(
        body,
        out_shape=outs,
        in_specs=specs,
        out_specs=[VMEM] * len(outs),
        scratch_shapes=scratch,
        compiler_params=PARAMS,
        cost_estimate=pl.CostEstimate(flops=us * 10**9, bytes_accessed=0, transcendentals=0),
        name=name,
    )(*args)


def near(value):
    return pltpu.with_memory_space_constraint(value, pltpu.VMEM)


def sds(shape, dtype):
    return jax.ShapeDtypeStruct(shape, dtype)


def swap(axis, k, size, value):
    return lax.ppermute(value, axis, [(i, i ^ k) for i in range(size)])


def shift(k, size, value):
    return lax.ppermute(value, "grp", [(i, i + k) for i in range(size) if 0 <= i + k < size])


def xor(a, b):
    return lax.bitwise_xor(a, jnp.int32(b)) if isinstance(b, int) else lax.bitwise_xor(a, b)


def aligned(index):
    return pl.multiple_of(index, SR)


def rotary_tables(plan):
    halves = HD // 2
    frequency = 10000.0 ** (-2.0 * np.arange(halves) / HD)
    place = np.concatenate([np.arange(plan.local) - k * plan.local for k in range(plan.grp)])
    angle = place[:, None] * frequency[None, :]
    cosine = np.tile(np.cos(angle), (1, 4)).astype(np.float32)
    sines = np.tile(np.concatenate([-np.sin(angle), np.sin(angle)], axis=1), (1, 2))
    return cosine, sines.astype(np.float32)


def swap_halves(value):
    wide = value.shape[1]
    lane = lax.broadcasted_iota(jnp.int32, value.shape, 1)
    first = (lane % HD) < HD // 2
    return jnp.where(
        first, pltpu.roll(value, wide - HD // 2, 1), pltpu.roll(value, HD // 2, 1)
    )


def tile_heads(table, wide):
    return jnp.concatenate([table] * (wide // table.shape[1]), axis=1)


def rotate(value, cosine, sines):
    wide = value.shape[1]
    return value * tile_heads(cosine, wide) + swap_halves(value) * tile_heads(sines, wide)


def rotate_back(value, cosine, sines):
    wide = value.shape[1]
    return value * tile_heads(cosine, wide) - swap_halves(value) * tile_heads(sines, wide)


def two_heads(value):
    lane = lax.broadcasted_iota(jnp.int32, value.shape, 1)
    zero = jnp.zeros_like(value)
    return jnp.concatenate(
        [jnp.where(lane < HD, value, zero), jnp.where(lane < HD, zero, value)], axis=0
    )


def one_pair(value):
    count = value.shape[1] // 2
    return jnp.concatenate([value[:HD, :count], value[HD:, count:]], axis=0).T


def mask_bias(plan, reach, bias_ref):
    n = plan.local
    key = lax.broadcasted_iota(jnp.int32, (n, n), 0)
    query = lax.broadcasted_iota(jnp.int32, (n, n), 1)
    for k in range(plan.grp):
        offset = query - key + k * n
        seen = (offset >= 0) & (offset <= reach)
        bias = jnp.where(seen, 0.0, NEGATIVE).astype(F32)
        bias_ref[k * n : (k + 1) * n, :] = jnp.concatenate([bias, bias], axis=1)


def each_slice(plan, place, slice_id, mine, part, store):
    for c, source in enumerate((mine, part)):
        for o in range(plan.half):
            for i, k in enumerate(plan.order):
                row = (o * (plan.grp - 1) + i) * SR
                rows = [ref[row : row + SR, :] for ref in source]
                rows = jnp.concatenate(rows, axis=1) if len(rows) > 1 else rows[0]
                store(xor(place, k), xor(slice_id, 2 * o + c), rows)


def pack_a_kernel(plan, ids, wq, wk, wv, gain1, gain2, out_ref):
    start = aligned(ids[1] * SR)
    for i, w in enumerate((wq, wk, wv)):
        out_ref[:, i * D : (i + 1) * D] = w[pl.ds(start, SR), :]
    out_ref[:, 3 * D :] = jnp.zeros((SR, 128), BF16)
    out_ref[0:1, 3 * D : 3 * D + plan.rows] = gain1[...]
    out_ref[1:2, 3 * D : 3 * D + plan.rows] = gain2[...]


def pack_b_kernel(plan, ids, gate_t, up_t, out, down, own_ref, slab_ref):
    for i, w in enumerate((gate_t, up_t)):
        for z in range(plan.grp):
            rows = w[z * plan.down : (z + 1) * plan.down, :].astype(F32)
            gap = jnp.zeros((plan.down_pad - plan.down, plan.rows), F32)
            at = i * plan.ffp + z * plan.down_pad
            block = jnp.concatenate([rows, gap], axis=0).T
            own_ref[:, at : at + plan.down_pad] = block.astype(BF16)
    own_ref[:, 2 * plan.ffp : plan.tall_b] = out[...]
    for s in range(plan.slices):
        for i in range(plan.pieces):
            at = (s * plan.pieces + i) * SR
            have = max(0, min(SR, plan.down - at))
            rows = []
            if have:
                rows.append(down[at : at + have, :])
            if have < SR:
                rows.append(jnp.zeros((SR - have, D), BF16))
            cols = slice(plan.tall_b + i * D, plan.tall_b + (i + 1) * D)
            own_ref[s * SR : (s + 1) * SR, cols] = (
                jnp.concatenate(rows, axis=0) if len(rows) > 1 else rows[0]
            )
    slab_ref[...] = own_ref[pl.ds(aligned(ids[1] * SR), SR), :]


def gather_slices(plan, slice_id, mine, part, target):
    for c, source in enumerate((mine, part)):
        for o in range(plan.half):
            s = xor(slice_id, 2 * o + c)
            target[pl.ds(aligned(s * SR), SR), :] = source[o * SR : (o + 1) * SR, :]


def row_sums(value):
    ones = jnp.ones((8, value.shape[1]), F32)
    return lax.dot_general(
        ones, value, (((1,), (1,)), ((), ())), precision=lax.Precision.HIGHEST,
        preferred_element_type=F32,
    )[0:1, :]


def finish_a_kernel(plan, ids, mine, part, wq, wk, wv, gain, *refs):
    scratch = refs[-1]
    gather_slices(plan, ids[1], mine, part, scratch)
    dots = jnp.zeros((plan.rows, D), F32)
    for i, w in enumerate((wq, wk, wv)):
        grad = scratch[:, i * D : (i + 1) * D].astype(F32)
        refs[i][...] = grad
        dots = dots + grad * w[...].astype(F32)
    refs[3][...] = row_sums(dots) / gain[...].astype(F32)


def finish_b_kernel(plan, ids, mine, part, gate_t, up_t, gain, gate_ref, up_ref, down_ref, out_ref, norm_ref, scratch):
    gather_slices(plan, ids[1], mine, part, scratch)
    norm = jnp.zeros((1, plan.rows), F32)
    for i, (ref, weight) in enumerate(((gate_ref, gate_t), (up_ref, up_t))):
        for z in range(plan.grp):
            at = i * plan.ffp + z * plan.down_pad
            block = scratch[:, at : at + plan.down_pad].astype(F32).T[: plan.down, :]
            rows = slice(z * plan.down, (z + 1) * plan.down)
            ref[rows, :] = block
            norm = norm + jnp.sum(block * weight[rows, :].astype(F32), axis=0, keepdims=True)
    norm_ref[...] = norm / gain[...].astype(F32)
    out_ref[...] = scratch[:, 2 * plan.ffp : plan.tall_b].astype(F32)
    for s in range(plan.slices):
        for i in range(plan.pieces):
            at = (s * plan.pieces + i) * SR
            have = max(0, min(SR, plan.down - at))
            if have:
                cols = slice(plan.tall_b + i * D, plan.tall_b + (i + 1) * D)
                rows = scratch[s * SR : (s + 1) * SR, cols].astype(F32)
                down_ref[at : at + have, :] = rows[:have, :]


def attend_kernel(plan, ids, *refs):
    g = plan.grp
    parts = refs[:g]
    own = refs[g : g + 3]
    mine, part, gain, cosine, sines, reach = refs[g + 3 : g + 9]
    attn_ref, q_ref, k_ref, v_ref, n1_ref, lse_ref, wa_ref = refs[g + 9 : g + 16]
    bias_ref, = refs[g + 16 :]
    n = plan.local
    place, slice_id = ids[0], ids[1]
    for i in range(3):
        wa_ref[pl.ds(aligned(place * plan.rows), plan.rows), i * D : (i + 1) * D] = own[i][...]

    def store(z, s, rows):
        wa_ref[pl.ds(aligned(z * plan.rows + s * SR), SR), :] = rows[:, : 3 * D]

    each_slice(plan, place, slice_id, [mine], [part], store)
    mask_bias(plan, reach[...], bias_ref)
    gains = gain[...]
    for k in range(g):
        x = parts[k][...].astype(F32)
        unit = x * lax.rsqrt(jnp.mean(x * x, axis=1, keepdims=True) + EPSILON)
        n1 = (unit * gains).astype(BF16)
        rows = slice(k * n, (k + 1) * n)
        n1_ref[rows, :] = n1
        cos_k, sin_k = cosine[rows, :], sines[rows, :]
        k_ref[rows, :] = rotate(mm(n1, wa_ref[:, D : 2 * D]), cos_k, sin_k).astype(BF16)
        v_ref[rows, :] = mm(n1, wa_ref[:, 2 * D : 3 * D]).astype(BF16)
        if k == 0:
            q_ref[...] = rotate(mm(n1, wa_ref[:, :D]), cos_k, sin_k).astype(BF16) * BF16(
                HD**-0.5
            )

    def pair(i, carry):
        lanes = pl.ds(pl.multiple_of(i * PAIR, PAIR), PAIR)
        score = against(k_ref[:, lanes], two_heads(q_ref[:, lanes])) + bias_ref[...]
        peak = jnp.max(score, axis=0, keepdims=True)
        exponent = jnp.exp(score - peak)
        total = jnp.sum(exponent, axis=0, keepdims=True)
        out = rows_of(v_ref[:, lanes], exponent.astype(BF16)) / total
        attn_ref[:, lanes] = one_pair(out)
        lse_ref[i] = peak + jnp.log(total)
        return carry

    lax.fori_loop(0, H // 2, pair, 0)


def mlp_kernel(plan, ids, *refs):
    attn, x0, gain, cot, own = refs[:5]
    mine, part = refs[5:7], refs[7:9]
    out_ref, dx1_ref, dout_ref, dattn_ref, n2_ref, hid_ref, dg_ref, dup_ref, attn_ref = refs[9:18]
    wgu_ref, wd_ref = refs[18:]
    ffp, tall = plan.ffp, plan.tall_b
    place, slice_id = ids[0], ids[1]

    def store(z, s, rows):
        wgu_ref[pl.ds(aligned(z * plan.rows + s * SR), SR), :] = rows[:, :tall]
        for i in range(plan.pieces):
            at = z * plan.down_pad + (s * plan.pieces + i) * SR
            wd_ref[pl.ds(aligned(at), SR), :] = rows[:, tall + i * D : tall + (i + 1) * D]

    for s in range(plan.slices):
        store(place, s, own[s * SR : (s + 1) * SR, :])
    each_slice(plan, place, slice_id, mine, part, store)

    attn_low = attn[...].astype(BF16)
    attn_ref[...] = attn_low
    x1 = x0[...].astype(F32) + mm(attn_low, wgu_ref[:, 2 * ffp :])
    scale = lax.rsqrt(jnp.mean(x1 * x1, axis=1, keepdims=True) + EPSILON)
    unit = x1 * scale
    gains = gain[...]
    n2 = (unit * gains).astype(BF16)
    n2_ref[...] = n2
    c = cot[...]
    out = x1
    dn2 = jnp.zeros_like(x1)
    step = 512 if ffp % 512 == 0 else ffp
    for f in range(0, ffp, step):
        cols = slice(f, f + step)
        up_cols = slice(ffp + f, ffp + f + step)
        gate = mm(n2, wgu_ref[:, cols])
        up = mm(n2, wgu_ref[:, up_cols])
        dhid = against(c, wd_ref[cols, :])
        sig = 1.0 / (1.0 + jnp.exp(-gate))
        silu = gate * sig
        hid = (silu * up).astype(BF16)
        dup = (dhid * silu).astype(BF16)
        dg = (dhid * up * (sig * (1.0 + gate * (1.0 - sig)))).astype(BF16)
        hid_ref[:, cols] = hid
        dg_ref[:, cols] = dg
        dup_ref[:, cols] = dup
        out = out + mm(hid, wd_ref[cols, :])
        dn2 = dn2 + against(dg, wgu_ref[:, cols]) + against(dup, wgu_ref[:, up_cols])
    out_ref[...] = out.astype(BF16)
    e2 = dn2 * gains
    dx1 = c.astype(F32) + scale * (e2 - unit * jnp.mean(e2 * unit, axis=1, keepdims=True))
    dx1_ref[...] = dx1
    dout = dx1.astype(BF16)
    dout_ref[...] = dout
    dattn_ref[...] = against(dout, wgu_ref[:, 2 * ffp :]).astype(BF16)


def spread(plan, place, slice_id, keep, send, copy):
    for c, target in enumerate((keep, send)):
        for o in range(plan.half):
            for k in range(plan.grp):
                copy(xor(place, k), xor(slice_id, 2 * o + c), target, o, k)


def mlp_grads_kernel(plan, ids, n2, hid, dg, dup, cot, attn, dout, keep, send, gu_ref, d_ref):
    ffp, tall = plan.ffp, plan.tall_b
    n2_t = n2[...].T
    gu_ref[:, :ffp] = mm(n2_t, dg[...]).astype(BF16)
    gu_ref[:, ffp : 2 * ffp] = mm(n2_t, dup[...]).astype(BF16)
    gu_ref[:, 2 * ffp :] = rows_of(attn[...], dout[...]).astype(BF16)
    d_ref[...] = rows_of(hid[...], cot[...]).astype(BF16)

    def copy(z, s, target, o, k):
        target[o, k, :, :tall] = gu_ref[pl.ds(aligned(z * plan.rows + s * SR), SR), :]
        for i in range(plan.pieces):
            at = z * plan.down_pad + (s * plan.pieces + i) * SR
            target[o, k, :, tall + i * D : tall + (i + 1) * D] = d_ref[pl.ds(aligned(at), SR), :]

    spread(plan, ids[0], ids[1], keep, send, copy)


def attend_back_kernel(plan, first, count, q, k_in, v_in, attn, dattn, lse, cosine, sines, reach, dq_ref, dk_ref, dv_ref, bias_ref, dq_scr, dk_scr):
    mask_bias(plan, reach[...], bias_ref)

    def pair(i, carry):
        lanes = pl.ds(pl.multiple_of((first + i) * PAIR, PAIR), PAIR)
        outs = pl.ds(pl.multiple_of(i * PAIR, PAIR), PAIR)
        q2 = two_heads(q[:, lanes])
        da = dattn[:, lanes]
        da2 = two_heads(da)
        prod = two_heads(da.astype(F32) * attn[:, lanes])
        ones = jnp.ones((8, PAIR), F32)
        mean = lax.dot_general(
            ones, prod, (((1,), (1,)), ((), ())), precision=lax.Precision.HIGHEST,
            preferred_element_type=F32,
        )[0:1, :]
        keys = k_in[:, lanes]
        values = v_in[:, lanes]
        prob = jnp.exp(against(keys, q2) + (bias_ref[...] - lse[first + i]))
        dprob = against(values, da2)
        dscore = (prob * (dprob - mean)).astype(BF16)
        dv_ref[:, outs] = mm(prob.astype(BF16), da2).astype(BF16)
        dk_scr[:, outs] = mm(dscore, q2)
        dq_scr[:, outs] = one_pair(rows_of(keys, dscore)) * (HD**-0.5)
        return carry

    lax.fori_loop(0, count, pair, 0)
    n = plan.local
    dq_ref[...] = rotate_back(dq_scr[...], cosine[:n, :], sines[:n, :]).astype(BF16)
    for k in range(plan.grp):
        rows = slice(k * n, (k + 1) * n)
        dk_ref[rows, :] = rotate_back(dk_scr[rows, :], cosine[rows, :], sines[rows, :]).astype(BF16)


def input_kernel(plan, halves, *refs):
    back = refs[: 3 * halves]
    wa, own_ref = refs[3 * halves : 3 * halves + 2]
    sends = refs[3 * halves + 2 :]
    n = plan.local
    wide = D // halves
    for k in reversed(range(plan.grp)):
        rows = slice(k * n, (k + 1) * n)
        dn1 = None
        for h in range(halves):
            dq, dk, dv = back[3 * h : 3 * h + 3]
            at = h * wide
            term = against(dk[rows, :], wa[:, D + at : D + at + wide])
            term = term + against(dv[rows, :], wa[:, 2 * D + at : 2 * D + at + wide])
            if k == 0:
                term = term + against(dq[...], wa[:, at : at + wide])
            dn1 = term if dn1 is None else dn1 + term
        if k == 0:
            own_ref[...] = dn1
        else:
            sends[k - 1][...] = dn1.astype(BF16)


def attend_grads_kernel(plan, halves, ids, n1, *refs):
    back = refs[: 3 * halves]
    keep, send, ga_ref = refs[3 * halves :]
    n1_t = n1[...].T
    wide = D // halves
    for h in range(halves):
        dq, dk, dv = back[3 * h : 3 * h + 3]
        at = h * wide
        ga_ref[:, at : at + wide] = mm(n1_t[:, : plan.local], dq[...]).astype(BF16)
        ga_ref[:, D + at : D + at + wide] = mm(n1_t, dk[...]).astype(BF16)
        ga_ref[:, 2 * D + at : 2 * D + at + wide] = mm(n1_t, dv[...]).astype(BF16)

    def copy(z, s, target, o, k):
        target[o, k] = ga_ref[pl.ds(aligned(z * plan.rows + s * SR), SR), :]

    spread(plan, ids[0], ids[1], keep, send, copy)


def finish_kernel(plan, ids, mine, part, out_ref):
    for c, source in enumerate((mine, part)):
        for o in range(plan.half):
            s = xor(ids[1], 2 * o + c)
            out_ref[pl.ds(aligned(s * SR), SR), :] = source[o * SR : (o + 1) * SR, :].astype(F32)


def residual_kernel(plan, *refs):
    own, x0, dx1, gain = refs[:4]
    received = refs[4:-1]
    out_ref = refs[-1]
    dn1 = own[...]
    for r in received:
        dn1 = dn1 + r[...].astype(F32)
    x = x0[...].astype(F32)
    scale = lax.rsqrt(jnp.mean(x * x, axis=1, keepdims=True) + EPSILON)
    unit = x * scale
    e1 = dn1 * gain[...]
    out_ref[...] = dx1[...] + scale * (e1 - unit * jnp.mean(e1 * unit, axis=1, keepdims=True))


def fetch_line(plan, slab):
    blocks = [slab]
    for bit in reversed(plan.line):
        got = swap("grp", bit, plan.grp, jnp.concatenate(blocks, axis=0))
        blocks += jnp.split(got, len(blocks), axis=0)
    return jnp.concatenate(blocks[1:], axis=0)


def fetch_plane(plan, block):
    return jnp.concatenate(
        [block] + [swap("rep", 2 * o, plan.rep, block) for o in range(1, plan.half)], axis=0
    )


def fetch_plane_halves(plan, block, after):
    terms = []
    for half, bits in zip(column_halves(block), (plan.plane, plan.plane[::-1])):
        terms.append(({0: half}, bits))
    for step in range(len(plan.plane)):
        done = []
        for blocks, bits in terms:
            moved = tie(jnp.concatenate(list(blocks.values()), axis=0), *after[step : step + 1])
            got = jnp.split(swap("rep", 2 * bits[step], plan.rep, moved), len(blocks), axis=0)
            done.append((blocks | {o ^ bits[step]: g for o, g in zip(list(blocks), got)}, bits))
        terms = done
    return [jnp.concatenate([mine[o] for o in range(plan.half)], axis=0) for mine, _ in terms]


def column_halves(value):
    middle = value.shape[-1] // 256 * 128
    return value[..., :middle], value[..., middle:]


def fetch_core(plan, mine):
    return swap("rep", 1, plan.rep, mine)


def tie(value, *others):
    return lax.optimization_barrier((value, *others))[0]


def add(*values):
    total = values[0].astype(F32)
    for v in values[1:]:
        total = total + v.astype(F32)
    return total.astype(BF16)


def combine_cores(plan, keep, send):
    got = swap("rep", 1, plan.rep, send)
    return add(keep, got)


def plane_terms(plan, total):
    orders = (plan.plane, plan.plane[::-1])
    return [
        ({o: half[o] for o in range(plan.half)}, bits)
        for half, bits in zip(column_halves(total), orders)
    ]


def plane_step(plan, terms, before=(), after=()):
    done = []
    for mine, bits in terms:
        leave = [o for o in mine if o & bits[0]]
        moved = tie(jnp.stack([mine[o] for o in leave]), *before)
        got = swap("rep", 2 * bits[0], plan.rep, moved)
        kept = {}
        for i, o in enumerate(leave):
            kept[o ^ bits[0]] = add(tie(mine[o ^ bits[0]], *after), got[i])
        done.append((kept, bits[1:]))
    return done


def arrays_of(terms):
    return [value for mine, _ in terms for value in mine.values()]


def combine_line(plan, total, after=()):
    terms = {k: total[k] for k in range(plan.grp)}
    for step, bit in enumerate(plan.line):
        leave = [k for k in terms if k & bit]
        moved = tie(jnp.stack([terms[k] for k in leave]), *after[step : step + 1])
        got = swap("grp", bit, plan.grp, moved)
        terms = {k ^ bit: add(terms[k ^ bit], got[i]) for i, k in enumerate(leave)}
    final = terms[0]
    bit = plan.slices
    while bit < plan.rep:
        final = add(final, swap("rep", bit, plan.rep, final))
        bit *= 2
    return final


def share(plan, final):
    mine = fetch_plane(plan, final)
    return mine, fetch_core(plan, mine)


def pad_columns(plan, weight):
    rows = weight.shape[0]
    blocks = weight.reshape(rows, plan.grp, plan.down)
    blocks = jnp.pad(blocks, ((0, 0), (0, 0), (0, plan.down_pad - plan.down)))
    return blocks.reshape(rows, plan.ffp)


def drop_columns(plan, grad):
    return jnp.concatenate(
        [grad[:, z * plan.down_pad : z * plan.down_pad + plan.down] for z in range(plan.grp)],
        axis=1,
    )


def pack_b(plan, ids, w_gate, w_up, w_out, w_down):
    if plan.down % 8 == 0:
        return call(
            functools.partial(pack_b_kernel, plan),
            [pltpu.VMEM((plan.rows, plan.wide_b), BF16), pltpu.VMEM((SR, plan.wide_b), BF16)],
            "pack_b",
            (ids, w_gate.T, w_up.T, w_out, w_down),
        )
    rows = jnp.pad(w_down, ((0, plan.down_pad - plan.down), (0, 0)))
    rows = rows.reshape(plan.slices, plan.pieces, SR, D).transpose(0, 2, 1, 3)
    own = jnp.concatenate(
        [
            pad_columns(plan, w_gate),
            pad_columns(plan, w_up),
            w_out,
            rows.reshape(plan.rows, plan.pieces * D),
        ],
        axis=1,
    )
    return own, lax.dynamic_slice(own, (ids[1] * SR, 0), (SR, plan.wide_b))


def finish_b(plan, ids, final, w_gate, w_up, gain):
    line = gain.reshape(1, -1)
    if plan.down % 8 == 0:
        tall = sds((FF, plan.rows), F32)
        gate, up, down, out, norm = call(
            functools.partial(finish_b_kernel, plan),
            [tall, tall, sds((plan.down, D), F32), sds((plan.rows, D), F32), sds(line.shape, F32)],
            "finish_b",
            (ids, *final, w_gate.T, w_up.T, line),
            [pltpu.VMEM((plan.rows, plan.wide_b), BF16)],
        )
        return gate.T, up.T, down, out, norm.reshape(-1)
    (grads,) = call(
        functools.partial(finish_kernel, plan),
        [sds((plan.rows, plan.wide_b), F32)],
        "finish_b",
        (ids, *final),
    )
    ffp = plan.ffp
    down = grads[:, plan.tall_b :].reshape(plan.slices, SR, plan.pieces, D).transpose(0, 2, 1, 3)
    gate = drop_columns(plan, grads[:, :ffp])
    up = drop_columns(plan, grads[:, ffp : 2 * ffp])
    norm = jnp.sum(gate * w_gate.astype(F32) + up * w_up.astype(F32), axis=1) / gain.astype(F32)
    return (
        gate,
        up,
        down.reshape(plan.down_pad, D)[: plan.down],
        grads[:, 2 * ffp : plan.tall_b],
        norm,
    )


def body(plan, tokens, segments, positions, norm1_gain, w_query, w_key, w_value, w_out, norm2_gain, w_gate, w_up, w_down, cotangent):
    g, n = plan.grp, plan.local
    place = lax.axis_index("grp").astype(jnp.int32)
    slice_id = (lax.axis_index("rep") % plan.slices).astype(jnp.int32)
    ids = jnp.stack([place, slice_id])
    x0 = tokens.reshape(n, D)
    cot = cotangent.reshape(n, D)
    reach = jnp.where(segments != 0, positions, 0).reshape(1, n)
    table_cos, table_sin = rotary_tables(plan)
    cosine, sines = jnp.asarray(table_cos), jnp.asarray(table_sin)

    own_a = (w_query, w_key, w_value)
    gains = jnp.stack([norm1_gain, norm2_gain])
    (slab_a,) = call(
        functools.partial(pack_a_kernel, plan),
        [pltpu.VMEM((SR, plan.wide_a), BF16)],
        "pack_a",
        (ids, *own_a, norm1_gain.reshape(1, -1), norm2_gain.reshape(1, -1)),
        us=2,
    )
    own_b, slab_b = pack_b(plan, ids, w_gate, w_up, w_out, w_down)

    parts = [x0]
    for _ in range(1, g):
        parts.append(shift(1, g, parts[-1]))
    block_a = fetch_line(plan, slab_a)
    block_b = fetch_line(plan, slab_b)
    mine_a = fetch_plane(plan, tie(block_a, parts[1]))
    mine_b = fetch_plane_halves(plan, tie(block_b, mine_a), (parts[-2], parts[-1]))
    part_a = fetch_core(plan, mine_a)

    lines = [mine_a[i * SR : i * SR + 2, 3 * D : 3 * D + plan.rows] for i in range(g - 1)]
    order = jnp.bitwise_xor(jnp.arange(g, dtype=jnp.int32), place)
    chosen = sum(
        jnp.where((order == k)[:, None, None], tile[None], 0).astype(F32)
        for k, tile in zip([0, *plan.order], [gains, *lines])
    )
    gain1 = chosen[:, 0].reshape(1, D)
    gain2 = chosen[:, 1].reshape(1, D)

    full = plan.full
    attn, q, k_all, v_all, n1, lse, wa = call(
        functools.partial(attend_kernel, plan),
        [
            pltpu.VMEM((n, D), F32),
            pltpu.VMEM((n, D), BF16),
            pltpu.VMEM((full, D), BF16),
            pltpu.VMEM((full, D), BF16),
            pltpu.VMEM((full, D), BF16),
            pltpu.VMEM((H // 2, 1, 2 * n), F32),
            pltpu.VMEM((D, 3 * D), BF16),
        ],
        "attend",
        (ids, *parts, *own_a, mine_a, part_a, gain1, cosine, sines, reach),
        [pltpu.VMEM((full, 2 * n), F32)],
        us=11,
    )
    part_b = [fetch_core(plan, tie(half, attn)) for half in mine_b]

    ffp = plan.ffp
    output, dx1, dout, dattn, n2, hid, dg, dup, attn_low = call(
        functools.partial(mlp_kernel, plan),
        [
            sds((n, D), BF16),
            pltpu.VMEM((n, D), F32),
            pltpu.VMEM((n, D), BF16),
            pltpu.VMEM((n, D), BF16),
            pltpu.VMEM((n, D), BF16),
            pltpu.VMEM((n, ffp), BF16),
            pltpu.VMEM((n, ffp), BF16),
            pltpu.VMEM((n, ffp), BF16),
            pltpu.VMEM((n, D), BF16),
        ],
        "mlp",
        (ids, attn, x0, gain2, cot, own_b, *mine_b, *part_b),
        [pltpu.VMEM((D, plan.tall_b), BF16), pltpu.VMEM((ffp, D), BF16)],
        us=8,
    )

    slabs_b = pltpu.VMEM((plan.half, g, SR, plan.wide_b), BF16)
    keep_b, send_b = call(
        functools.partial(mlp_grads_kernel, plan),
        [slabs_b, slabs_b],
        "mlp_grads",
        (ids, n2, hid, dg, dup, cot, attn_low, dout),
        [pltpu.VMEM((D, plan.tall_b), BF16), pltpu.VMEM((ffp, D), BF16)],
        us=6,
    )
    halves = 2
    count = H // 2 // halves
    wide = D // halves

    def attend_back(first, dattn):
        return call(
            functools.partial(attend_back_kernel, plan, first, count),
            [pltpu.VMEM((n, wide), BF16), pltpu.VMEM((full, wide), BF16), pltpu.VMEM((full, wide), BF16)],
            "attend_back",
            (q, k_all, v_all, attn, dattn, lse, cosine, sines, reach),
            [
                pltpu.VMEM((full, 2 * n), F32),
                pltpu.VMEM((n, wide), F32),
                pltpu.VMEM((full, wide), F32),
            ],
            us=8,
        )

    back = list(attend_back(0, tie(dattn, keep_b)))
    core_b = combine_cores(plan, keep_b, send_b)
    back += attend_back(count, tie(dattn, core_b, back[0]))
    terms_b = plane_terms(plan, core_b)
    steps = len(plan.plane)
    if steps:
        terms_b = plane_step(plan, terms_b)

    slabs_a = pltpu.VMEM((plan.half, g, SR, 3 * D), BF16)
    keep_a, send_a = call(
        functools.partial(attend_grads_kernel, plan, halves),
        [slabs_a, slabs_a],
        "attend_grads",
        (ids, n1, *back),
        [pltpu.VMEM((D, 3 * D), BF16)],
        us=0,
    )
    own, *sends = call(
        functools.partial(input_kernel, plan, halves),
        [pltpu.VMEM((n, D), F32)] + [pltpu.VMEM((n, D), BF16)] * (g - 1),
        "dn1",
        (*back, tie(wa, keep_a, *arrays_of(terms_b))),
        us=4,
    )
    moving = sends[g - 2]
    hops = []
    for k in reversed(range(1, g)):
        moving = shift(-1, g, moving)
        hops.append(moving)
        if k > 1:
            moving = add(moving, sends[k - 2])
    core_a = combine_cores(plan, keep_a, send_a)
    terms_a = plane_terms(plan, tie(core_a, own))
    for step in range(steps):
        if step:
            terms_b = plane_step(plan, terms_b, after=(own,))
        terms_a = plane_step(plan, terms_a)
    total_a = jnp.concatenate([mine[0] for mine, _ in terms_a], axis=-1)
    total_b = jnp.concatenate([mine[0] for mine, _ in terms_b], axis=-1)
    final_b = share(plan, tie(combine_line(plan, total_b, (own, hops[0])), hops[1]))
    final_a = share(plan, tie(combine_line(plan, total_a, (hops[0], hops[1])), hops[-1]))
    (input_grad,) = call(
        functools.partial(residual_kernel, plan),
        [sds((n, D), F32)],
        "residual",
        (own, x0, dx1, gain1, moving),
        us=2,
    )
    gate, up, down, out, norm2 = finish_b(plan, ids, final_b, w_gate, w_up, norm2_gain)
    shard = sds((plan.rows, D), F32)
    query, key, value, norm1 = call(
        functools.partial(finish_a_kernel, plan),
        [shard, shard, shard, sds((1, plan.rows), F32)],
        "finish_a",
        (ids, *final_a, *own_a, norm1_gain.reshape(1, -1)),
        [pltpu.VMEM((plan.rows, 3 * D), BF16)],
        us=2,
    )
    return (
        output.reshape(tokens.shape),
        input_grad.reshape(tokens.shape),
        norm1.reshape(-1),
        query,
        key,
        value,
        out,
        norm2,
        gate,
        up,
        down,
    )


def solution(mesh):
    wide, line, pair = P("grp", None), P("grp"), P("rep", "grp")
    three = P("rep", "grp", None)

    def run(tokens, *rest):
        plan = Plan(mesh, tokens.shape)
        return jax.shard_map(
            functools.partial(body, plan),
            mesh=mesh,
            in_specs=(three, pair, pair, line, wide, wide, wide, wide, line, wide, wide, wide, three),
            out_specs=(three, three, line, wide, wide, wide, wide, line, wide, wide, wide),
            check_vma=False,
        )(tokens, *rest)

    return run
```

```python
import functools

import jax
import jax.numpy as jnp
import numpy as np
from jax import lax
from jax.experimental import pallas as pl
from jax.experimental.pallas import tpu as pltpu
from jax.sharding import PartitionSpec as P

D = 512
H = 8
HD = 64
FF = 1376
EPSILON = 1e-05
NEGATIVE = -1e30
SR = 16
PAIR = 2 * HD
F32 = jnp.float32
BF16 = jnp.bfloat16
VMEM = pl.BlockSpec(memory_space=pltpu.VMEM)
SMEM = pl.BlockSpec(memory_space=pltpu.SMEM)
PARAMS = pltpu.CompilerParams(vmem_limit_bytes=32 * 1024 * 1024)


class Plan:
    def __init__(self, mesh, tokens_shape):
        self.rep = mesh.shape["rep"]
        self.grp = mesh.shape["grp"]
        self.rows = D // self.grp
        self.slices = min(self.rep, self.rows // SR)
        self.half = self.slices // 2
        self.down = FF // self.grp
        self.pieces = -(-self.down // (self.slices * SR))
        self.down_pad = self.pieces * self.slices * SR
        self.ffp = self.down_pad * self.grp
        self.local = tokens_shape[1] // self.grp
        self.full = self.local * self.grp
        self.wide_a = 3 * D + 128
        self.tall_b = 2 * self.ffp + D
        self.wide_b = self.tall_b + self.pieces * D
        self.line = [bit for bit in (1, 2, 4, 8, 16) if bit < self.grp]
        self.plane = [bit for bit in (1, 2, 4, 8, 16) if bit < self.half]
        order = [0]
        for bit in reversed(self.line):
            order += [k ^ bit for k in order]
        self.order = order[1:]


def dot(left, right, dims):
    return lax.dot_general(left, right, ((dims[0], dims[1]), ((), ())), preferred_element_type=F32)


def mm(left, right):
    return dot(left, right, ((1,), (0,)))


def against(left, right):
    return dot(left, right, ((1,), (1,)))


def rows_of(left, right):
    return dot(left, right, ((0,), (0,)))


def call(body, outs, name, args, scratch=(), us=0, far=()):
    specs = [SMEM if a.dtype == jnp.int32 and a.ndim == 1 else VMEM for a in args]
    spaces = [pltpu.HBM if any(a is b for b in far) else pltpu.VMEM for a in args]
    args = [
        pltpu.with_memory_space_constraint(a, space) if spec is VMEM else a
        for a, space, spec in zip(args, spaces, specs)
    ]
    return pl.pallas_call(
        body,
        out_shape=outs,
        in_specs=specs,
        out_specs=[VMEM] * len(outs),
        scratch_shapes=scratch,
        compiler_params=PARAMS,
        cost_estimate=pl.CostEstimate(flops=us * 10**9, bytes_accessed=0, transcendentals=0),
        name=name,
    )(*args)


def sds(shape, dtype):
    return jax.ShapeDtypeStruct(shape, dtype)


def swap(axis, k, size, value):
    return lax.ppermute(value, axis, [(i, i ^ k) for i in range(size)])


def shift(k, size, value):
    return lax.ppermute(value, "grp", [(i, i + k) for i in range(size) if 0 <= i + k < size])


def xor(a, b):
    return lax.bitwise_xor(a, jnp.int32(b)) if isinstance(b, int) else lax.bitwise_xor(a, b)


def aligned(index):
    return pl.multiple_of(index, SR)


def rotary_tables(plan):
    halves = HD // 2
    frequency = 10000.0 ** (-2.0 * np.arange(halves) / HD)
    place = np.concatenate([np.arange(plan.local) - k * plan.local for k in range(plan.grp)])
    angle = place[:, None] * frequency[None, :]
    cosine = np.tile(np.cos(angle), (1, 4)).astype(np.float32)
    sines = np.tile(np.concatenate([-np.sin(angle), np.sin(angle)], axis=1), (1, 2))
    return cosine, sines.astype(np.float32)


def swap_halves(value):
    wide = value.shape[1]
    lane = lax.broadcasted_iota(jnp.int32, value.shape, 1)
    first = (lane % HD) < HD // 2
    return jnp.where(
        first, pltpu.roll(value, wide - HD // 2, 1), pltpu.roll(value, HD // 2, 1)
    )


def tile_heads(table, wide):
    return jnp.concatenate([table] * (wide // table.shape[1]), axis=1)


def rotate(value, cosine, sines):
    wide = value.shape[1]
    return value * tile_heads(cosine, wide) + swap_halves(value) * tile_heads(sines, wide)


def rotate_back(value, cosine, sines):
    wide = value.shape[1]
    return value * tile_heads(cosine, wide) - swap_halves(value) * tile_heads(sines, wide)


def two_heads(value):
    lane = lax.broadcasted_iota(jnp.int32, value.shape, 1)
    zero = jnp.zeros_like(value)
    return jnp.concatenate(
        [jnp.where(lane < HD, value, zero), jnp.where(lane < HD, zero, value)], axis=0
    )


def one_pair(value):
    count = value.shape[1] // 2
    return jnp.concatenate([value[:HD, :count], value[HD:, count:]], axis=0).T


def mask_bias(plan, reach, bias_ref, parts):
    n = plan.local
    key = lax.broadcasted_iota(jnp.int32, (n, n), 0)
    query = lax.broadcasted_iota(jnp.int32, (n, n), 1)
    for i, k in enumerate(parts):
        offset = query - key + k * n
        seen = (offset >= 0) & (offset <= reach)
        bias = jnp.where(seen, 0.0, NEGATIVE).astype(F32)
        bias_ref[i * n : (i + 1) * n, :] = jnp.concatenate([bias, bias], axis=1)


def each_slice(plan, place, slice_id, mine, part, store):
    for c, source in enumerate((mine, part)):
        for o in range(plan.half):
            for i, k in enumerate(plan.order):
                row = (o * (plan.grp - 1) + i) * SR
                rows = [ref[row : row + SR, :] for ref in source]
                rows = jnp.concatenate(rows, axis=1) if len(rows) > 1 else rows[0]
                store(xor(place, k), xor(slice_id, 2 * o + c), rows)


def pack_a_kernel(plan, ids, wq, wk, wv, gain1, gain2, out_ref):
    start = aligned(ids[1] * SR)
    for i, w in enumerate((wq, wk, wv)):
        out_ref[:, i * D : (i + 1) * D] = w[pl.ds(start, SR), :]
    out_ref[:, 3 * D :] = jnp.zeros((SR, 128), BF16)
    out_ref[0:1, 3 * D : 3 * D + plan.rows] = gain1[...]
    out_ref[1:2, 3 * D : 3 * D + plan.rows] = gain2[...]


def pack_b_kernel(plan, ids, gate_t, up_t, out, down, own_ref, slab_ref):
    for i, w in enumerate((gate_t, up_t)):
        for z in range(plan.grp):
            rows = w[z * plan.down : (z + 1) * plan.down, :].astype(F32)
            gap = jnp.zeros((plan.down_pad - plan.down, plan.rows), F32)
            at = i * plan.ffp + z * plan.down_pad
            block = jnp.concatenate([rows, gap], axis=0).T
            own_ref[:, at : at + plan.down_pad] = block.astype(BF16)
    own_ref[:, 2 * plan.ffp : plan.tall_b] = out[...]
    for s in range(plan.slices):
        for i in range(plan.pieces):
            at = (s * plan.pieces + i) * SR
            have = max(0, min(SR, plan.down - at))
            rows = []
            if have:
                rows.append(down[at : at + have, :])
            if have < SR:
                rows.append(jnp.zeros((SR - have, D), BF16))
            cols = slice(plan.tall_b + i * D, plan.tall_b + (i + 1) * D)
            own_ref[s * SR : (s + 1) * SR, cols] = (
                jnp.concatenate(rows, axis=0) if len(rows) > 1 else rows[0]
            )
    slab_ref[...] = own_ref[pl.ds(aligned(ids[1] * SR), SR), :]


def gather_slices(plan, slice_id, mine, part, target):
    for c, source in enumerate((mine, part)):
        for o in range(plan.half):
            s = xor(slice_id, 2 * o + c)
            target[pl.ds(aligned(s * SR), SR), :] = source[o * SR : (o + 1) * SR, :]


def row_sums(value):
    ones = jnp.ones((8, value.shape[1]), F32)
    return lax.dot_general(
        ones, value, (((1,), (1,)), ((), ())), precision=lax.Precision.HIGHEST,
        preferred_element_type=F32,
    )[0:1, :]


def finish_a_kernel(plan, ids, mine, part, wq, wk, wv, gain, *refs):
    scratch = refs[-1]
    gather_slices(plan, ids[1], mine, part, scratch)
    dots = jnp.zeros((plan.rows, D), F32)
    for i, w in enumerate((wq, wk, wv)):
        grad = scratch[:, i * D : (i + 1) * D].astype(F32)
        refs[i][...] = grad
        dots = dots + grad * w[...].astype(F32)
    refs[3][...] = row_sums(dots) / gain[...].astype(F32)


def finish_b_kernel(plan, ids, mine, part, gate_t, up_t, gain, gate_ref, up_ref, down_ref, out_ref, norm_ref, scratch):
    gather_slices(plan, ids[1], mine, part, scratch)
    norm = jnp.zeros((1, plan.rows), F32)
    for i, (ref, weight) in enumerate(((gate_ref, gate_t), (up_ref, up_t))):
        for z in range(plan.grp):
            at = i * plan.ffp + z * plan.down_pad
            block = scratch[:, at : at + plan.down_pad].astype(F32).T[: plan.down, :]
            rows = slice(z * plan.down, (z + 1) * plan.down)
            ref[rows, :] = block
            norm = norm + jnp.sum(block * weight[rows, :].astype(F32), axis=0, keepdims=True)
    norm_ref[...] = norm / gain[...].astype(F32)
    out_ref[...] = scratch[:, 2 * plan.ffp : plan.tall_b].astype(F32)
    for s in range(plan.slices):
        for i in range(plan.pieces):
            at = (s * plan.pieces + i) * SR
            have = max(0, min(SR, plan.down - at))
            if have:
                cols = slice(plan.tall_b + i * D, plan.tall_b + (i + 1) * D)
                rows = scratch[s * SR : (s + 1) * SR, cols].astype(F32)
                down_ref[at : at + have, :] = rows[:have, :]


def attend_kernel(plan, ids, *refs):
    g = plan.grp
    parts = refs[:g]
    own = refs[g : g + 3]
    mine, part, gain, cosine, sines, reach = refs[g + 3 : g + 9]
    attn_ref, q_ref, k_ref, v_ref, n1_ref, lse_ref, wa_ref = refs[g + 9 : g + 16]
    bias_ref, = refs[g + 16 :]
    n = plan.local
    place, slice_id = ids[0], ids[1]
    for i in range(3):
        wa_ref[pl.ds(aligned(place * plan.rows), plan.rows), i * D : (i + 1) * D] = own[i][...]

    def store(z, s, rows):
        wa_ref[pl.ds(aligned(z * plan.rows + s * SR), SR), :] = rows[:, : 3 * D]

    each_slice(plan, place, slice_id, [mine], [part], store)
    mask_bias(plan, reach[...], bias_ref, range(g))
    gains = gain[...]
    for k in range(g):
        x = parts[k][...].astype(F32)
        unit = x * lax.rsqrt(jnp.mean(x * x, axis=1, keepdims=True) + EPSILON)
        n1 = (unit * gains).astype(BF16)
        rows = slice(k * n, (k + 1) * n)
        n1_ref[rows, :] = n1
        cos_k, sin_k = cosine[rows, :], sines[rows, :]
        k_ref[rows, :] = rotate(mm(n1, wa_ref[:, D : 2 * D]), cos_k, sin_k).astype(BF16)
        v_ref[rows, :] = mm(n1, wa_ref[:, 2 * D : 3 * D]).astype(BF16)
        if k == 0:
            q_ref[...] = rotate(mm(n1, wa_ref[:, :D]), cos_k, sin_k).astype(BF16) * BF16(
                HD**-0.5
            )

    def pair(i, carry):
        lanes = pl.ds(pl.multiple_of(i * PAIR, PAIR), PAIR)
        score = against(k_ref[:, lanes], two_heads(q_ref[:, lanes])) + bias_ref[...]
        peak = jnp.max(score, axis=0, keepdims=True)
        exponent = jnp.exp(score - peak)
        total = jnp.sum(exponent, axis=0, keepdims=True)
        out = rows_of(v_ref[:, lanes], exponent.astype(BF16)) / total
        attn_ref[:, lanes] = one_pair(out)
        lse_ref[i] = peak + jnp.log(total)
        return carry

    lax.fori_loop(0, H // 2, pair, 0)


def mlp_kernel(plan, ids, *refs):
    attn, x0, gain, cot, own = refs[:5]
    mine, part = refs[5:7], refs[7:9]
    out_ref, dx1_ref, dout_ref, dattn_ref, n2_ref, hid_ref, dg_ref, dup_ref, attn_ref = refs[9:18]
    wgu_ref, wd_ref = refs[18:]
    ffp, tall = plan.ffp, plan.tall_b
    place, slice_id = ids[0], ids[1]

    def store(z, s, rows):
        wgu_ref[pl.ds(aligned(z * plan.rows + s * SR), SR), :] = rows[:, :tall]
        for i in range(plan.pieces):
            at = z * plan.down_pad + (s * plan.pieces + i) * SR
            wd_ref[pl.ds(aligned(at), SR), :] = rows[:, tall + i * D : tall + (i + 1) * D]

    for s in range(plan.slices):
        store(place, s, own[s * SR : (s + 1) * SR, :])
    each_slice(plan, place, slice_id, mine, part, store)

    attn_low = attn[...].astype(BF16)
    attn_ref[...] = attn_low
    x1 = x0[...].astype(F32) + mm(attn_low, wgu_ref[:, 2 * ffp :])
    scale = lax.rsqrt(jnp.mean(x1 * x1, axis=1, keepdims=True) + EPSILON)
    unit = x1 * scale
    gains = gain[...]
    n2 = (unit * gains).astype(BF16)
    n2_ref[...] = n2
    c = cot[...]
    out = x1
    dn2 = jnp.zeros_like(x1)
    step = 512 if ffp % 512 == 0 else ffp
    for f in range(0, ffp, step):
        cols = slice(f, f + step)
        up_cols = slice(ffp + f, ffp + f + step)
        gate = mm(n2, wgu_ref[:, cols])
        up = mm(n2, wgu_ref[:, up_cols])
        dhid = against(c, wd_ref[cols, :])
        sig = 1.0 / (1.0 + jnp.exp(-gate))
        silu = gate * sig
        hid = (silu * up).astype(BF16)
        dup = (dhid * silu).astype(BF16)
        dg = (dhid * up * (sig * (1.0 + gate * (1.0 - sig)))).astype(BF16)
        hid_ref[:, cols] = hid
        dg_ref[:, cols] = dg
        dup_ref[:, cols] = dup
        out = out + mm(hid, wd_ref[cols, :])
        dn2 = dn2 + against(dg, wgu_ref[:, cols]) + against(dup, wgu_ref[:, up_cols])
    out_ref[...] = out.astype(BF16)
    e2 = dn2 * gains
    dx1 = c.astype(F32) + scale * (e2 - unit * jnp.mean(e2 * unit, axis=1, keepdims=True))
    dx1_ref[...] = dx1
    dout = dx1.astype(BF16)
    dout_ref[...] = dout
    dattn_ref[...] = against(dout, wgu_ref[:, 2 * ffp :]).astype(BF16)


def spread(plan, place, slice_id, keep, send, copy):
    for c, target in enumerate((keep, send)):
        for o in range(plan.half):
            for k in range(plan.grp):
                copy(xor(place, k), xor(slice_id, 2 * o + c), target, o, k)


def mlp_grads_kernel(plan, ids, n2, hid, dg, dup, cot, attn, dout, keep, send, gu_ref, d_ref):
    ffp, tall = plan.ffp, plan.tall_b
    n2_t = n2[...].T
    gu_ref[:, :ffp] = mm(n2_t, dg[...]).astype(BF16)
    gu_ref[:, ffp : 2 * ffp] = mm(n2_t, dup[...]).astype(BF16)
    gu_ref[:, 2 * ffp :] = rows_of(attn[...], dout[...]).astype(BF16)
    d_ref[...] = rows_of(hid[...], cot[...]).astype(BF16)

    def copy(z, s, target, o, k):
        target[o, k, :, :tall] = gu_ref[pl.ds(aligned(z * plan.rows + s * SR), SR), :]
        for i in range(plan.pieces):
            at = z * plan.down_pad + (s * plan.pieces + i) * SR
            target[o, k, :, tall + i * D : tall + (i + 1) * D] = d_ref[pl.ds(aligned(at), SR), :]

    spread(plan, ids[0], ids[1], keep, send, copy)


def attend_back_kernel(plan, low, high, *refs):
    q, k_in, v_in, attn, dattn, lse, cosine, sines, reach, wa = refs[:10]
    first, last = high == plan.grp, low == 0
    refs = refs[10:]
    if not first:
        dq_in, refs = refs[0], refs[1:]
    dk_ref, dv_ref, dq_ref = refs[:3]
    dn1_refs = refs[3 : 3 + high - low]
    bias_ref, dk_scr, dq_scr = refs[3 + high - low :]
    n = plan.local
    keys_of = slice(low * n, high * n)
    mask_bias(plan, reach[...], bias_ref, range(low, high))

    def pair(i, carry):
        lanes = pl.ds(pl.multiple_of(i * PAIR, PAIR), PAIR)
        q2 = two_heads(q[:, lanes])
        da = dattn[:, lanes]
        da2 = two_heads(da)
        mean = row_sums(two_heads(da.astype(F32) * attn[:, lanes]))
        keys = k_in[keys_of, lanes]
        values = v_in[keys_of, lanes]
        prob = jnp.exp(against(keys, q2) + (bias_ref[...] - lse[i]))
        dprob = against(values, da2)
        dscore = (prob * (dprob - mean)).astype(BF16)
        dv_ref[:, lanes] = mm(prob.astype(BF16), da2).astype(BF16)
        dk_scr[:, lanes] = mm(dscore, q2)
        dq = one_pair(rows_of(keys, dscore)) * (HD**-0.5)
        dq_scr[:, lanes] = dq if first else dq + dq_in[:, lanes]
        return carry

    lax.fori_loop(0, H // 2, pair, 0)
    dq = dq_scr[...]
    if last:
        dq = rotate_back(dq, cosine[:n, :], sines[:n, :]).astype(BF16)
    dq_ref[...] = dq
    for i, k in enumerate(range(low, high)):
        rows, at = slice(i * n, (i + 1) * n), slice(k * n, (k + 1) * n)
        dk = rotate_back(dk_scr[rows, :], cosine[at, :], sines[at, :]).astype(BF16)
        dk_ref[rows, :] = dk
        dn1 = against(dk, wa[:, D : 2 * D]) + against(dv_ref[rows, :], wa[:, 2 * D :])
        if k == 0:
            dn1 = dn1 + against(dq, wa[:, :D])
        dn1_refs[i][...] = dn1.astype(dn1_refs[i].dtype)


def attend_grads_kernel(plan, pieces, ids, n1, dq, *refs):
    keys, values = refs[: len(pieces)], refs[len(pieces) : 2 * len(pieces)]
    keep, send, ga_ref = refs[2 * len(pieces) :]
    n = plan.local
    n1_t = n1[...].T
    ga_ref[:, :D] = mm(n1_t[:, :n], dq[...]).astype(BF16)
    for i, grads in enumerate((keys, values)):
        total = None
        for (low, high), grad in zip(pieces, grads):
            term = mm(n1_t[:, low * n : high * n], grad[...])
            total = term if total is None else total + term
        ga_ref[:, (i + 1) * D : (i + 2) * D] = total.astype(BF16)

    def copy(z, s, target, o, k):
        target[o, k] = ga_ref[pl.ds(aligned(z * plan.rows + s * SR), SR), :]

    spread(plan, ids[0], ids[1], keep, send, copy)


def finish_kernel(plan, ids, mine, part, out_ref):
    for c, source in enumerate((mine, part)):
        for o in range(plan.half):
            s = xor(ids[1], 2 * o + c)
            out_ref[pl.ds(aligned(s * SR), SR), :] = source[o * SR : (o + 1) * SR, :].astype(F32)


def residual_kernel(plan, *refs):
    own, x0, dx1, gain = refs[:4]
    received = refs[4:-1]
    out_ref = refs[-1]
    dn1 = own[...]
    for r in received:
        dn1 = dn1 + r[...].astype(F32)
    x = x0[...].astype(F32)
    scale = lax.rsqrt(jnp.mean(x * x, axis=1, keepdims=True) + EPSILON)
    unit = x * scale
    e1 = dn1 * gain[...]
    out_ref[...] = dx1[...] + scale * (e1 - unit * jnp.mean(e1 * unit, axis=1, keepdims=True))


def join(*values):
    return lax.optimization_barrier(values)


def line_step(plan, bit, blocks):
    return swap("grp", bit, plan.grp, jnp.concatenate(blocks, axis=0))


def fetch_plane(plan, block, *beside):
    got = [swap("rep", 2 * o, plan.rep, block) for o in range(1, plan.half)]
    joined = join(*got, *beside)
    return [jnp.concatenate([block, *joined[: len(got)]], axis=0), *joined[len(got) :]]


def halves_move(plan, terms, step):
    moved = [jnp.concatenate(list(blocks.values()), axis=0) for blocks, _ in terms]
    return [swap("rep", 2 * bits[step], plan.rep, m) for m, (_, bits) in zip(moved, terms)]


def halves_take(plan, terms, step, got):
    done = []
    for whole, (blocks, bits) in zip(got, terms):
        new = jnp.split(whole, len(blocks), axis=0)
        done.append((blocks | {o ^ bits[step]: g for o, g in zip(list(blocks), new)}, bits))
    return done


def column_halves(value):
    middle = value.shape[-1] // 256 * 128
    return value[..., :middle], value[..., middle:]


def fetch_core(plan, mine):
    return swap("rep", 1, plan.rep, mine)


def tie(value, *others):
    return lax.optimization_barrier((value, *others))[0]


def add(*values):
    total = values[0].astype(F32)
    for v in values[1:]:
        total = total + v.astype(F32)
    return total.astype(BF16)


def combine_cores(plan, keep, send):
    got = swap("rep", 1, plan.rep, send)
    return add(keep, got)


def plane_terms(plan, total):
    orders = (plan.plane, plan.plane[::-1])
    return [
        ({o: half[o] for o in range(plan.half)}, bits)
        for half, bits in zip(column_halves(total), orders)
    ]


def plane_step(plan, terms, before=(), after=()):
    arrived = []
    for mine, bits in terms:
        moved = tie(jnp.stack([mine[o] for o in mine if o & bits[0]]), *before)
        arrived.append(swap("rep", 2 * bits[0], plan.rep, moved))
    *arrived, _ = lax.optimization_barrier((*arrived, tuple(after)))
    done = []
    for got, (mine, bits) in zip(arrived, terms):
        leave = [o for o in mine if o & bits[0]]
        done.append(({o ^ bits[0]: add(mine[o ^ bits[0]], got[i]) for i, o in enumerate(leave)}, bits[1:]))
    return done


def arrays_of(terms):
    return [value for mine, _ in terms for value in mine.values()]


def combine_line(plan, total, after=()):
    terms = {k: total[k] for k in range(plan.grp)}
    for step, bit in enumerate(plan.line):
        leave = [k for k in terms if k & bit]
        moved = tie(jnp.stack([terms[k] for k in leave]), *after[step : step + 1])
        got = swap("grp", bit, plan.grp, moved)
        terms = {k ^ bit: add(terms[k ^ bit], got[i]) for i, k in enumerate(leave)}
    final = terms[0]
    bit = plan.slices
    while bit < plan.rep:
        final = add(final, swap("rep", bit, plan.rep, final))
        bit *= 2
    return final


def share(plan, final):
    (mine,) = fetch_plane(plan, final)
    return mine, fetch_core(plan, mine)


def pad_columns(plan, weight):
    rows = weight.shape[0]
    blocks = weight.reshape(rows, plan.grp, plan.down)
    blocks = jnp.pad(blocks, ((0, 0), (0, 0), (0, plan.down_pad - plan.down)))
    return blocks.reshape(rows, plan.ffp)


def drop_columns(plan, grad):
    return jnp.concatenate(
        [grad[:, z * plan.down_pad : z * plan.down_pad + plan.down] for z in range(plan.grp)],
        axis=1,
    )


def pack_b(plan, ids, w_gate, w_up, w_out, w_down):
    if plan.down % 8 == 0:
        return call(
            functools.partial(pack_b_kernel, plan),
            [pltpu.VMEM((plan.rows, plan.wide_b), BF16), pltpu.VMEM((SR, plan.wide_b), BF16)],
            "pack_b",
            (ids, w_gate.T, w_up.T, w_out, w_down),
            us=3,
            far=(w_out, w_down),
        )
    rows = jnp.pad(w_down, ((0, plan.down_pad - plan.down), (0, 0)))
    rows = rows.reshape(plan.slices, plan.pieces, SR, D).transpose(0, 2, 1, 3)
    own = jnp.concatenate(
        [
            pad_columns(plan, w_gate),
            pad_columns(plan, w_up),
            w_out,
            rows.reshape(plan.rows, plan.pieces * D),
        ],
        axis=1,
    )
    return own, lax.dynamic_slice(own, (ids[1] * SR, 0), (SR, plan.wide_b))


def finish_b(plan, ids, final, w_gate, w_up, gain):
    line = gain.reshape(1, -1)
    if plan.down % 8 == 0:
        tall = sds((FF, plan.rows), F32)
        gate, up, down, out, norm = call(
            functools.partial(finish_b_kernel, plan),
            [tall, tall, sds((plan.down, D), F32), sds((plan.rows, D), F32), sds(line.shape, F32)],
            "finish_b",
            (ids, *final, w_gate.T, w_up.T, line),
            [pltpu.VMEM((plan.rows, plan.wide_b), BF16)],
            far=(line,),
        )
        return gate.T, up.T, down, out, norm.reshape(-1)
    (grads,) = call(
        functools.partial(finish_kernel, plan),
        [sds((plan.rows, plan.wide_b), F32)],
        "finish_b",
        (ids, *final),
    )
    ffp = plan.ffp
    down = grads[:, plan.tall_b :].reshape(plan.slices, SR, plan.pieces, D).transpose(0, 2, 1, 3)
    gate = drop_columns(plan, grads[:, :ffp])
    up = drop_columns(plan, grads[:, ffp : 2 * ffp])
    norm = jnp.sum(gate * w_gate.astype(F32) + up * w_up.astype(F32), axis=1) / gain.astype(F32)
    return (
        gate,
        up,
        down.reshape(plan.down_pad, D)[: plan.down],
        grads[:, 2 * ffp : plan.tall_b],
        norm,
    )


def body(plan, tokens, segments, positions, norm1_gain, w_query, w_key, w_value, w_out, norm2_gain, w_gate, w_up, w_down, cotangent):
    g, n = plan.grp, plan.local
    place = lax.axis_index("grp").astype(jnp.int32)
    slice_id = (lax.axis_index("rep") % plan.slices).astype(jnp.int32)
    ids = jnp.stack([place, slice_id])
    x0 = tokens.reshape(n, D)
    cot = cotangent.reshape(n, D)
    reach = jnp.where(segments != 0, positions, 0).reshape(1, n)
    table_cos, table_sin = rotary_tables(plan)
    cosine, sines = jnp.asarray(table_cos), jnp.asarray(table_sin)

    own_a = (w_query, w_key, w_value)
    gains = jnp.stack([norm1_gain, norm2_gain])
    lines = (norm1_gain.reshape(1, -1), norm2_gain.reshape(1, -1))
    (slab_a,) = call(
        functools.partial(pack_a_kernel, plan),
        [pltpu.VMEM((SR, plan.wide_a), BF16)],
        "pack_a",
        (ids, *own_a, *lines),
        us=2,
        far=(*own_a, *lines),
    )
    own_b, slab_b = pack_b(plan, ids, w_gate, w_up, w_out, tie(w_down, slab_a))
    parts, blocks_a, blocks_b = [x0], [slab_a], [slab_b]
    for i, bit in enumerate(reversed(plan.line)):
        got = line_step(plan, bit, blocks_a)
        if i == 0:
            got, first = join(got, shift(1, g, x0))
            parts.append(first)
        else:
            got, blocks_b[-1] = join(got, blocks_b[-1])
        blocks_a += jnp.split(got, len(blocks_a), axis=0)
        count = len(blocks_b)
        blocks_b = [*blocks_b, line_step(plan, bit, blocks_b)]
        if i:
            blocks_b = [*blocks_b[:count], *jnp.split(blocks_b[count], count, axis=0)]
    block_a = jnp.concatenate(blocks_a[1:], axis=0)
    block_b = jnp.concatenate(blocks_b[1:], axis=0)
    for _ in range(2, g - 2):
        parts.append(shift(1, g, parts[-1]))
    mine_a, moving = fetch_plane(plan, block_a, shift(1, g, parts[-1]))
    if g > 3:
        parts.append(moving)
        moving = shift(1, g, moving)
    terms = [
        ({0: half}, bits)
        for half, bits in zip(column_halves(block_b), (plan.plane, plan.plane[::-1]))
    ]
    arriving = halves_move(plan, terms, 0) if plan.plane else []
    *arriving, moving = join(*arriving, moving)
    for step in range(1, len(plan.plane)):
        terms = halves_take(plan, terms, step - 1, arriving)
        arriving = halves_move(plan, terms, step)
    parts.append(moving)
    part_a = fetch_core(plan, tie(mine_a, moving))

    tiles = [mine_a[i * SR : i * SR + 2, 3 * D : 3 * D + plan.rows] for i in range(g - 1)]
    order = jnp.bitwise_xor(jnp.arange(g, dtype=jnp.int32), place)
    chosen = sum(
        jnp.where((order == k)[:, None, None], tile[None], 0).astype(F32)
        for k, tile in zip([0, *plan.order], [gains, *tiles])
    )
    gain1 = chosen[:, 0].reshape(1, D)
    gain2 = chosen[:, 1].reshape(1, D)

    full = plan.full
    attn, q, k_all, v_all, n1, lse, wa = call(
        functools.partial(attend_kernel, plan),
        [
            pltpu.VMEM((n, D), F32),
            pltpu.VMEM((n, D), BF16),
            pltpu.VMEM((full, D), BF16),
            pltpu.VMEM((full, D), BF16),
            pltpu.VMEM((full, D), BF16),
            pltpu.VMEM((H // 2, 1, 2 * n), F32),
            pltpu.VMEM((D, 3 * D), BF16),
        ],
        "attend",
        (ids, *parts, *own_a, mine_a, part_a, gain1, cosine, sines, reach),
        [pltpu.VMEM((full, 2 * n), F32)],
        us=11,
        far=own_a,
    )
    *arriving, attn = join(*arriving, attn)
    if plan.plane:
        terms = halves_take(plan, terms, len(plan.plane) - 1, arriving)
    mine_b = [jnp.concatenate([mine[o] for o in range(plan.half)], axis=0) for mine, _ in terms]
    part_b = [fetch_core(plan, half) for half in mine_b]

    ffp = plan.ffp
    output, dx1, dout, dattn, n2, hid, dg, dup, attn_low = call(
        functools.partial(mlp_kernel, plan),
        [
            sds((n, D), BF16),
            pltpu.VMEM((n, D), F32),
            pltpu.VMEM((n, D), BF16),
            pltpu.VMEM((n, D), BF16),
            pltpu.VMEM((n, D), BF16),
            pltpu.VMEM((n, ffp), BF16),
            pltpu.VMEM((n, ffp), BF16),
            pltpu.VMEM((n, ffp), BF16),
            pltpu.VMEM((n, D), BF16),
        ],
        "mlp",
        (ids, attn, x0, gain2, cot, own_b, *mine_b, *part_b),
        [pltpu.VMEM((D, plan.tall_b), BF16), pltpu.VMEM((ffp, D), BF16)],
        us=8,
    )

    slabs_b = pltpu.VMEM((plan.half, g, SR, plan.wide_b), BF16)
    keep_b, send_b = call(
        functools.partial(mlp_grads_kernel, plan),
        [slabs_b, slabs_b],
        "mlp_grads",
        (ids, n2, hid, dg, dup, cot, attn_low, dout),
        [pltpu.VMEM((D, plan.tall_b), BF16), pltpu.VMEM((ffp, D), BF16)],
        us=6,
    )
    core_b = combine_cores(plan, keep_b, send_b)
    terms_b = plane_terms(plan, core_b)
    steps = len(plan.plane)
    if steps:
        terms_b = plane_step(plan, terms_b)

    pieces = [(k, k + 1) for k in reversed(range(2, g))] + [(0, min(2, g))]
    dq, carry, dks, dvs, sends, hops = None, [], [], [], {}, []
    for low, high in pieces:
        count = high - low
        dk, dv, dq, *dn1 = call(
            functools.partial(attend_back_kernel, plan, low, high),
            [
                pltpu.VMEM((count * n, D), BF16),
                pltpu.VMEM((count * n, D), BF16),
                pltpu.VMEM((n, D), BF16 if low == 0 else F32),
                *[pltpu.VMEM((n, D), F32 if k == 0 else BF16) for k in range(low, high)],
            ],
            "attend_back",
            (q, k_all, v_all, attn, tie(dattn, core_b if carry else keep_b), lse, cosine, sines, reach, wa, *carry),
            [
                pltpu.VMEM((count * n, 2 * n), F32),
                pltpu.VMEM((count * n, D), F32),
                pltpu.VMEM((n, D), F32),
            ],
            us=8,
        )
        carry = [dq]
        dks.append(dk)
        dvs.append(dv)
        sends |= dict(zip(range(low, high), dn1))
    own = sends[0]
    moving = sends[g - 1]
    for k in reversed(range(1, g)):
        moving = shift(-1, g, moving)
        hops.append(moving)
        if k > 1:
            moving = add(tie(moving, *arrays_of(terms_b)), sends[k - 1])

    slabs_a = pltpu.VMEM((plan.half, g, SR, 3 * D), BF16)
    keep_a, send_a = call(
        functools.partial(attend_grads_kernel, plan, pieces),
        [slabs_a, slabs_a],
        "attend_grads",
        (ids, tie(n1, *arrays_of(terms_b)), dq, *dks, *dvs),
        [pltpu.VMEM((D, 3 * D), BF16)],
        us=4,
    )
    core_a = combine_cores(plan, keep_a, send_a)
    terms_a = plane_terms(plan, core_a)
    for step in range(steps):
        if step:
            terms_b = plane_step(plan, terms_b, after=(keep_a,))
        terms_a = plane_step(plan, terms_a)
    total_a = jnp.concatenate([mine[0] for mine, _ in terms_a], axis=-1)
    total_b = jnp.concatenate([mine[0] for mine, _ in terms_b], axis=-1)
    final_b = share(plan, combine_line(plan, total_b, (own, hops[-1])))
    final_a = share(plan, combine_line(plan, total_a, (own, hops[-1])))
    (input_grad,) = call(
        functools.partial(residual_kernel, plan),
        [sds((n, D), F32)],
        "residual",
        (own, x0, dx1, gain1, moving),
        us=2,
    )
    gate, up, down, out, norm2 = finish_b(plan, ids, final_b, w_gate, w_up, norm2_gain)
    shard = sds((plan.rows, D), F32)
    query, key, value, norm1 = call(
        functools.partial(finish_a_kernel, plan),
        [shard, shard, shard, sds((1, plan.rows), F32)],
        "finish_a",
        (ids, *final_a, *own_a, norm1_gain.reshape(1, -1)),
        [pltpu.VMEM((plan.rows, 3 * D), BF16)],
        us=2,
        far=own_a,
    )
    return (
        output.reshape(tokens.shape),
        input_grad.reshape(tokens.shape),
        norm1.reshape(-1),
        query,
        key,
        value,
        out,
        norm2,
        gate,
        up,
        down,
    )


def solution(mesh):
    wide, line, pair = P("grp", None), P("grp"), P("rep", "grp")
    three = P("rep", "grp", None)

    def run(tokens, *rest):
        plan = Plan(mesh, tokens.shape)
        return jax.shard_map(
            functools.partial(body, plan),
            mesh=mesh,
            in_specs=(three, pair, pair, line, wide, wide, wide, wide, line, wide, wide, wide, three),
            out_specs=(three, three, line, wide, wide, wide, wide, line, wide, wide, wide),
            check_vma=False,
        )(tokens, *rest)

    return run
```

```python
import functools

import jax
import jax.numpy as jnp
import numpy as np
from jax import lax
from jax.experimental import pallas as pl
from jax.experimental.pallas import tpu as pltpu
from jax.sharding import PartitionSpec as P

D = 512
H = 8
HD = 64
FF = 1376
EPSILON = 1e-05
NEGATIVE = -1e30
SR = 16
PAIR = 2 * HD
F32 = jnp.float32
BF16 = jnp.bfloat16
VMEM = pl.BlockSpec(memory_space=pltpu.VMEM)
SMEM = pl.BlockSpec(memory_space=pltpu.SMEM)
PARAMS = pltpu.CompilerParams(vmem_limit_bytes=32 * 1024 * 1024)


class Plan:
    def __init__(self, mesh, tokens_shape):
        self.rep = mesh.shape["rep"]
        self.grp = mesh.shape["grp"]
        self.rows = D // self.grp
        self.slices = min(self.rep, self.rows // SR)
        self.half = self.slices // 2
        self.down = FF // self.grp
        self.pieces = -(-self.down // (self.slices * SR))
        self.down_pad = self.pieces * self.slices * SR
        self.ffp = self.down_pad * self.grp
        self.local = tokens_shape[1] // self.grp
        self.full = self.local * self.grp
        self.wide_a = 3 * D + 128
        self.tall_b = 2 * self.ffp + D
        self.wide_b = self.tall_b + self.pieces * D
        self.line = [bit for bit in (1, 2, 4, 8, 16) if bit < self.grp]
        self.plane = [bit for bit in (1, 2, 4, 8, 16) if bit < self.half]
        order = [0]
        for bit in reversed(self.line):
            order += [k ^ bit for k in order]
        self.order = order[1:]


def dot(left, right, dims):
    return lax.dot_general(left, right, ((dims[0], dims[1]), ((), ())), preferred_element_type=F32)


def mm(left, right):
    return dot(left, right, ((1,), (0,)))


def against(left, right):
    return dot(left, right, ((1,), (1,)))


def rows_of(left, right):
    return dot(left, right, ((0,), (0,)))


def call(body, outs, name, args, scratch=(), us=0, far=()):
    specs = [SMEM if a.dtype == jnp.int32 and a.ndim == 1 else VMEM for a in args]
    spaces = [pltpu.HBM if any(a is b for b in far) else pltpu.VMEM for a in args]
    args = [
        pltpu.with_memory_space_constraint(a, space) if spec is VMEM else a
        for a, space, spec in zip(args, spaces, specs)
    ]
    return pl.pallas_call(
        body,
        out_shape=outs,
        in_specs=specs,
        out_specs=[VMEM] * len(outs),
        scratch_shapes=scratch,
        compiler_params=PARAMS,
        cost_estimate=pl.CostEstimate(flops=us * 10**9, bytes_accessed=0, transcendentals=0),
        name=name,
    )(*args)


def sds(shape, dtype):
    return jax.ShapeDtypeStruct(shape, dtype)


def swap(axis, k, size, value):
    return lax.ppermute(value, axis, [(i, i ^ k) for i in range(size)])


def shift(k, size, value):
    return lax.ppermute(value, "grp", [(i, i + k) for i in range(size) if 0 <= i + k < size])


def xor(a, b):
    return lax.bitwise_xor(a, jnp.int32(b)) if isinstance(b, int) else lax.bitwise_xor(a, b)


def aligned(index):
    return pl.multiple_of(index, SR)


def rotary_tables(plan):
    halves = HD // 2
    frequency = 10000.0 ** (-2.0 * np.arange(halves) / HD)
    place = np.concatenate([np.arange(plan.local) - k * plan.local for k in range(plan.grp)])
    angle = place[:, None] * frequency[None, :]
    cosine = np.tile(np.cos(angle), (1, 4)).astype(np.float32)
    sines = np.tile(np.concatenate([-np.sin(angle), np.sin(angle)], axis=1), (1, 2))
    return cosine, sines.astype(np.float32)


def swap_halves(value):
    wide = value.shape[1]
    lane = lax.broadcasted_iota(jnp.int32, value.shape, 1)
    first = (lane % HD) < HD // 2
    return jnp.where(
        first, pltpu.roll(value, wide - HD // 2, 1), pltpu.roll(value, HD // 2, 1)
    )


def tile_heads(table, wide):
    return jnp.concatenate([table] * (wide // table.shape[1]), axis=1)


def rotate(value, cosine, sines):
    wide = value.shape[1]
    return value * tile_heads(cosine, wide) + swap_halves(value) * tile_heads(sines, wide)


def rotate_back(value, cosine, sines):
    wide = value.shape[1]
    return value * tile_heads(cosine, wide) - swap_halves(value) * tile_heads(sines, wide)


def two_heads(value):
    lane = lax.broadcasted_iota(jnp.int32, value.shape, 1)
    zero = jnp.zeros_like(value)
    return jnp.concatenate(
        [jnp.where(lane < HD, value, zero), jnp.where(lane < HD, zero, value)], axis=0
    )


def one_pair(value):
    count = value.shape[1] // 2
    return jnp.concatenate([value[:HD, :count], value[HD:, count:]], axis=0).T


def mask_bias(plan, reach, bias_ref, parts):
    n = plan.local
    key = lax.broadcasted_iota(jnp.int32, (n, n), 0)
    query = lax.broadcasted_iota(jnp.int32, (n, n), 1)
    for i, k in enumerate(parts):
        offset = query - key + k * n
        seen = (offset >= 0) & (offset <= reach)
        bias = jnp.where(seen, 0.0, NEGATIVE).astype(F32)
        bias_ref[i * n : (i + 1) * n, :] = jnp.concatenate([bias, bias], axis=1)


def each_slice(plan, place, slice_id, mine, part, store):
    for c, source in enumerate((mine, part)):
        for o in range(plan.half):
            for i, k in enumerate(plan.order):
                row = (o * (plan.grp - 1) + i) * SR
                rows = [ref[row : row + SR, :] for ref in source]
                rows = jnp.concatenate(rows, axis=1) if len(rows) > 1 else rows[0]
                store(xor(place, k), xor(slice_id, 2 * o + c), rows)


def pack_a_kernel(plan, ids, wq, wk, wv, gain1, gain2, out_ref):
    start = aligned(ids[1] * SR)
    for i, w in enumerate((wq, wk, wv)):
        out_ref[:, i * D : (i + 1) * D] = w[pl.ds(start, SR), :]
    out_ref[:, 3 * D :] = jnp.zeros((SR, 128), BF16)
    out_ref[0:1, 3 * D : 3 * D + plan.rows] = gain1[...]
    out_ref[1:2, 3 * D : 3 * D + plan.rows] = gain2[...]


def pack_b_kernel(plan, ids, gate_t, up_t, out, down, own_ref, slab_ref):
    for i, w in enumerate((gate_t, up_t)):
        for z in range(plan.grp):
            rows = w[z * plan.down : (z + 1) * plan.down, :].astype(F32)
            gap = jnp.zeros((plan.down_pad - plan.down, plan.rows), F32)
            at = i * plan.ffp + z * plan.down_pad
            block = jnp.concatenate([rows, gap], axis=0).T
            own_ref[:, at : at + plan.down_pad] = block.astype(BF16)
    own_ref[:, 2 * plan.ffp : plan.tall_b] = out[...]
    for s in range(plan.slices):
        for i in range(plan.pieces):
            at = (s * plan.pieces + i) * SR
            have = max(0, min(SR, plan.down - at))
            rows = []
            if have:
                rows.append(down[at : at + have, :])
            if have < SR:
                rows.append(jnp.zeros((SR - have, D), BF16))
            cols = slice(plan.tall_b + i * D, plan.tall_b + (i + 1) * D)
            own_ref[s * SR : (s + 1) * SR, cols] = (
                jnp.concatenate(rows, axis=0) if len(rows) > 1 else rows[0]
            )
    slab_ref[...] = own_ref[pl.ds(aligned(ids[1] * SR), SR), :]


def gather_slices(plan, slice_id, mine, part, target):
    for c, source in enumerate((mine, part)):
        for o in range(plan.half):
            s = xor(slice_id, 2 * o + c)
            target[pl.ds(aligned(s * SR), SR), :] = source[o * SR : (o + 1) * SR, :]


def row_sums(value):
    ones = jnp.ones((8, value.shape[1]), F32)
    return lax.dot_general(
        ones, value, (((1,), (1,)), ((), ())), precision=lax.Precision.HIGHEST,
        preferred_element_type=F32,
    )[0:1, :]


def finish_a_kernel(plan, ids, mine, part, wq, wk, wv, gain, *refs):
    scratch = refs[-1]
    gather_slices(plan, ids[1], mine, part, scratch)
    dots = jnp.zeros((plan.rows, D), F32)
    for i, w in enumerate((wq, wk, wv)):
        grad = scratch[:, i * D : (i + 1) * D].astype(F32)
        refs[i][...] = grad
        dots = dots + grad * w[...].astype(F32)
    refs[3][...] = row_sums(dots) / gain[...].astype(F32)


def finish_b_kernel(plan, ids, mine, part, gate_t, up_t, gain, gate_ref, up_ref, down_ref, out_ref, norm_ref, scratch):
    gather_slices(plan, ids[1], mine, part, scratch)
    norm = jnp.zeros((1, plan.rows), F32)
    for i, (ref, weight) in enumerate(((gate_ref, gate_t), (up_ref, up_t))):
        for z in range(plan.grp):
            at = i * plan.ffp + z * plan.down_pad
            block = scratch[:, at : at + plan.down_pad].astype(F32).T[: plan.down, :]
            rows = slice(z * plan.down, (z + 1) * plan.down)
            ref[rows, :] = block
            norm = norm + jnp.sum(block * weight[rows, :].astype(F32), axis=0, keepdims=True)
    norm_ref[...] = norm / gain[...].astype(F32)
    out_ref[...] = scratch[:, 2 * plan.ffp : plan.tall_b].astype(F32)
    for s in range(plan.slices):
        for i in range(plan.pieces):
            at = (s * plan.pieces + i) * SR
            have = max(0, min(SR, plan.down - at))
            if have:
                cols = slice(plan.tall_b + i * D, plan.tall_b + (i + 1) * D)
                rows = scratch[s * SR : (s + 1) * SR, cols].astype(F32)
                down_ref[at : at + have, :] = rows[:have, :]


def attend_kernel(plan, ids, *refs):
    g = plan.grp
    parts = refs[:g]
    own = refs[g : g + 3]
    mine, part, gain, cosine, sines, reach = refs[g + 3 : g + 9]
    attn_ref, q_ref, k_ref, v_ref, n1_ref, lse_ref, wa_ref = refs[g + 9 : g + 16]
    bias_ref, = refs[g + 16 :]
    n = plan.local
    place, slice_id = ids[0], ids[1]
    for i in range(3):
        wa_ref[pl.ds(aligned(place * plan.rows), plan.rows), i * D : (i + 1) * D] = own[i][...]

    def store(z, s, rows):
        wa_ref[pl.ds(aligned(z * plan.rows + s * SR), SR), :] = rows[:, : 3 * D]

    each_slice(plan, place, slice_id, [mine], [part], store)
    mask_bias(plan, reach[...], bias_ref, range(g))
    gains = gain[...]
    for k in range(g):
        x = parts[k][...].astype(F32)
        unit = x * lax.rsqrt(jnp.mean(x * x, axis=1, keepdims=True) + EPSILON)
        n1 = (unit * gains).astype(BF16)
        rows = slice(k * n, (k + 1) * n)
        n1_ref[rows, :] = n1
        cos_k, sin_k = cosine[rows, :], sines[rows, :]
        k_ref[rows, :] = rotate(mm(n1, wa_ref[:, D : 2 * D]), cos_k, sin_k).astype(BF16)
        v_ref[rows, :] = mm(n1, wa_ref[:, 2 * D : 3 * D]).astype(BF16)
        if k == 0:
            q_ref[...] = rotate(mm(n1, wa_ref[:, :D]), cos_k, sin_k).astype(BF16) * BF16(
                HD**-0.5
            )

    def pair(i, carry):
        lanes = pl.ds(pl.multiple_of(i * PAIR, PAIR), PAIR)
        score = against(k_ref[:, lanes], two_heads(q_ref[:, lanes])) + bias_ref[...]
        peak = jnp.max(score, axis=0, keepdims=True)
        exponent = jnp.exp(score - peak)
        total = jnp.sum(exponent, axis=0, keepdims=True)
        out = rows_of(v_ref[:, lanes], exponent.astype(BF16)) / total
        attn_ref[:, lanes] = one_pair(out)
        lse_ref[i] = peak + jnp.log(total)
        return carry

    lax.fori_loop(0, H // 2, pair, 0)


def mlp_kernel(plan, ids, *refs):
    attn, x0, gain, cot, own = refs[:5]
    mine, part = refs[5:7], refs[7:9]
    out_ref, dx1_ref, dout_ref, dattn_ref, n2_ref, hid_ref, dg_ref, dup_ref, attn_ref = refs[9:18]
    wgu_ref, wd_ref = refs[18:]
    ffp, tall = plan.ffp, plan.tall_b
    place, slice_id = ids[0], ids[1]

    def store(z, s, rows):
        wgu_ref[pl.ds(aligned(z * plan.rows + s * SR), SR), :] = rows[:, :tall]
        for i in range(plan.pieces):
            at = z * plan.down_pad + (s * plan.pieces + i) * SR
            wd_ref[pl.ds(aligned(at), SR), :] = rows[:, tall + i * D : tall + (i + 1) * D]

    for s in range(plan.slices):
        store(place, s, own[s * SR : (s + 1) * SR, :])
    each_slice(plan, place, slice_id, mine, part, store)

    attn_low = attn[...].astype(BF16)
    attn_ref[...] = attn_low
    x1 = x0[...].astype(F32) + mm(attn_low, wgu_ref[:, 2 * ffp :])
    scale = lax.rsqrt(jnp.mean(x1 * x1, axis=1, keepdims=True) + EPSILON)
    unit = x1 * scale
    gains = gain[...]
    n2 = (unit * gains).astype(BF16)
    n2_ref[...] = n2
    c = cot[...]
    out = x1
    dn2 = jnp.zeros_like(x1)
    step = 512 if ffp % 512 == 0 else ffp
    for f in range(0, ffp, step):
        cols = slice(f, f + step)
        up_cols = slice(ffp + f, ffp + f + step)
        gate = mm(n2, wgu_ref[:, cols])
        up = mm(n2, wgu_ref[:, up_cols])
        dhid = against(c, wd_ref[cols, :])
        sig = 1.0 / (1.0 + jnp.exp(-gate))
        silu = gate * sig
        hid = (silu * up).astype(BF16)
        dup = (dhid * silu).astype(BF16)
        dg = (dhid * up * (sig * (1.0 + gate * (1.0 - sig)))).astype(BF16)
        hid_ref[:, cols] = hid
        dg_ref[:, cols] = dg
        dup_ref[:, cols] = dup
        out = out + mm(hid, wd_ref[cols, :])
        dn2 = dn2 + against(dg, wgu_ref[:, cols]) + against(dup, wgu_ref[:, up_cols])
    out_ref[...] = out.astype(BF16)
    e2 = dn2 * gains
    dx1 = c.astype(F32) + scale * (e2 - unit * jnp.mean(e2 * unit, axis=1, keepdims=True))
    dx1_ref[...] = dx1
    dout = dx1.astype(BF16)
    dout_ref[...] = dout
    dattn_ref[...] = against(dout, wgu_ref[:, 2 * ffp :]).astype(BF16)


def spread(plan, place, slice_id, keep, send, copy):
    for c, target in enumerate((keep, send)):
        for o in range(plan.half):
            for k in range(plan.grp):
                copy(xor(place, k), xor(slice_id, 2 * o + c), target, o, k)


def mlp_grads_kernel(plan, ids, n2, hid, dg, dup, cot, attn, dout, keep, send, gu_ref, d_ref):
    ffp, tall = plan.ffp, plan.tall_b
    n2_t = n2[...].T
    gu_ref[:, :ffp] = mm(n2_t, dg[...]).astype(BF16)
    gu_ref[:, ffp : 2 * ffp] = mm(n2_t, dup[...]).astype(BF16)
    gu_ref[:, 2 * ffp :] = rows_of(attn[...], dout[...]).astype(BF16)
    d_ref[...] = rows_of(hid[...], cot[...]).astype(BF16)

    def copy(z, s, target, o, k):
        target[o, k, :, :tall] = gu_ref[pl.ds(aligned(z * plan.rows + s * SR), SR), :]
        for i in range(plan.pieces):
            at = z * plan.down_pad + (s * plan.pieces + i) * SR
            target[o, k, :, tall + i * D : tall + (i + 1) * D] = d_ref[pl.ds(aligned(at), SR), :]

    spread(plan, ids[0], ids[1], keep, send, copy)


def attend_back_kernel(plan, low, high, *refs):
    q, k_in, v_in, attn, dattn, lse, cosine, sines, reach, wa = refs[:10]
    first, last = high == plan.grp, low == 0
    refs = refs[10:]
    if not first:
        dq_in, refs = refs[0], refs[1:]
    dk_ref, dv_ref, dq_ref = refs[:3]
    dn1_refs = refs[3 : 3 + high - low]
    bias_ref, dk_scr, dq_scr = refs[3 + high - low :]
    n = plan.local
    keys_of = slice(low * n, high * n)
    mask_bias(plan, reach[...], bias_ref, range(low, high))

    def pair(i, carry):
        lanes = pl.ds(pl.multiple_of(i * PAIR, PAIR), PAIR)
        q2 = two_heads(q[:, lanes])
        da = dattn[:, lanes]
        da2 = two_heads(da)
        mean = row_sums(two_heads(da.astype(F32) * attn[:, lanes]))
        keys = k_in[keys_of, lanes]
        values = v_in[keys_of, lanes]
        prob = jnp.exp(against(keys, q2) + (bias_ref[...] - lse[i]))
        dprob = against(values, da2)
        dscore = (prob * (dprob - mean)).astype(BF16)
        dv_ref[:, lanes] = mm(prob.astype(BF16), da2).astype(BF16)
        dk_scr[:, lanes] = mm(dscore, q2)
        dq = one_pair(rows_of(keys, dscore)) * (HD**-0.5)
        dq_scr[:, lanes] = dq if first else dq + dq_in[:, lanes]
        return carry

    lax.fori_loop(0, H // 2, pair, 0)
    dq = dq_scr[...]
    if last:
        dq = rotate_back(dq, cosine[:n, :], sines[:n, :]).astype(BF16)
    dq_ref[...] = dq
    for i, k in enumerate(range(low, high)):
        rows, at = slice(i * n, (i + 1) * n), slice(k * n, (k + 1) * n)
        dk = rotate_back(dk_scr[rows, :], cosine[at, :], sines[at, :]).astype(BF16)
        dk_ref[rows, :] = dk
        dn1 = against(dk, wa[:, D : 2 * D]) + against(dv_ref[rows, :], wa[:, 2 * D :])
        if k == 0:
            dn1 = dn1 + against(dq, wa[:, :D])
        dn1_refs[i][...] = dn1.astype(dn1_refs[i].dtype)


def attend_grads_kernel(plan, pieces, ids, n1, dq, *refs):
    keys, values = refs[: len(pieces)], refs[len(pieces) : 2 * len(pieces)]
    keep, send, ga_ref = refs[2 * len(pieces) :]
    n = plan.local
    n1_t = n1[...].T
    ga_ref[:, :D] = mm(n1_t[:, :n], dq[...]).astype(BF16)
    for i, grads in enumerate((keys, values)):
        total = None
        for (low, high), grad in zip(pieces, grads):
            term = mm(n1_t[:, low * n : high * n], grad[...])
            total = term if total is None else total + term
        ga_ref[:, (i + 1) * D : (i + 2) * D] = total.astype(BF16)

    def copy(z, s, target, o, k):
        target[o, k] = ga_ref[pl.ds(aligned(z * plan.rows + s * SR), SR), :]

    spread(plan, ids[0], ids[1], keep, send, copy)


def finish_kernel(plan, ids, mine, part, out_ref):
    for c, source in enumerate((mine, part)):
        for o in range(plan.half):
            s = xor(ids[1], 2 * o + c)
            out_ref[pl.ds(aligned(s * SR), SR), :] = source[o * SR : (o + 1) * SR, :].astype(F32)


def residual_kernel(plan, *refs):
    own, x0, dx1, gain = refs[:4]
    received = refs[4:-1]
    out_ref = refs[-1]
    dn1 = own[...]
    for r in received:
        dn1 = dn1 + r[...].astype(F32)
    x = x0[...].astype(F32)
    scale = lax.rsqrt(jnp.mean(x * x, axis=1, keepdims=True) + EPSILON)
    unit = x * scale
    e1 = dn1 * gain[...]
    out_ref[...] = dx1[...] + scale * (e1 - unit * jnp.mean(e1 * unit, axis=1, keepdims=True))


def join(*values):
    return lax.optimization_barrier(values)


def line_step(plan, bit, blocks):
    return swap("grp", bit, plan.grp, jnp.concatenate(blocks, axis=0))


def fetch_plane(plan, block, *beside):
    got = [swap("rep", 2 * o, plan.rep, block) for o in range(1, plan.half)]
    joined = join(*got, *beside)
    return [jnp.concatenate([block, *joined[: len(got)]], axis=0), *joined[len(got) :]]


def halves_move(plan, terms, step):
    moved = [jnp.concatenate(list(blocks.values()), axis=0) for blocks, _ in terms]
    return [swap("rep", 2 * bits[step], plan.rep, m) for m, (_, bits) in zip(moved, terms)]


def halves_take(plan, terms, step, got):
    done = []
    for whole, (blocks, bits) in zip(got, terms):
        new = jnp.split(whole, len(blocks), axis=0)
        done.append((blocks | {o ^ bits[step]: g for o, g in zip(list(blocks), new)}, bits))
    return done


def column_halves(value):
    middle = value.shape[-1] // 256 * 128
    return value[..., :middle], value[..., middle:]


def fetch_core(plan, mine):
    return swap("rep", 1, plan.rep, mine)


def tie(value, *others):
    return lax.optimization_barrier((value, *others))[0]


def add(*values):
    total = values[0].astype(F32)
    for v in values[1:]:
        total = total + v.astype(F32)
    return total.astype(BF16)


def combine_cores(plan, keep, send):
    got = swap("rep", 1, plan.rep, send)
    return add(keep, got)


def plane_terms(plan, total):
    orders = (plan.plane, plan.plane[::-1])
    return [
        ({o: half[o] for o in range(plan.half)}, bits)
        for half, bits in zip(column_halves(total), orders)
    ]


def plane_step(plan, terms, before=(), after=()):
    arrived = []
    for mine, bits in terms:
        moved = tie(jnp.stack([mine[o] for o in mine if o & bits[0]]), *before)
        arrived.append(swap("rep", 2 * bits[0], plan.rep, moved))
    *arrived, _ = lax.optimization_barrier((*arrived, tuple(after)))
    done = []
    for got, (mine, bits) in zip(arrived, terms):
        leave = [o for o in mine if o & bits[0]]
        done.append(({o ^ bits[0]: add(mine[o ^ bits[0]], got[i]) for i, o in enumerate(leave)}, bits[1:]))
    return done


def arrays_of(terms):
    return [value for mine, _ in terms for value in mine.values()]


def combine_line(plan, total, after=()):
    terms = {k: total[k] for k in range(plan.grp)}
    for step, bit in enumerate(plan.line):
        leave = [k for k in terms if k & bit]
        moved = tie(jnp.stack([terms[k] for k in leave]), *after[step : step + 1])
        got = swap("grp", bit, plan.grp, moved)
        terms = {k ^ bit: add(terms[k ^ bit], got[i]) for i, k in enumerate(leave)}
    final = terms[0]
    bit = plan.slices
    while bit < plan.rep:
        final = add(final, swap("rep", bit, plan.rep, final))
        bit *= 2
    return final


def share(plan, final):
    (mine,) = fetch_plane(plan, final)
    return mine, fetch_core(plan, mine)


def pad_columns(plan, weight):
    rows = weight.shape[0]
    blocks = weight.reshape(rows, plan.grp, plan.down)
    blocks = jnp.pad(blocks, ((0, 0), (0, 0), (0, plan.down_pad - plan.down)))
    return blocks.reshape(rows, plan.ffp)


def drop_columns(plan, grad):
    return jnp.concatenate(
        [grad[:, z * plan.down_pad : z * plan.down_pad + plan.down] for z in range(plan.grp)],
        axis=1,
    )


def pack_b(plan, ids, w_gate, w_up, w_out, w_down):
    if plan.down % 8 == 0:
        return call(
            functools.partial(pack_b_kernel, plan),
            [pltpu.VMEM((plan.rows, plan.wide_b), BF16), pltpu.VMEM((SR, plan.wide_b), BF16)],
            "pack_b",
            (ids, w_gate.T, w_up.T, w_out, w_down),
            us=3,
            far=(w_out, w_down),
        )
    rows = jnp.pad(w_down, ((0, plan.down_pad - plan.down), (0, 0)))
    rows = rows.reshape(plan.slices, plan.pieces, SR, D).transpose(0, 2, 1, 3)
    own = jnp.concatenate(
        [
            pad_columns(plan, w_gate),
            pad_columns(plan, w_up),
            w_out,
            rows.reshape(plan.rows, plan.pieces * D),
        ],
        axis=1,
    )
    return own, lax.dynamic_slice(own, (ids[1] * SR, 0), (SR, plan.wide_b))


def finish_b(plan, ids, final, w_gate, w_up, gain):
    line = gain.reshape(1, -1)
    if plan.down % 8 == 0:
        tall = sds((FF, plan.rows), F32)
        gate, up, down, out, norm = call(
            functools.partial(finish_b_kernel, plan),
            [tall, tall, sds((plan.down, D), F32), sds((plan.rows, D), F32), sds(line.shape, F32)],
            "finish_b",
            (ids, *final, w_gate.T, w_up.T, line),
            [pltpu.VMEM((plan.rows, plan.wide_b), BF16)],
            far=(line,),
        )
        return gate.T, up.T, down, out, norm.reshape(-1)
    (grads,) = call(
        functools.partial(finish_kernel, plan),
        [sds((plan.rows, plan.wide_b), F32)],
        "finish_b",
        (ids, *final),
    )
    ffp = plan.ffp
    down = grads[:, plan.tall_b :].reshape(plan.slices, SR, plan.pieces, D).transpose(0, 2, 1, 3)
    gate = drop_columns(plan, grads[:, :ffp])
    up = drop_columns(plan, grads[:, ffp : 2 * ffp])
    norm = jnp.sum(gate * w_gate.astype(F32) + up * w_up.astype(F32), axis=1) / gain.astype(F32)
    return (
        gate,
        up,
        down.reshape(plan.down_pad, D)[: plan.down],
        grads[:, 2 * ffp : plan.tall_b],
        norm,
    )


def body(plan, tokens, segments, positions, norm1_gain, w_query, w_key, w_value, w_out, norm2_gain, w_gate, w_up, w_down, cotangent):
    g, n = plan.grp, plan.local
    place = lax.axis_index("grp").astype(jnp.int32)
    slice_id = (lax.axis_index("rep") % plan.slices).astype(jnp.int32)
    ids = jnp.stack([place, slice_id])
    x0 = tokens.reshape(n, D)
    cot = cotangent.reshape(n, D)
    reach = jnp.where(segments != 0, positions, 0).reshape(1, n)
    table_cos, table_sin = rotary_tables(plan)
    cosine, sines = jnp.asarray(table_cos), jnp.asarray(table_sin)

    own_a = (w_query, w_key, w_value)
    gains = jnp.stack([norm1_gain, norm2_gain])
    lines = (norm1_gain.reshape(1, -1), norm2_gain.reshape(1, -1))
    (slab_a,) = call(
        functools.partial(pack_a_kernel, plan),
        [pltpu.VMEM((SR, plan.wide_a), BF16)],
        "pack_a",
        (ids, *own_a, *lines),
        us=2,
        far=(*own_a, *lines),
    )
    own_b, slab_b = pack_b(plan, ids, w_gate, w_up, w_out, tie(w_down, slab_a))
    parts, blocks_a, blocks_b = [x0], [slab_a], [slab_b]
    for i, bit in enumerate(reversed(plan.line)):
        got = line_step(plan, bit, blocks_a)
        if i == 0:
            got, first = join(got, shift(1, g, x0))
            parts.append(first)
        else:
            got, blocks_b[-1] = join(got, blocks_b[-1])
        blocks_a += jnp.split(got, len(blocks_a), axis=0)
        count = len(blocks_b)
        blocks_b = [*blocks_b, line_step(plan, bit, blocks_b)]
        if i:
            blocks_b = [*blocks_b[:count], *jnp.split(blocks_b[count], count, axis=0)]
    block_a = jnp.concatenate(blocks_a[1:], axis=0)
    block_b = jnp.concatenate(blocks_b[1:], axis=0)
    for _ in range(2, g - 2):
        parts.append(shift(1, g, parts[-1]))
    mine_a, moving = fetch_plane(plan, block_a, shift(1, g, parts[-1]))
    if g > 3:
        parts.append(moving)
        moving = shift(1, g, moving)
    terms = [
        ({0: half}, bits)
        for half, bits in zip(column_halves(block_b), (plan.plane, plan.plane[::-1]))
    ]
    arriving = halves_move(plan, terms, 0) if plan.plane else []
    *arriving, moving = join(*arriving, moving)
    for step in range(1, len(plan.plane)):
        terms = halves_take(plan, terms, step - 1, arriving)
        arriving = halves_move(plan, terms, step)
    parts.append(moving)
    part_a = fetch_core(plan, tie(mine_a, moving))

    tiles = [mine_a[i * SR : i * SR + 2, 3 * D : 3 * D + plan.rows] for i in range(g - 1)]
    order = jnp.bitwise_xor(jnp.arange(g, dtype=jnp.int32), place)
    chosen = sum(
        jnp.where((order == k)[:, None, None], tile[None], 0).astype(F32)
        for k, tile in zip([0, *plan.order], [gains, *tiles])
    )
    gain1 = chosen[:, 0].reshape(1, D)
    gain2 = chosen[:, 1].reshape(1, D)

    full = plan.full
    attn, q, k_all, v_all, n1, lse, wa = call(
        functools.partial(attend_kernel, plan),
        [
            pltpu.VMEM((n, D), F32),
            pltpu.VMEM((n, D), BF16),
            pltpu.VMEM((full, D), BF16),
            pltpu.VMEM((full, D), BF16),
            pltpu.VMEM((full, D), BF16),
            pltpu.VMEM((H // 2, 1, 2 * n), F32),
            pltpu.VMEM((D, 3 * D), BF16),
        ],
        "attend",
        (ids, *parts, *own_a, mine_a, part_a, gain1, cosine, sines, reach),
        [pltpu.VMEM((full, 2 * n), F32)],
        us=11,
        far=own_a,
    )
    *arriving, attn = join(*arriving, attn)
    if plan.plane:
        terms = halves_take(plan, terms, len(plan.plane) - 1, arriving)
    mine_b = [jnp.concatenate([mine[o] for o in range(plan.half)], axis=0) for mine, _ in terms]
    part_b = [fetch_core(plan, half) for half in mine_b]

    ffp = plan.ffp
    output, dx1, dout, dattn, n2, hid, dg, dup, attn_low = call(
        functools.partial(mlp_kernel, plan),
        [
            sds((n, D), BF16),
            pltpu.VMEM((n, D), F32),
            pltpu.VMEM((n, D), BF16),
            pltpu.VMEM((n, D), BF16),
            pltpu.VMEM((n, D), BF16),
            pltpu.VMEM((n, ffp), BF16),
            pltpu.VMEM((n, ffp), BF16),
            pltpu.VMEM((n, ffp), BF16),
            pltpu.VMEM((n, D), BF16),
        ],
        "mlp",
        (ids, attn, x0, gain2, cot, own_b, *mine_b, *part_b),
        [pltpu.VMEM((D, plan.tall_b), BF16), pltpu.VMEM((ffp, D), BF16)],
        us=8,
    )

    slabs_b = pltpu.VMEM((plan.half, g, SR, plan.wide_b), BF16)
    keep_b, send_b = call(
        functools.partial(mlp_grads_kernel, plan),
        [slabs_b, slabs_b],
        "mlp_grads",
        (ids, n2, hid, dg, dup, cot, attn_low, dout),
        [pltpu.VMEM((D, plan.tall_b), BF16), pltpu.VMEM((ffp, D), BF16)],
        us=6,
    )
    core_b = combine_cores(plan, keep_b, send_b)
    terms_b = plane_terms(plan, core_b)
    steps = len(plan.plane)
    if steps:
        terms_b = plane_step(plan, terms_b)

    pieces = [(k, k + 1) for k in reversed(range(2, g))] + [(0, min(2, g))]
    dq, carry, dks, dvs, sends, hops = None, [], [], [], {}, []
    for low, high in pieces:
        count = high - low
        dk, dv, dq, *dn1 = call(
            functools.partial(attend_back_kernel, plan, low, high),
            [
                pltpu.VMEM((count * n, D), BF16),
                pltpu.VMEM((count * n, D), BF16),
                pltpu.VMEM((n, D), BF16 if low == 0 else F32),
                *[pltpu.VMEM((n, D), F32 if k == 0 else BF16) for k in range(low, high)],
            ],
            "attend_back",
            (q, k_all, v_all, attn, tie(dattn, core_b if carry else keep_b), lse, cosine, sines, reach, wa, *carry),
            [
                pltpu.VMEM((count * n, 2 * n), F32),
                pltpu.VMEM((count * n, D), F32),
                pltpu.VMEM((n, D), F32),
            ],
            us=8,
        )
        carry = [dq]
        dks.append(dk)
        dvs.append(dv)
        sends |= dict(zip(range(low, high), dn1))
    own = sends[0]
    moving = sends[g - 1]
    for k in reversed(range(1, g)):
        moving = shift(-1, g, moving)
        hops.append(moving)
        if k > 1:
            moving = add(tie(moving, *arrays_of(terms_b)), sends[k - 1])

    slabs_a = pltpu.VMEM((plan.half, g, SR, 3 * D), BF16)
    keep_a, send_a = call(
        functools.partial(attend_grads_kernel, plan, pieces),
        [slabs_a, slabs_a],
        "attend_grads",
        (ids, tie(n1, *arrays_of(terms_b)), dq, *dks, *dvs),
        [pltpu.VMEM((D, 3 * D), BF16)],
        us=4,
    )
    core_a = combine_cores(plan, keep_a, send_a)
    terms_a = plane_terms(plan, core_a)
    for step in range(steps):
        if step:
            terms_b = plane_step(plan, terms_b, after=(keep_a,))
        terms_a = plane_step(plan, terms_a)
    total_a = jnp.concatenate([mine[0] for mine, _ in terms_a], axis=-1)
    total_b = jnp.concatenate([mine[0] for mine, _ in terms_b], axis=-1)
    final_b = share(plan, combine_line(plan, total_b, (own, own)))
    final_a = share(plan, combine_line(plan, total_a, (own, hops[-1])))
    (input_grad,) = call(
        functools.partial(residual_kernel, plan),
        [sds((n, D), F32)],
        "residual",
        (own, x0, dx1, gain1, moving),
        us=2,
    )
    gate, up, down, out, norm2 = finish_b(plan, ids, final_b, w_gate, w_up, norm2_gain)
    shard = sds((plan.rows, D), F32)
    query, key, value, norm1 = call(
        functools.partial(finish_a_kernel, plan),
        [shard, shard, shard, sds((1, plan.rows), F32)],
        "finish_a",
        (ids, *final_a, *own_a, norm1_gain.reshape(1, -1)),
        [pltpu.VMEM((plan.rows, 3 * D), BF16)],
        us=2,
        far=own_a,
    )
    return (
        output.reshape(tokens.shape),
        input_grad.reshape(tokens.shape),
        norm1.reshape(-1),
        query,
        key,
        value,
        out,
        norm2,
        gate,
        up,
        down,
    )


def solution(mesh):
    wide, line, pair = P("grp", None), P("grp"), P("rep", "grp")
    three = P("rep", "grp", None)

    def run(tokens, *rest):
        plan = Plan(mesh, tokens.shape)
        return jax.shard_map(
            functools.partial(body, plan),
            mesh=mesh,
            in_specs=(three, pair, pair, line, wide, wide, wide, wide, line, wide, wide, wide, three),
            out_specs=(three, three, line, wide, wide, wide, wide, line, wide, wide, wide),
            check_vma=False,
        )(tokens, *rest)

    return run
```
